32 devices in a mesh: cuts: 4 (over x, core), exp: 2 (over y), fsdp: 4 (over z).
Axes of the slice: x: 2, y: 2, z: 4, core: 2. Of those that a mesh axis runs over, the one named last changes fastest.
Arguments:
- tokens: bfloat16 [4096, 4096], P(('cuts', 'exp', 'fsdp')), may hold values from -6 to 6
- out_grad: bfloat16 [4096, 4096], P(('cuts', 'exp', 'fsdp')), may hold values from -6 to 6
- expert_ids: int32 [4096, 2], P(('cuts', 'exp', 'fsdp')), may hold values from 0 to 7, as said below
- gate_probs: bfloat16 [4096, 2], P(('cuts', 'exp', 'fsdp')), may hold values from 0.049804688 to 0.94921875
- params: float32 [3, 8, 4096, 256], P(None, 'exp', ('cuts', 'fsdp')), may hold values from -0.1875 to 0.1875
- moment_first: float32 [3, 8, 4096, 256], P(None, 'exp', ('cuts', 'fsdp')), may hold values from -60 to 60
- moment_second: float32 [3, 8, 4096, 256], P(None, 'exp', ('cuts', 'fsdp')), may hold values from 64 to 1024
Outputs:
- token_grad: bfloat16 [4096, 4096], P(('cuts', 'exp', 'fsdp'))
- gate_grad: bfloat16 [4096, 2], P(('cuts', 'exp', 'fsdp'))
- new_params: float32 [3, 8, 4096, 256], P(None, 'exp', ('cuts', 'fsdp'))
- new_first: float32 [3, 8, 4096, 256], P(None, 'exp', ('cuts', 'fsdp'))
- new_second: float32 [3, 8, 4096, 256], P(None, 'exp', ('cuts', 'fsdp'))
The draws below stay inside these ranges and needn't reach their ends.
Inputs may be any that keep to these rules, and one draw needn't show every extreme that they name: `expert_ids`: the two ids of a token differ. Among the tokens of one device no expert is named more than 40 times. Each device names some expert exactly 40 times, and the devices that share their cuts and fsdp indices have one such expert in common.
All inputs are finite; a program needn't handle non-finite values.
Results may differ from the reference program's by a relative error of at most 0.0079.
Values may be sent and summed in bfloat16 or wider, within the bound.
A program may use at most 192 MiB of HBM per device.

```python
import math
import jax
import jax.numpy as jnp
from jax import lax

D = 4096
EXPERTS = 8
F = 256
TOK_DEV = 128
CAP = 40
SENDERS = 2
SHARDS = 4
TOKENS = 4096


def draw_expert_ids(key, part):
    blocks = TOKENS // TOK_DEV
    unit = TOK_DEV // 32
    groups = blocks // SENDERS
    pattern = jnp.array([10, 9, 9, 8, 8, 7, 7, 6], jnp.int32) * unit
    shifts = jax.random.randint(jax.random.fold_in(key, 11), (blocks, 3), -unit, unit + 1).astype(jnp.int32)
    nothing = jnp.zeros((blocks,), jnp.int32)
    delta = jnp.stack([nothing, shifts[:, 0], -shifts[:, 0], shifts[:, 1], -shifts[:, 1], shifts[:, 2], -shifts[:, 2], nothing], axis=1)
    counts = pattern[None, :] + delta
    ends = jnp.cumsum(counts, axis=1)
    position = jnp.arange(2 * TOK_DEV, dtype=jnp.int32)
    pattern_slot = jnp.sum((position[None, :, None] >= ends[:, None, :]).astype(jnp.int32), axis=2)
    block_number = jnp.arange(blocks, dtype=jnp.int32)
    group_number = block_number // (SENDERS * SHARDS) * SHARDS + block_number % SHARDS
    full_expert = jax.random.randint(jax.random.fold_in(key, 12), (groups,), 0, 8).astype(jnp.int32)[group_number]
    order_keys = jax.random.split(jax.random.fold_in(key, 13), blocks)
    orders = jax.vmap(lambda one: jax.random.permutation(one, 8))(order_keys).astype(jnp.int32)
    labels = (orders - orders[:, :1] + full_expert[:, None]) % 8
    named = jnp.take_along_axis(labels, pattern_slot, axis=1)
    first_half = named[:, :TOK_DEV]
    second_half = named[:, TOK_DEV:]
    flipped = jax.random.randint(jax.random.fold_in(key, 14), (blocks, TOK_DEV), 0, 2).astype(jnp.int32)
    paired = jnp.stack([jnp.where(flipped == 1, second_half, first_half), jnp.where(flipped == 1, first_half, second_half)], axis=-1)
    shuffle_keys = jax.random.split(jax.random.fold_in(key, 15), blocks)
    shuffles = jax.vmap(lambda one: jax.random.permutation(one, TOK_DEV))(shuffle_keys).astype(jnp.int32)
    paired = jnp.take_along_axis(paired, shuffles[:, :, None], axis=1)
    return paired.reshape(TOKENS, 2).astype(jnp.int32)


def with_spikes(values, stream_key, source, target, parts, factor):
    def block_of(dim):
        return (jnp.arange(values.shape[dim]) // (values.shape[dim] // parts)).reshape((-1,) + (1,) * (values.ndim - 1 - dim))

    near = jax.random.permutation(stream_key, parts)[block_of(target)]
    other_side = (block_of(target) + parts // 2) % parts
    return jnp.where((block_of(source) == near) | (block_of(source) == other_side), factor * values, values)


def steps_of(key, extent, shards, low, top_value):
    factor_of, own = 1.0, jax.random.fold_in(key, 6)
    for dim, shards_of in shards:
        draws = jnp.exp(jax.random.uniform(jax.random.fold_in(own, dim), (shards_of,), jnp.float32, low / len(shards), top_value / len(shards)))
        factor_of = factor_of * jnp.repeat(draws, extent[dim] // shards_of).reshape([-1 if axis == dim else 1 for axis in range(len(extent))])
    return factor_of


def noise(rng, shape, scale, most, cuts=(), kind=jnp.bfloat16):
    result = jax.random.normal(rng, shape, jnp.float32) * scale
    if len(cuts) > 0:
        result = steps_of(rng, shape, cuts, -0.22, 0.18) * result
    return jnp.clip(result, min=-most, max=most).astype(kind)


def heavy_noise(key, extent, scale, most, cuts, heavy, kind=jnp.bfloat16):
    result = scale * jax.random.normal(key, extent, jnp.float32)
    if cuts:
        result = result * steps_of(key, extent, cuts, -0.22, 0.18)
    return jnp.clip(with_spikes(result, jax.random.fold_in(key, 3), *heavy), -most, most).astype(kind)


def setup_inputs(seed: int = 0) -> dict:
    splits = jax.random.split(jax.random.key(seed), 8)
    tokens = noise(splits[0], (TOKENS, D), 1.0, 6.0, ((0, 32),))
    out_grad = heavy_noise(splits[1], (TOKENS, D), 1.0, 6.0, ((0, 32),), (0, 1, 32, 2.75))
    expert_ids = draw_expert_ids(jax.random.fold_in(splits[7], 71), 0)
    gate_probs = jnp.clip(0.049804688 + 0.89941406 * jax.random.uniform(splits[3], (TOKENS, 2), jnp.float32) ** steps_of(splits[3], (TOKENS, 2), ((0, 32),), -0.2, 0.2), 0.049804688, 0.94921875).astype(jnp.bfloat16)
    params = noise(splits[4], (3, EXPERTS, D, F), (D // 4) ** -0.5, 0.1875, ((1, 2), (2, 16)), jnp.float32)
    moment_first = noise(splits[5], (3, EXPERTS, D, F), 10.0, 60.0, ((1, 2), (2, 16)), jnp.float32)
    moment_second = jnp.clip(jnp.exp(math.log(1024.0) - 2.7725887 * jax.random.uniform(splits[6], (3, EXPERTS, D, F), jnp.float32) ** steps_of(splits[6], (3, EXPERTS, D, F), ((1, 2), (2, 16)), -0.2, 0.2)), 64.0, 1024.0)
    return dict(tokens=tokens, out_grad=out_grad, expert_ids=expert_ids, gate_probs=gate_probs, params=params, moment_first=moment_first, moment_second=moment_second)


decay_first = 0.9
decay_second = 0.95
correct_first = 1.0 - 0.9 ** 10
correct_second = 1.0 - 0.95 ** 10
epsilon = 1e-08
learn_rate = 0.0003
weight_decay = 0.1

def adam_update(params, gradient, moment_first, moment_second):
    new_first = decay_first * moment_first + (1.0 - decay_first) * gradient
    new_second = decay_second * moment_second + (1.0 - decay_second) * gradient * gradient
    stepped = new_first / correct_first / (jnp.sqrt(new_second / correct_second) + epsilon)
    new_params = params - learn_rate * (stepped + weight_decay * params)
    return (new_params, new_first, new_second)

def reference(tokens, out_grad, expert_ids, gate_probs, params, moment_first, moment_second):
    weights = params.astype(jnp.bfloat16)
    token_count = tokens.shape[0]
    slots_most = CAP * (TOKENS // TOK_DEV)
    flat_ids = expert_ids.reshape(-1)
    flat_gate = gate_probs.reshape(-1)

    def expert_step(totals, expert):
        token_acc, gate_acc = totals
        chosen = flat_ids == expert
        picked = jnp.nonzero(chosen, size=slots_most, fill_value=0)[0].astype(jnp.int32)
        filled = jnp.arange(slots_most, dtype=jnp.int32) < jnp.sum(chosen.astype(jnp.int32))
        token_rows = picked // 2
        inputs = tokens[token_rows]
        upstream = out_grad[token_rows]
        gate_values = jnp.where(filled, flat_gate[picked], jnp.zeros((), flat_gate.dtype)).astype(jnp.float32)[:, None]
        w_gate = weights[0, expert]
        w_up = weights[1, expert]
        w_down = weights[2, expert]
        pre_gate = jnp.dot(inputs, w_gate, preferred_element_type=jnp.float32)
        pre_up = jnp.dot(inputs, w_up, preferred_element_type=jnp.float32)
        sigmoid_gate = jax.nn.sigmoid(pre_gate)
        activated = pre_gate * sigmoid_gate
        hidden = activated * pre_up
        projected = jnp.dot(upstream, w_down, preferred_element_type=jnp.float32)
        slot_gate = lax.optimization_barrier(jnp.sum(hidden * projected, axis=1)).astype(jnp.bfloat16)
        delta_hidden = gate_values * projected
        delta_gate = (delta_hidden * pre_up * sigmoid_gate * (1.0 + pre_gate * (1.0 - sigmoid_gate))).astype(jnp.bfloat16)
        delta_up = (delta_hidden * activated).astype(jnp.bfloat16)
        scaled = (gate_values * upstream.astype(jnp.float32)).astype(jnp.bfloat16)
        slot_grads = (jnp.dot(delta_gate, w_gate.T, preferred_element_type=jnp.float32) + jnp.dot(delta_up, w_up.T, preferred_element_type=jnp.float32)).astype(jnp.bfloat16)
        grad_gate = jnp.dot(inputs.T, delta_gate, preferred_element_type=jnp.float32)
        grad_up = jnp.dot(inputs.T, delta_up, preferred_element_type=jnp.float32)
        grad_down = jnp.dot(scaled.T, hidden.astype(jnp.bfloat16), preferred_element_type=jnp.float32)
        token_acc = token_acc.at[token_rows].add(jnp.where(filled[:, None], slot_grads.astype(jnp.float32), jnp.zeros((), jnp.float32)))
        gate_acc = gate_acc.at[picked].add(jnp.where(filled, slot_gate.astype(jnp.float32), jnp.zeros((), jnp.float32)))
        return ((token_acc, gate_acc), jnp.stack([grad_gate, grad_up, grad_down]))
    start = (jnp.zeros(tokens.shape, jnp.float32), jnp.zeros((token_count * 2,), jnp.float32))
    (token_acc, gate_acc), gradient = lax.scan(expert_step, start, jnp.arange(EXPERTS, dtype=jnp.int32))
    gradient = jnp.transpose(gradient, (1, 0, 2, 3))
    new_params, new_first, new_second = adam_update(params, gradient, moment_first, moment_second)
    return (token_acc.astype(jnp.bfloat16), gate_acc.reshape(token_count, 2).astype(jnp.bfloat16), new_params, new_first, new_second)
```

```python
import functools

import jax
import jax.numpy as jnp
from jax import lax
from jax.experimental import pallas as pl
from jax.experimental.pallas import tpu as pltpu
from jax.sharding import PartitionSpec as P

EXPERTS = 8
CORES = 2
MESH = pl.DeviceIdType.MESH

decay_first = 0.9
decay_second = 0.95
correct_first = 1.0 - 0.9**10
correct_second = 1.0 - 0.95**10
epsilon = 1e-08
learn_rate = 0.0003
weight_decay = 0.1


def adam_update(params, gradient, moment_first, moment_second):
    new_first = decay_first * moment_first + (1.0 - decay_first) * gradient
    new_second = decay_second * moment_second + (1.0 - decay_second) * gradient * gradient
    stepped = new_first / correct_first / (jnp.sqrt(new_second / correct_second) + epsilon)
    new_params = params - learn_rate * (stepped + weight_decay * params)
    return (new_params, new_first, new_second)


def loop(count, body):
    def step(i, carry):
        body(i)
        return carry

    lax.fori_loop(0, count, step, 0)


def dot(a, b, dims):
    return lax.dot_general(a, b, (dims, ((), ())), preferred_element_type=jnp.float32)


def kernel(
    sizes,
    info_ref, tok_ref, og_ref, w_ref,
    tg_ref, gg_ref, grad_ref,
    info, weights, tokb, ogb, place, inp, ups, pre_s, prj_s, pre_r, prj_r, own, dl, sg, ret_r, tg_s,
    gg_s, gg_r, g1_out, g1_in, g2_out, g2_in,
    si, ri, sz, rz, sy, ry, sw, rw, sv, rv, sp, rp, sa, ra, st, rt, so, ro, sg_sem, rg_sem, s1, r1, s2, r2,
    local_sem,
):
    nk, ne, nf, local, cap, tcount, rows, units = sizes
    chips = nk // CORES
    span = ne * cap
    slots = local * span
    depth = nk * rows
    bf = jnp.bfloat16
    f32 = jnp.float32
    k, e, f = lax.axis_index("cuts"), lax.axis_index("exp"), lax.axis_index("fsdp")
    x, c = k // CORES, lax.rem(k, CORES)

    def f_at(d):
        return lax.rem(f + d, nf)

    def e_at(d):
        return lax.rem(e + d, ne)

    def x_at(d):
        return lax.rem(x + d, chips)

    partner = x * CORES + 1 - c

    def put(src, dst, send, recv, device):
        return pltpu.make_async_remote_copy(
            src_ref=src, dst_ref=dst, send_sem=send, recv_sem=recv, device_id=device, device_id_type=MESH
        )

    def strip(kk, ff):
        return pl.ds(pl.multiple_of((kk * nf + ff) * rows, rows), rows)

    def cut(kk):
        return pl.ds(pl.multiple_of(kk * rows, rows), rows)

    def mine(ee):
        return pl.ds(pl.multiple_of(ee * tcount, tcount), tcount)

    def group(g):
        return pl.ds(pl.multiple_of(g * span, span), span)

    barrier = pltpu.get_barrier_semaphore()
    partners = 0
    for de in range(ne):
        for d in range(nf):
            if de or d:
                pl.semaphore_signal(barrier, inc=1, device_id=(k, e_at(de), f_at(d)), device_id_type=MESH)
                partners += 1
    pl.semaphore_signal(barrier, inc=1, device_id=(partner, e, f), device_id_type=MESH)
    partners += 1
    for dx in range(1, chips):
        pl.semaphore_signal(barrier, inc=1, device_id=(x_at(dx) * CORES + c, e, f), device_id_type=MESH)
        partners += 1
    pl.semaphore_wait(barrier, partners)

    def info_copy(de, d):
        return put(info_ref, info.at[f, e], si.at[de, d], ri.at[de, d], (k, e_at(de), f_at(d)))

    for de in range(ne):
        for d in range(nf):
            if de or d:
                info_copy(de, d).start()

    arrays = ((tok_ref, tokb), (og_ref, ogb))
    order = sorted(range(1, nf), key=lambda d: -min(d, nf - d))
    for a, (src, dst) in enumerate(arrays):
        for d in order:
            ff = f_at(d)
            for kk in range(nk):
                put(
                    src.at[:, strip(kk, ff)], dst.at[f, mine(e), cut(kk)], sz.at[a, d], rz.at[a, d], (k, e, ff)
                ).start()
        for de in range(1, ne):
            for kk in range(nk):
                put(
                    src.at[:, strip(kk, f)], dst.at[f, mine(e), cut(kk)], sy.at[a, f, de], ry.at[a, f, de],
                    (k, e_at(de), f),
                ).start()
        if a == 0:
            for dx in range(1, chips):
                put(
                    w_ref, weights.at[:, cut(k), :], sw.at[dx], rw.at[dx], (x_at(dx) * CORES + c, e, f)
                ).start()
            put(w_ref, weights.at[:, cut(k), :], sv.at[0], rv.at[0], (partner, e, f)).start()

    info[f, e] = info_ref[...]
    for src, dst in arrays:
        for kk in range(nk):
            dst[f, mine(e), cut(kk)] = src[:, strip(kk, f)]
    weights[:, cut(k), :] = w_ref[...]

    def whole(a, dst, g, ee, send, recv, device):
        return put(dst.at[g, mine(ee), :], dst.at[g, mine(ee), :], send, recv, device)

    for a, (src, dst) in enumerate(arrays):
        for d in order:
            g = f_at(nf - d)
            whole(a, dst, g, e, sz.at[a, d], rz.at[a, d], (k, e, f_at(d))).wait_recv()
            for de in range(1, ne):
                whole(a, dst, g, e, sy.at[a, g, de], ry.at[a, g, de], (k, e_at(de), f)).start()
        if a == 0:
            for de in range(ne):
                for d in range(nf):
                    if de or d:
                        info_copy(de, d).wait_recv()

    for dx in range(1, chips):
        held = weights.at[:, cut(x_at(chips - dx) * CORES + c), :]
        put(w_ref, held, sw.at[dx], rw.at[dx], (x_at(dx) * CORES + c, e, f)).wait_recv()
        put(held, held, sv.at[dx], rv.at[dx], (partner, e, f)).start()
    for dx in range(chips):
        held = weights.at[:, cut(x_at(chips - dx) * CORES + 1 - c), :]
        put(held, held, sv.at[dx], rv.at[dx], (partner, e, f)).wait_recv()

    def codes(g, row):
        return jnp.concatenate([info[g, ee, row : row + 1, :] for ee in range(ne)], axis=1)

    first_slot = (e * slots).astype(f32)

    def choose(g, base, count):
        ids = lax.broadcasted_iota(jnp.int32, (count, ne * tcount), 0).astype(f32) + base
        return [codes(g, j) - first_slot == ids for j in range(2)]

    def picked(a, src, dst, g):
        for de in range(1, ne):
            ee = e_at(ne - de)
            whole(a, src, g, ee, sy.at[a, g, de], ry.at[a, g, de], (k, e_at(de), f)).wait_recv()

        def column(kk):
            out = dot(place[g], src[g, :, cut(kk)], ((1,), (0,))).astype(bf)
            for l in range(local):
                dst[l, group(g), cut(kk)] = out[l * span : (l + 1) * span]

        loop(nk, column)

    def rs_copy(a, d):
        sent, got = ((pre_s, pre_r), (prj_s, prj_r))[a]
        g = f_at(d)
        return put(sent.at[g], got.at[d], sp.at[a, d], rp.at[a, d], (k, e, g))

    def forward(i):
        d = lax.rem(i + 1, nf)
        g = f_at(d)
        zero, one = choose(g, 0.0, slots)
        place[g] = jnp.where(zero, 1.0, 0.0).astype(bf) + jnp.where(one, 1.0, 0.0).astype(bf)
        picked(0, tokb, inp, g)

        def expert(l):
            out = dot(inp[l, group(g), :], weights[l, :, : 2 * units], ((1,), (0,)))
            own[pl.ds(pl.multiple_of(l * span, span), span), : 2 * units] = out
            pre_s[g, pl.ds(pl.multiple_of(l * span, span), span), :] = out.astype(bf)

        loop(local, expert)

        @pl.when(d > 0)
        def _():
            rs_copy(0, d).start()

    loop(nf, forward)

    def backward(i):
        d = lax.rem(i + 1, nf)
        g = f_at(d)
        picked(1, ogb, ups, g)

        def expert(l):
            out = dot(ups[l, group(g), :], weights[l, :, 2 * units :], ((1,), (0,)))
            own[pl.ds(pl.multiple_of(l * span, span), span), 2 * units :] = out
            prj_s[g, pl.ds(pl.multiple_of(l * span, span), span), :] = out.astype(bf)

        loop(local, expert)

        @pl.when(d > 0)
        def _():
            rs_copy(1, d).start()

    loop(nf, backward)

    for a in range(2):
        for d in range(1, nf):
            rs_copy(a, d).wait_recv()

    def middle(l, carry):
        here = pl.ds(pl.multiple_of(l * span, span), span)
        gate = own[here, :units]
        up = own[here, units : 2 * units]
        proj = own[here, 2 * units :]
        for d in range(1, nf):
            gate += pre_r[d, here, :units].astype(f32)
            up += pre_r[d, here, units:].astype(f32)
            proj += prj_r[d, here, :].astype(f32)
        zero, one = choose(f, (l * span).astype(f32), span)
        scale = jnp.sum(
            jnp.where(zero, codes(f, 2), 0.0) + jnp.where(one, codes(f, 3), 0.0), axis=1, keepdims=True
        )
        sig = jax.nn.sigmoid(gate)
        act = gate * sig
        hidden = act * up
        slot_gate = jnp.sum(hidden * proj, axis=1, keepdims=True)
        delta = scale * proj
        dl[l, group(f), :units] = (delta * up * sig * (1.0 + gate * (1.0 - sig))).astype(bf)
        dl[l, group(f), units : 2 * units] = (delta * act).astype(bf)
        dl[l, group(f), 2 * units :] = (scale * hidden).astype(bf)
        return (
            carry[0] + jnp.sum(jnp.where(zero, slot_gate, 0.0), axis=0, keepdims=True),
            carry[1] + jnp.sum(jnp.where(one, slot_gate, 0.0), axis=0, keepdims=True),
        )

    nothing = jnp.zeros((1, ne * tcount), f32)
    parts = lax.fori_loop(0, local, middle, (nothing, nothing))

    def ag_copy(d):
        held = dl.at[:, group(f), :]
        return put(held, held, sa.at[d], ra.at[d], (k, e, f_at(d)))

    for d in order:
        ag_copy(d).start()

    for ee in range(ne):
        for j in range(2):
            gg_s[ee, j : j + 1, :] = parts[j][:, ee * tcount : (ee + 1) * tcount]

    def gg_copy(de):
        return put(gg_s.at[e_at(de)], gg_r.at[de], sg_sem.at[de], rg_sem.at[de], (k, e_at(de), f))

    for de in range(1, ne):
        gg_copy(de).start()

    for de in range(1, ne):
        for g in range(nf):
            whole(0, tokb, g, e, sy.at[0, g, de], ry.at[0, g, de], (k, e_at(de), f)).wait_send()

    def ret_copy(g, de):
        ee = e_at(de)
        return put(tokb.at[g, mine(ee), :], ret_r.at[g, de], st.at[g, de], rt.at[g, de], (k, ee, f))

    def returned(d):
        g = f_at(nf - d)

        @pl.when(d > 0)
        def _():
            held = dl.at[:, group(g), :]
            put(held, held, sa.at[d], ra.at[d], (k, e, f_at(d))).wait_recv()

        def column(kk):
            for l in range(local):
                sg[l * span : (l + 1) * span, :] = dot(
                    dl[l, group(g), : 2 * units], weights[l, cut(kk), : 2 * units], ((1,), (1,))
                ).astype(bf)
            tokb[g, :, cut(kk)] = dot(place[g], sg[...], ((0,), (0,))).astype(bf)

        loop(nk, column)
        for de in range(1, ne):
            ret_copy(g, de).start()

    loop(nf, returned)

    def gradient(kk, l):
        ahead = dot(inp[l, :, cut(kk)], dl[l, :, : 2 * units], ((0,), (0,)))
        down = dot(ups[l, :, cut(kk)], dl[l, :, 2 * units :], ((0,), (0,)))
        return ahead, down

    def g1_copy(dx, l):
        return put(g1_out.at[dx, l], g1_in.at[dx, l], s1.at[dx, l], r1.at[dx, l], (partner, e, f))

    def g2_copy(dx, l):
        return put(
            g2_out.at[dx, l], g2_in.at[dx, l], s2.at[dx, l], r2.at[dx, l], (x_at(dx) * CORES + c, e, f)
        )

    for dx in [*range(1, chips), 0]:

        def share(l):
            ahead, down = gradient(x_at(dx) * CORES + 1 - c, l)
            g1_out[dx, l, :, : 2 * units] = ahead.astype(bf)
            g1_out[dx, l, :, 2 * units :] = down.astype(bf)
            g1_copy(dx, l).start()
            ahead, down = gradient(x_at(dx) * CORES + c, l)
            g1_copy(dx, l).wait_recv()
            ahead += g1_in[dx, l, :, : 2 * units].astype(f32)
            down += g1_in[dx, l, :, 2 * units :].astype(f32)
            if dx:
                g2_out[dx, l, :, : 2 * units] = ahead.astype(bf)
                g2_out[dx, l, :, 2 * units :] = down.astype(bf)
                g2_copy(dx, l).start()
            else:
                grad_ref[0, l] = ahead[:, :units]
                grad_ref[1, l] = ahead[:, units:]
                grad_ref[2, l] = down

        loop(local, share)

    def tg_wait(d):
        return put(tg_s.at[0], tg_s.at[0], so.at[d], ro.at[d], (k, e, f_at(d)))

    def final(d):
        g = f_at(nf - d)
        total = tokb[g, mine(e), :].astype(f32)
        for de in range(1, ne):
            put(ret_r.at[g, de], ret_r.at[g, de], st.at[g, de], rt.at[g, de], (k, e_at(de), f)).wait_recv()
            total += ret_r[g, de].astype(f32)
        tg_s[g] = total.astype(bf)
        for kk in range(nk):
            there = tg_ref.at[:, strip(kk, f)]

            @pl.when(d > 0)
            def _():
                put(
                    tg_s.at[g, :, cut(kk)], there, so.at[nf - d], ro.at[nf - d], (k, e, g)
                ).start()

            @pl.when(d == 0)
            def _():
                pltpu.make_async_copy(tg_s.at[g, :, cut(kk)], there, local_sem).start()

    loop(nf, final)

    total = [gg_s[e, j : j + 1, :] for j in range(2)]
    for de in range(1, ne):
        gg_copy(de).wait_recv()
        for j in range(2):
            total[j] += gg_r[de, j : j + 1, :]
    for j in range(2):
        gg_ref[j : j + 1, :] = total[j]

    def collect(l):
        for dx in range(1, chips):
            g2_copy(dx, l).wait_recv()
            got = g2_in[dx, l].astype(f32)
            for part in range(3):
                grad_ref[part, l] += got[:, part * units : (part + 1) * units]

    loop(local, collect)

    for d in range(1, nf):
        tg_wait(d).wait()
    pltpu.make_async_copy(tg_s.at[0], tg_s.at[0], local_sem).wait()

    for de in range(ne):
        for d in range(nf):
            if de or d:
                info_copy(de, d).wait_send()
    for d in range(1, nf):
        for a, (src, dst) in enumerate(arrays):
            whole(a, dst, f, e, sz.at[a, d], rz.at[a, d], (k, e, f_at(d))).wait_send()
            rs_copy(a, d).wait_send()
        ag_copy(d).wait_send()
    for de in range(1, ne):
        gg_copy(de).wait_send()
        for g in range(nf):
            whole(1, ogb, g, e, sy.at[1, g, de], ry.at[1, g, de], (k, e_at(de), f)).wait_send()
            ret_copy(g, de).wait_send()
    for dx in range(chips):
        put(w_ref, w_ref, sv.at[dx], rv.at[dx], (partner, e, f)).wait_send()
        if dx:
            put(w_ref, w_ref, sw.at[dx], rw.at[dx], (partner, e, f)).wait_send()

        def sent(l):
            g1_copy(dx, l).wait_send()
            if dx:
                g2_copy(dx, l).wait_send()

        loop(local, sent)


def per_device(mesh_shape, tokens, out_grad, expert_ids, gate_probs, params, moment_first, moment_second):
    nk, ne, nf = mesh_shape["cuts"], mesh_shape["exp"], mesh_shape["fsdp"]
    token_count, width = tokens.shape
    local, rows, units = params.shape[1:]
    cap = 10 * token_count // 32
    chips = nk // CORES
    span = ne * cap
    slots = local * span
    depth = nk * rows
    bf, f32 = jnp.bfloat16, jnp.float32

    weights = params.astype(bf)
    w_block = jnp.concatenate([weights[0], weights[1], weights[2]], axis=2)

    flat_ids = expert_ids.reshape(-1)
    onehot = (flat_ids[:, None] == jnp.arange(EXPERTS, dtype=jnp.int32)).astype(jnp.int32)
    before = jnp.cumsum(onehot, axis=0) - onehot
    position = jnp.sum(before * onehot, axis=1)
    code = flat_ids * span + lax.axis_index("exp") * cap + position
    info = jnp.concatenate(
        [
            code.reshape(token_count, 2).T.astype(f32),
            gate_probs.T.astype(f32),
            jnp.zeros((4, token_count), f32),
        ]
    )

    sizes = (nk, ne, nf, local, cap, token_count, rows, units)
    vm = lambda shape, kind=bf: pltpu.VMEM(shape, kind)
    sem = lambda *shape: pltpu.SemaphoreType.DMA(shape)
    scratch = [
        vm((nf, ne, 8, token_count), f32),
        vm((local, depth, 3 * units)),
        vm((nf, ne * token_count, depth)),
        vm((nf, ne * token_count, depth)),
        vm((nf, slots, ne * token_count)),
        vm((local, nf * span, depth)),
        vm((local, nf * span, depth)),
        vm((nf, slots, 2 * units)),
        vm((nf, slots, units)),
        vm((nf, slots, 2 * units)),
        vm((nf, slots, units)),
        vm((slots, 3 * units), f32),
        vm((local, nf * span, 3 * units)),
        vm((slots, rows)),
        vm((nf, ne, token_count, depth)),
        vm((nf, token_count, depth)),
        vm((ne, 8, token_count), f32),
        vm((ne, 8, token_count), f32),
        vm((chips, local, rows, 3 * units)),
        vm((chips, local, rows, 3 * units)),
        vm((chips, local, rows, 3 * units)),
        vm((chips, local, rows, 3 * units)),
        sem(ne, nf), sem(ne, nf),
        sem(2, nf), sem(2, nf),
        sem(2, nf, ne), sem(2, nf, ne),
        sem(chips), sem(chips),
        sem(chips), sem(chips),
        sem(2, nf), sem(2, nf),
        sem(nf), sem(nf),
        sem(nf, ne), sem(nf, ne),
        sem(nf), sem(nf),
        sem(ne), sem(ne),
        sem(chips, local), sem(chips, local),
        sem(chips, local), sem(chips, local),
        pltpu.SemaphoreType.DMA,
    ]
    vmem = pl.BlockSpec(memory_space=pltpu.VMEM)
    token_grad, gates, gradient = pl.pallas_call(
        functools.partial(kernel, sizes),
        out_shape=(
            jax.ShapeDtypeStruct((token_count, width), bf),
            jax.ShapeDtypeStruct((8, token_count), f32),
            jax.ShapeDtypeStruct((3, local, rows, units), f32),
        ),
        in_specs=[vmem] * 4,
        out_specs=(pl.BlockSpec(memory_space=pl.ANY), vmem, vmem),
        scratch_shapes=scratch,
        compiler_params=pltpu.CompilerParams(
            collective_id=0, has_side_effects=True, vmem_limit_bytes=67043328
        ),
    )(info, tokens, out_grad, w_block)
    gate_grad = gates[:2].T.astype(bf)
    new_params, new_first, new_second = adam_update(params, gradient, moment_first, moment_second)
    return (token_grad, gate_grad, new_params, new_first, new_second)


def solution(mesh):
    tokens_spec = P(("cuts", "exp", "fsdp"), None)
    weights_spec = P(None, "exp", ("cuts", "fsdp"), None)
    return jax.shard_map(
        functools.partial(per_device, dict(mesh.shape)),
        mesh=mesh,
        in_specs=(tokens_spec,) * 4 + (weights_spec,) * 3,
        out_specs=(tokens_spec,) * 2 + (weights_spec,) * 3,
        check_vma=False,
    )
```

```python
import functools

import jax
import jax.numpy as jnp
from jax import lax
from jax.experimental import pallas as pl
from jax.experimental.pallas import tpu as pltpu
from jax.sharding import PartitionSpec as P

CORES = 2
MESH = pl.DeviceIdType.MESH

decay_first = 0.9
decay_second = 0.95
correct_first = 1.0 - 0.9**10
correct_second = 1.0 - 0.95**10
epsilon = 1e-08
learn_rate = 0.0003
weight_decay = 0.1


def adam_update(params, gradient, moment_first, moment_second):
    new_first = decay_first * moment_first + (1.0 - decay_first) * gradient
    new_second = decay_second * moment_second + (1.0 - decay_second) * gradient * gradient
    stepped = new_first / correct_first / (jnp.sqrt(new_second / correct_second) + epsilon)
    new_params = params - learn_rate * (stepped + weight_decay * params)
    return (new_params, new_first, new_second)


def loop(count, body):
    def step(i, carry):
        body(i)
        return carry

    lax.fori_loop(0, count, step, 0)


def dot(a, b, dims):
    return lax.dot_general(a, b, (dims, ((), ())), preferred_element_type=jnp.float32)


def kernel(
    sizes,
    ids_ref, gates_ref, tok_hbm, og_hbm, params_hbm,
    tg_ref, gg_ref, grad_ref,
    tok_ref, og_ref, par_ref, info, weights, tokb, ogb, place, inp, ups, pre_s, prj_s, pre_r, prj_r, own, dl, sg,
    ret_r, tg_s, gg_s, gg_r, g1_out, g1_in, g2_out, g2_in,
    si, ri, sz, rz, sy, ry, sw, rw, sv, rv, sp, rp, sa, ra, st, rt, so, ro, sg_sem, rg_sem, s1, r1, s2, r2,
    own_sems,
):
    nk, ne, nf, local, cap, tcount, rows, units = sizes
    chips = nk // CORES
    span = ne * cap
    slots = local * span
    halves = 2 if local % 2 == 0 else 1
    part = local // halves
    bf = jnp.bfloat16
    f32 = jnp.float32
    k, e, f = lax.axis_index("cuts"), lax.axis_index("exp"), lax.axis_index("fsdp")
    x, c = k // CORES, lax.rem(k, CORES)
    scope = jax.named_scope

    def f_at(d):
        return lax.rem(f + d, nf)

    def e_at(d):
        return lax.rem(e + d, ne)

    def chip_at(d, core):
        return lax.rem(x + d, chips) * CORES + core

    partner = x * CORES + 1 - c

    def put(src, dst, send, recv, device):
        return pltpu.make_async_remote_copy(
            src_ref=src, dst_ref=dst, send_sem=send, recv_sem=recv, device_id=device, device_id_type=MESH
        )

    def strip(kk, ff):
        return pl.ds(pl.multiple_of((kk * nf + ff) * rows, rows), rows)

    def cut(kk):
        return pl.ds(pl.multiple_of(kk * rows, rows), rows)

    def mine(ee):
        return pl.ds(pl.multiple_of(ee * tcount, tcount), tcount)

    def group(g):
        return pl.ds(pl.multiple_of(g * span, span), span)

    barrier = pltpu.get_barrier_semaphore()
    partners = 0
    for de in range(ne):
        for d in range(nf):
            if de or d:
                pl.semaphore_signal(barrier, inc=1, device_id=(k, e_at(de), f_at(d)), device_id_type=MESH)
                partners += 1
    pl.semaphore_signal(barrier, inc=1, device_id=(partner, e, f), device_id_type=MESH)
    partners += 1
    for dx in range(1, chips):
        pl.semaphore_signal(barrier, inc=1, device_id=(chip_at(dx, c), e, f), device_id_type=MESH)
        partners += 1

    staged = ((tok_hbm, tok_ref), (og_hbm, og_ref), (params_hbm, par_ref))
    for n, (src, dst) in enumerate(staged):
        pltpu.make_async_copy(src, dst, own_sems.at[n]).start()

    def iota(shape, dim):
        return lax.broadcasted_iota(jnp.int32, shape, dim)

    experts = iota((local * ne, tcount), 0)
    named = [jnp.where(experts == ids_ref[j : j + 1, :], 1.0, 0.0).astype(f32) for j in range(2)]
    earlier = jnp.where(iota((tcount, tcount), 0) < iota((tcount, tcount), 1), 1.0, 0.0).astype(bf)
    before = dot((named[0] + named[1]).astype(bf), earlier, ((1,), (0,)))
    info[f, e] = jnp.zeros((8, tcount), f32)
    for j in range(2):
        position = jnp.sum(named[j] * before, axis=0, keepdims=True)
        info[f, e, j : j + 1, :] = (ids_ref[j : j + 1, :] * span + e * cap).astype(f32) + position
        info[f, e, j + 2 : j + 3, :] = gates_ref[j : j + 1, :].astype(f32)

    pltpu.make_async_copy(params_hbm, par_ref, own_sems.at[2]).wait()
    for l in range(local):
        for n in range(3):
            weights[l, cut(k), n * units : (n + 1) * units] = par_ref[n, l].astype(bf)
    for n, (src, dst) in enumerate(staged[:2]):
        pltpu.make_async_copy(src, dst, own_sems.at[n]).wait()
    with scope("barrier"):
        pl.semaphore_wait(barrier, partners)

    def info_copy(de, d):
        mark = info.at[f, e]
        return put(mark, mark, si.at[de, d], ri.at[de, d], (k, e_at(de), f_at(d)))

    order = sorted(range(1, nf), key=lambda d: -min(d, nf - d))
    arrays = ((tok_ref, tokb), (og_ref, ogb))
    wide = (pl.ds(0, 2 * units), pl.ds(2 * units, units))

    def z_start(a, d):
        src, dst = arrays[a]
        for kk in range(nk):
            put(
                src.at[:, strip(kk, f_at(d))], dst.at[f, mine(e), cut(kk)], sz.at[a, d], rz.at[a, d],
                (k, e, f_at(d)),
            ).start()

    def y_own_start(a):
        src, dst = arrays[a]
        for de in range(1, ne):
            for kk in range(nk):
                put(
                    src.at[:, strip(kk, f)], dst.at[f, mine(e), cut(kk)], sy.at[a, f, de], ry.at[a, f, de],
                    (k, e_at(de), f),
                ).start()

    def w_chip(a, dx, owner):
        held = weights.at[:, cut(owner), wide[a]]
        return put(held, held, sw.at[a, dx], rw.at[a, dx], (chip_at(dx, c), e, f))

    def w_core(a, dx, owner):
        held = weights.at[:, cut(owner), wide[a]]
        return put(held, held, sv.at[a, dx], rv.at[a, dx], (partner, e, f))

    def whole(dst, g, ee, send, recv, device):
        return put(dst.at[g, mine(ee), :], dst.at[g, mine(ee), :], send, recv, device)

    def z_whole(a, d):
        return whole(arrays[a][1], f_at(nf - d), e, sz.at[a, d], rz.at[a, d], (k, e, f_at(d)))

    def y_whole(a, g, de, ee):
        return whole(arrays[a][1], g, ee, sy.at[a, g, de], ry.at[a, g, de], (k, e_at(de), f))

    def z_pass(a, d):
        with scope("wait_z"):
            z_whole(a, d).wait_recv()
        for de in range(1, ne):
            y_whole(a, f_at(nf - d), de, e).start()

    for de in range(ne):
        for d in range(nf):
            if de or d:
                info_copy(de, d).start()
    for d in order:
        z_start(0, d)
    y_own_start(0)
    for a in range(2):
        for dx in range(1, chips):
            w_chip(a, dx, k).start()
        w_core(a, 0, k).start()
        if a == 0:
            for d in order:
                z_start(1, d)

    for src, dst in arrays:
        for kk in range(nk):
            dst[f, mine(e), cut(kk)] = src[:, strip(kk, f)]

    for n, d in enumerate(order):
        z_pass(0, d)
        if n == 0:
            y_own_start(1)
    for de in range(ne):
        for d in range(nf):
            if de or d:
                info_copy(de, d).wait_recv()

    def w_pass(a):
        with scope("wait_w"):
            for dx in range(1, chips):
                owner = chip_at(chips - dx, c)
                w_chip(a, dx, owner).wait_recv()
                w_core(a, dx, owner).start()
            for dx in range(chips):
                w_core(a, dx, chip_at(chips - dx, 1 - c)).wait_recv()

    def codes(g, row):
        return jnp.concatenate([info[g, ee, row : row + 1, :] for ee in range(ne)], axis=1)

    first_slot = (e * slots).astype(f32)

    def choose(g, base, count):
        ids = iota((count, ne * tcount), 0).astype(f32) + base
        return [codes(g, j) - first_slot == ids for j in range(2)]

    def at(l):
        return pl.ds(pl.multiple_of(l * span, span), span)

    def picked(a, dst, g):
        src = arrays[a][1]
        for de in range(1, ne):
            with scope("wait_y"):
                y_whole(a, g, de, e_at(ne - de)).wait_recv()

        def column(kk):
            out = dot(place[g], src[g, :, cut(kk)], ((1,), (0,))).astype(bf)
            for l in range(local):
                dst[l, group(g), cut(kk)] = out[l * span : (l + 1) * span]

        loop(nk, column)

    def partial_sum(a, g):
        with scope("partial"):
            if a == 0:
                zero, one = choose(g, 0.0, slots)
                place[g] = jnp.where(zero, 1.0, 0.0).astype(bf) + jnp.where(one, 1.0, 0.0).astype(bf)
            rows_of, sums = ((inp, pre_s), (ups, prj_s))[a]
            picked(a, rows_of, g)

            def expert(l):
                out = dot(rows_of[l, group(g), :], weights[l, :, wide[a]], ((1,), (0,)))
                own[at(l), wide[a]] = out
                sums[g, at(l), :] = out.astype(bf)

            loop(local, expert)

    def rs_copy(a, g, sign):
        sent, got = ((pre_s, pre_r), (prj_s, prj_r))[a]
        spot = jnp.where((sign < 0) & (g == f - 1), nf, g)
        return put(sent.at[g], got.at[spot], sp.at[a, g], rp.at[a, spot], (k, e, f + sign))

    def rs_wait(a, spot):
        got = (pre_r, prj_r)[a]
        put(got.at[spot], got.at[spot], sp.at[a, 0], rp.at[a, spot], (k, e, f_at(1))).wait_recv()

    def rs_step(a, g, sign):
        sent, got = ((pre_s, pre_r), (prj_s, prj_r))[a]
        behind = f - sign

        @pl.when((g - f) * sign > 0)
        def _():
            @pl.when((behind >= 0) & (behind < nf))
            def _():
                with scope("wait_rs"):
                    rs_wait(a, g)

                def add(l):
                    sent[g, at(l), :] = (sent[g, at(l), :].astype(f32) + got[g, at(l), :].astype(f32)).astype(bf)

                loop(local, add)

            rs_copy(a, g, sign).start()

    near = jnp.where(f < nf // 2, 1, -1)

    def rs_chain(a):
        def steps(t):
            for sign in (near, -near):
                rs_step(a, jnp.where(sign > 0, nf - 1 - t, t), sign)

        loop(nf - 1, steps)

    at_edge = (f == 0) | (f == nf - 1)

    w_pass(0)
    for n in range(nf):
        partial_sum(0, f_at(n + 1) if n < nf - 1 else f)
        if n < nf - 1:
            z_pass(1, order[n])

    @pl.when(at_edge)
    def _():
        rs_chain(0)

    w_pass(1)
    for n in range(nf):
        partial_sum(1, f_at(n + 1) if n < nf - 1 else f)

    @pl.when(jnp.logical_not(at_edge))
    def _():
        rs_chain(0)

    rs_chain(1)

    for a, got in enumerate((pre_r, prj_r)):
        for spot, edge in ((f, 0), (nf, nf - 1)):

            @pl.when(f == edge)
            def _():
                got[spot] = jnp.zeros(got.shape[1:], bf)

            @pl.when(f != edge)
            def _():
                with scope("wait_own"):
                    rs_wait(a, spot)

    def middle(l, carry):
        here = at(l)
        gate = own[here, :units] + pre_r[f, here, :units].astype(f32) + pre_r[nf, here, :units].astype(f32)
        up = own[here, units : 2 * units] + pre_r[f, here, units:].astype(f32) + pre_r[nf, here, units:].astype(f32)
        proj = own[here, 2 * units :] + prj_r[f, here, :].astype(f32) + prj_r[nf, here, :].astype(f32)
        zero, one = choose(f, (l * span).astype(f32), span)
        scale = jnp.sum(
            jnp.where(zero, codes(f, 2), 0.0) + jnp.where(one, codes(f, 3), 0.0), axis=1, keepdims=True
        )
        sig = jax.nn.sigmoid(gate)
        act = gate * sig
        hidden = act * up
        slot_gate = jnp.sum(hidden * proj, axis=1, keepdims=True)
        delta = scale * proj
        dl[l, group(f), :units] = (delta * up * sig * (1.0 + gate * (1.0 - sig))).astype(bf)
        dl[l, group(f), units : 2 * units] = (delta * act).astype(bf)
        dl[l, group(f), 2 * units :] = (scale * hidden).astype(bf)
        return (
            carry[0] + jnp.sum(jnp.where(zero, slot_gate, 0.0), axis=0, keepdims=True),
            carry[1] + jnp.sum(jnp.where(one, slot_gate, 0.0), axis=0, keepdims=True),
        )

    def ag_copy(h, g, sign, spot):
        held = dl.at[h * part : (h + 1) * part, group(g), :]
        return put(held, held, sa.at[h, spot], ra.at[h, g], (k, e, f + sign))

    def has(sign):
        return (f + sign >= 0) & (f + sign < nf)

    def ag_own(h):
        for sign, spot in ((1, f), (-1, nf)):

            @pl.when(has(sign))
            def _():
                ag_copy(h, f, sign, spot).start()

    def ag_step(h, t, sign):
        g = f - sign * t

        @pl.when((g >= 0) & (g < nf))
        def _():
            with scope("wait_ag"):
                ag_copy(h, g, sign, g).wait_recv()

            @pl.when(has(sign))
            def _():
                ag_copy(h, g, sign, g).start()

    nothing = jnp.zeros((1, ne * tcount), f32)
    parts = (nothing, nothing)
    for h in range(halves):
        with scope("middle"):
            parts = lax.fori_loop(h * part, (h + 1) * part, middle, parts)
        ag_own(h)

    for ee in range(ne):
        for j in range(2):
            gg_s[ee, j : j + 1, :] = parts[j][:, ee * tcount : (ee + 1) * tcount]

    def gg_copy(de):
        return put(gg_s.at[e_at(de)], gg_r.at[de], sg_sem.at[de], rg_sem.at[de], (k, e_at(de), f))

    for de in range(1, ne):
        gg_copy(de).start()

    for de in range(1, ne):
        for g in range(nf):
            y_whole(0, g, de, e).wait_send()

    def ret_copy(g, de):
        return put(
            tokb.at[g, mine(e_at(de)), :], ret_r.at[g, de], st.at[g, de], rt.at[g, de], (k, e_at(de), f)
        )

    def returned(g):
        with scope("returned"):

            def column(kk):
                for l in range(local):
                    sg[l * span : (l + 1) * span, :] = dot(
                        dl[l, group(g), : 2 * units], weights[l, cut(kk), : 2 * units], ((1,), (1,))
                    ).astype(bf)
                tokb[g, :, cut(kk)] = dot(place[g], sg[...], ((0,), (0,))).astype(bf)

            loop(nk, column)
        for de in range(1, ne):
            ret_copy(g, de).start()

    def final(g):
        with scope("final"):
            total = tokb[g, mine(e), :].astype(f32)
            for de in range(1, ne):
                with scope("wait_ret"):
                    put(ret_r.at[g, de], ret_r.at[g, de], st.at[g, de], rt.at[g, de], (k, e_at(de), f)).wait_recv()
                total += ret_r[g, de].astype(f32)
            tg_s[g] = total.astype(bf)
            d = lax.rem(g - f + nf, nf)
            for kk in range(nk):
                there = tg_ref.at[:, strip(kk, f)]

                @pl.when(d > 0)
                def _():
                    put(tg_s.at[g, :, cut(kk)], there, so.at[d], ro.at[d], (k, e, g)).start()

                @pl.when(d == 0)
                def _():
                    pltpu.make_async_copy(tg_s.at[g, :, cut(kk)], there, own_sems.at[3]).start()

    def both(t, work):
        def side(n):
            g = f - (1 - 2 * n) * t

            @pl.when((g >= 0) & (g < nf))
            def _():
                work(g)

        loop(2, side)

    def gradient(kk, l):
        ahead = dot(inp[l, :, cut(kk)], dl[l, :, : 2 * units], ((0,), (0,)))
        down = dot(ups[l, :, cut(kk)], dl[l, :, 2 * units :], ((0,), (0,)))
        return ahead, down

    def g1_copy(dx, l):
        return put(g1_out.at[dx, l], g1_in.at[dx, l], s1.at[dx, l], r1.at[dx, l], (partner, e, f))

    def g2_copy(dx, l):
        return put(g2_out.at[dx, l], g2_in.at[dx, l], s2.at[dx, l], r2.at[dx, l], (chip_at(dx, c), e, f))

    def to_core(h):
        def one(n):
            l = h * part + n
            for dx in [*range(1, chips), 0]:
                ahead, down = gradient(chip_at(dx, 1 - c), l)
                g1_out[dx, l, :, : 2 * units] = ahead.astype(bf)
                g1_out[dx, l, :, 2 * units :] = down.astype(bf)
                g1_copy(dx, l).start()

        with scope("to_core"):
            loop(part, one)

    def summed(dx, l):
        ahead, down = gradient(chip_at(dx, c), l)
        with scope("wait_g1"):
            g1_copy(dx, l).wait_recv()
        ahead += g1_in[dx, l, :, : 2 * units].astype(f32)
        down += g1_in[dx, l, :, 2 * units :].astype(f32)
        return ahead, down

    def to_chip(h):
        def one(n):
            l = h * part + n
            for dx in range(1, chips):
                ahead, down = summed(dx, l)
                g2_out[dx, l, :, : 2 * units] = ahead.astype(bf)
                g2_out[dx, l, :, 2 * units :] = down.astype(bf)
                g2_copy(dx, l).start()

        with scope("to_chip"):
            loop(part, one)

    def keep(l):
        ahead, down = summed(0, l)
        grad_ref[0, l] = ahead[:, :units]
        grad_ref[1, l] = ahead[:, units:]
        grad_ref[2, l] = down

    returned(f)
    for h in range(halves - 1):
        for t in range(1, nf):
            for sign in (1, -1):
                ag_step(h, t, sign)
        to_core(h)
    last = halves - 1
    for t in range(1, nf):
        for sign in (1, -1):
            ag_step(last, t, sign)
        if t == 1:
            for h in range(halves - 1):
                to_chip(h)
        if t == nf - 1:
            to_core(last)
            to_chip(last)
        both(t, returned)
        if t == 1:
            final(f)
        else:
            both(t - 1, final)
    both(nf - 1, final)
    with scope("keep"):
        loop(local, keep)

    total = [gg_s[e, j : j + 1, :] for j in range(2)]
    for de in range(1, ne):
        gg_copy(de).wait_recv()
        for j in range(2):
            total[j] += gg_r[de, j : j + 1, :]
    for j in range(2):
        gg_ref[j : j + 1, :] = total[j].astype(bf)

    def collect(l):
        for dx in range(1, chips):
            with scope("wait_g2"):
                g2_copy(dx, l).wait_recv()
            got = g2_in[dx, l].astype(f32)
            for n in range(3):
                grad_ref[n, l] += got[:, n * units : (n + 1) * units]

    loop(local, collect)

    for d in range(1, nf):
        with scope("wait_tg"):
            put(tg_s.at[0], tg_s.at[0], so.at[d], ro.at[d], (k, e, f_at(d))).wait()
    pltpu.make_async_copy(tg_s.at[0], tg_s.at[0], own_sems.at[3]).wait()

    for de in range(ne):
        for d in range(nf):
            if de or d:
                info_copy(de, d).wait_send()
    for d in range(1, nf):
        for a in range(2):
            z_whole(a, d).wait_send()
    for g in range(nf):

        @pl.when(f != g)
        def _():
            for a in range(2):
                rs_copy(a, g, 1).wait_send()

    for h in range(halves):
        for g in range(nf):
            sign = jnp.where(f >= g, 1, -1)

            @pl.when(has(sign))
            def _():
                ag_copy(h, g, sign, g).wait_send()

        @pl.when(f > 0)
        def _():
            ag_copy(h, f, -1, nf).wait_send()

    for de in range(1, ne):
        gg_copy(de).wait_send()
        for g in range(nf):
            y_whole(1, g, de, e).wait_send()
            ret_copy(g, de).wait_send()
    for dx in range(chips):
        for a in range(2):
            w_core(a, dx, k).wait_send()
            if dx:
                w_chip(a, dx, k).wait_send()

        def sent(l):
            g1_copy(dx, l).wait_send()
            if dx:
                g2_copy(dx, l).wait_send()

        loop(local, sent)


def per_device(mesh_shape, tokens, out_grad, expert_ids, gate_probs, params, moment_first, moment_second):
    nk, ne, nf = mesh_shape["cuts"], mesh_shape["exp"], mesh_shape["fsdp"]
    token_count, width = tokens.shape
    local, rows, units = params.shape[1:]
    cap = 10 * token_count // 32
    chips = nk // CORES
    span = ne * cap
    slots = local * span
    depth = nk * rows
    halves = 2 if local % 2 == 0 else 1
    bf, f32 = jnp.bfloat16, jnp.float32

    sizes = (nk, ne, nf, local, cap, token_count, rows, units)

    def vm(*shape, kind=bf):
        return pltpu.VMEM(shape, kind)

    def sem(*shape):
        return pltpu.SemaphoreType.DMA(shape)

    scratch = [
        vm(token_count, width),
        vm(token_count, width),
        vm(3, local, rows, units, kind=f32),
        vm(nf, ne, 8, token_count, kind=f32),
        vm(local, depth, 3 * units),
        vm(nf, ne * token_count, depth),
        vm(nf, ne * token_count, depth),
        vm(nf, slots, ne * token_count),
        vm(local, nf * span, depth),
        vm(local, nf * span, depth),
        vm(nf, slots, 2 * units),
        vm(nf, slots, units),
        vm(nf + 1, slots, 2 * units),
        vm(nf + 1, slots, units),
        vm(slots, 3 * units, kind=f32),
        vm(local, nf * span, 3 * units),
        vm(slots, rows),
        vm(nf, ne, token_count, depth),
        vm(nf, token_count, depth),
        vm(ne, 8, token_count, kind=f32),
        vm(ne, 8, token_count, kind=f32),
        vm(chips, local, rows, 3 * units),
        vm(chips, local, rows, 3 * units),
        vm(chips, local, rows, 3 * units),
        vm(chips, local, rows, 3 * units),
        sem(ne, nf), sem(ne, nf),
        sem(2, nf), sem(2, nf),
        sem(2, nf, ne), sem(2, nf, ne),
        sem(2, chips), sem(2, chips),
        sem(2, chips), sem(2, chips),
        sem(2, nf), sem(2, nf + 1),
        sem(halves, nf + 1), sem(halves, nf),
        sem(nf, ne), sem(nf, ne),
        sem(nf), sem(nf),
        sem(ne), sem(ne),
        sem(chips, local), sem(chips, local),
        sem(chips, local), sem(chips, local),
        sem(4),
    ]
    vmem = pl.BlockSpec(memory_space=pltpu.VMEM)
    hbm = pl.BlockSpec(memory_space=pl.ANY)
    token_grad, gates, gradient = pl.pallas_call(
        functools.partial(kernel, sizes),
        out_shape=(
            jax.ShapeDtypeStruct((token_count, width), bf),
            jax.ShapeDtypeStruct((2, token_count), bf),
            jax.ShapeDtypeStruct((3, local, rows, units), f32),
        ),
        in_specs=[vmem, vmem, hbm, hbm, hbm],
        out_specs=(hbm, vmem, vmem),
        scratch_shapes=scratch,
        compiler_params=pltpu.CompilerParams(
            collective_id=0, has_side_effects=True, vmem_limit_bytes=67043328
        ),
    )(expert_ids.T, gate_probs.T, tokens, out_grad, params)
    new_params, new_first, new_second = adam_update(params, gradient, moment_first, moment_second)
    return (token_grad, gates.T, new_params, new_first, new_second)


def solution(mesh):
    tokens_spec = P(("cuts", "exp", "fsdp"), None)
    weights_spec = P(None, "exp", ("cuts", "fsdp"), None)
    return jax.shard_map(
        functools.partial(per_device, dict(mesh.shape)),
        mesh=mesh,
        in_specs=(tokens_spec,) * 4 + (weights_spec,) * 3,
        out_specs=(tokens_spec,) * 2 + (weights_spec,) * 3,
        check_vma=False,
    )
```

```python
import functools

import jax
import jax.numpy as jnp
from jax import lax
from jax.experimental import pallas as pl
from jax.experimental.pallas import tpu as pltpu
from jax.sharding import PartitionSpec as P

CORES = 2
MESH = pl.DeviceIdType.MESH

decay_first = 0.9
decay_second = 0.95
correct_first = 1.0 - 0.9**10
correct_second = 1.0 - 0.95**10
epsilon = 1e-08
learn_rate = 0.0003
weight_decay = 0.1


def adam_update(params, gradient, moment_first, moment_second):
    new_first = decay_first * moment_first + (1.0 - decay_first) * gradient
    new_second = decay_second * moment_second + (1.0 - decay_second) * gradient * gradient
    stepped = new_first / correct_first / (jnp.sqrt(new_second / correct_second) + epsilon)
    new_params = params - learn_rate * (stepped + weight_decay * params)
    return (new_params, new_first, new_second)


def loop(count, body):
    def step(i, carry):
        body(i)
        return carry

    lax.fori_loop(0, count, step, 0)


def dot(a, b, dims):
    return lax.dot_general(a, b, (dims, ((), ())), preferred_element_type=jnp.float32)


def kernel(
    sizes,
    ids_ref, gates_ref, tok_hbm, og_hbm, params_hbm,
    tg_ref, gg_ref, grad_ref,
    tok_ref, og_ref, info, weights, tokb, ogb, place, inp, ups, pre_s, prj_s, pre_r, prj_r, own, dl, sg,
    ret_r, tg_s, gg_s, gg_r, g1_out, g1_in, g2_out, g2_in,
    si, ri, sz, rz, sy, ry, sw, rw, sv, rv, sp, rp, sa, ra, st, rt, so, ro, sg_sem, rg_sem, s1, r1, s2, r2,
    own_sems,
):
    nk, ne, nf, local, cap, tcount, rows, units = sizes
    chips = nk // CORES
    span = ne * cap
    slots = local * span
    bf = jnp.bfloat16
    f32 = jnp.float32
    k, e, f = lax.axis_index("cuts"), lax.axis_index("exp"), lax.axis_index("fsdp")
    x, c = k // CORES, lax.rem(k, CORES)
    scope = jax.named_scope

    def f_at(d):
        return lax.rem(f + d, nf)

    def e_at(d):
        return lax.rem(e + d, ne)

    def chip_at(d, core):
        return lax.rem(x + d, chips) * CORES + core

    partner = x * CORES + 1 - c

    def put(src, dst, send, recv, device):
        return pltpu.make_async_remote_copy(
            src_ref=src, dst_ref=dst, send_sem=send, recv_sem=recv, device_id=device, device_id_type=MESH
        )

    def strip(kk, ff):
        return pl.ds(pl.multiple_of((kk * nf + ff) * rows, rows), rows)

    def cut(kk):
        return pl.ds(pl.multiple_of(kk * rows, rows), rows)

    def mine(ee):
        return pl.ds(pl.multiple_of(ee * tcount, tcount), tcount)

    def group(g):
        return pl.ds(pl.multiple_of(g * span, span), span)

    barrier = pltpu.get_barrier_semaphore()
    partners = 0
    for de in range(ne):
        for d in range(nf):
            if de or d:
                pl.semaphore_signal(barrier, inc=1, device_id=(k, e_at(de), f_at(d)), device_id_type=MESH)
                partners += 1
    pl.semaphore_signal(barrier, inc=1, device_id=(partner, e, f), device_id_type=MESH)
    partners += 1
    for dx in range(1, chips):
        pl.semaphore_signal(barrier, inc=1, device_id=(chip_at(dx, c), e, f), device_id_type=MESH)
        partners += 1

    staged = ((tok_hbm, tok_ref), (og_hbm, og_ref), (params_hbm, grad_ref))
    for n, (src, dst) in enumerate(staged):
        pltpu.make_async_copy(src, dst, own_sems.at[n]).start()

    def iota(shape, dim):
        return lax.broadcasted_iota(jnp.int32, shape, dim)

    experts = iota((local * ne, tcount), 0)
    named = [jnp.where(experts == ids_ref[j : j + 1, :], 1.0, 0.0).astype(f32) for j in range(2)]
    earlier = jnp.where(iota((tcount, tcount), 0) < iota((tcount, tcount), 1), 1.0, 0.0).astype(bf)
    before = dot((named[0] + named[1]).astype(bf), earlier, ((1,), (0,)))
    info[f, e] = jnp.zeros((8, tcount), f32)
    for j in range(2):
        position = jnp.sum(named[j] * before, axis=0, keepdims=True)
        info[f, e, j : j + 1, :] = (ids_ref[j : j + 1, :] * span + e * cap).astype(f32) + position
        info[f, e, j + 2 : j + 3, :] = gates_ref[j : j + 1, :].astype(f32)

    pltpu.make_async_copy(params_hbm, grad_ref, own_sems.at[2]).wait()
    for l in range(local):
        for n in range(3):
            weights[l, cut(k), n * units : (n + 1) * units] = grad_ref[n, l].astype(bf)
    for n, (src, dst) in enumerate(staged[:2]):
        pltpu.make_async_copy(src, dst, own_sems.at[n]).wait()
    with scope("barrier"):
        pl.semaphore_wait(barrier, partners)

    def info_copy(de, d):
        mark = info.at[f, e]
        return put(mark, mark, si.at[de, d], ri.at[de, d], (k, e_at(de), f_at(d)))

    arrays = ((tok_ref, tokb), (og_ref, ogb))
    wide = (pl.ds(0, 2 * units), pl.ds(2 * units, units))

    def sides(t, work):
        for sign in (1, -1):
            g = f + sign * t

            @pl.when((g >= 0) & (g < nf))
            def _():
                work(g)

    def z_start(a, g):
        src, dst = arrays[a]
        for kk in range(nk):
            put(
                src.at[:, strip(kk, g)], dst.at[f, mine(e), cut(kk)], sz.at[a, g], rz.at[a, f], (k, e, g)
            ).start()

    def y_own_start(a):
        src, dst = arrays[a]
        for de in range(1, ne):
            for kk in range(nk):
                put(
                    src.at[:, strip(kk, f)], dst.at[f, mine(e), cut(kk)], sy.at[a, f, de], ry.at[a, f, de],
                    (k, e_at(de), f),
                ).start()

    def w_chip(a, dx, owner):
        held = weights.at[:, cut(owner), wide[a]]
        return put(held, held, sw.at[a, dx], rw.at[a, dx], (chip_at(dx, c), e, f))

    def w_core(a, dx, owner):
        held = weights.at[:, cut(owner), wide[a]]
        return put(held, held, sv.at[a, dx], rv.at[a, dx], (partner, e, f))

    def whole(dst, g, ee, send, recv, device):
        return put(dst.at[g, mine(ee), :], dst.at[g, mine(ee), :], send, recv, device)

    def z_whole(a, g):
        return whole(arrays[a][1], g, e, sz.at[a, g], rz.at[a, g], (k, e, g))

    def y_whole(a, g, de, ee):
        return whole(arrays[a][1], g, ee, sy.at[a, g, de], ry.at[a, g, de], (k, e_at(de), f))

    def z_pass(a, g):
        with scope("wait_z"):
            z_whole(a, g).wait_recv()
        for de in range(1, ne):
            y_whole(a, g, de, e).start()

    for de in range(ne):
        for d in range(nf):
            if de or d:
                info_copy(de, d).start()
    for t in range(1, nf):
        sides(t, functools.partial(z_start, 0))
    y_own_start(0)
    for a in range(2):
        for dx in range(1, chips):
            w_chip(a, dx, k).start()
        w_core(a, 0, k).start()
        if a == 0:
            for t in range(1, nf):
                sides(t, functools.partial(z_start, 1))

    for src, dst in arrays:
        for kk in range(nk):
            dst[f, mine(e), cut(kk)] = src[:, strip(kk, f)]

    for t in range(1, nf):
        sides(t, functools.partial(z_pass, 0))
        if t == 1:
            y_own_start(1)
    for de in range(ne):
        for d in range(nf):
            if de or d:
                info_copy(de, d).wait_recv()

    def w_pass(a):
        with scope("wait_w"):
            for dx in range(1, chips):
                owner = chip_at(chips - dx, c)
                w_chip(a, dx, owner).wait_recv()
                w_core(a, dx, owner).start()

    def w_done(a):
        with scope("wait_w2"):
            for dx in range(chips):
                w_core(a, dx, chip_at(chips - dx, 1 - c)).wait_recv()

    def codes(g, row):
        return jnp.concatenate([info[g, ee, row : row + 1, :] for ee in range(ne)], axis=1)

    first_slot = (e * slots).astype(f32)

    def choose(g, base, count):
        ids = iota((count, ne * tcount), 0).astype(f32) + base
        return [codes(g, j) - first_slot == ids for j in range(2)]

    def at(l):
        return pl.ds(pl.multiple_of(l * span, span), span)

    def picked(a, dst, g):
        src = arrays[a][1]
        for de in range(1, ne):
            with scope("wait_y"):
                y_whole(a, g, de, e_at(ne - de)).wait_recv()

        def column(kk):
            out = dot(place[g], src[g, :, cut(kk)], ((1,), (0,))).astype(bf)
            for l in range(local):
                dst[l, group(g), cut(kk)] = out[l * span : (l + 1) * span]

        loop(nk, column)

    def partial_sum(a, g):
        with scope("partial"):
            if a == 0:
                zero, one = choose(g, 0.0, slots)
                place[g] = jnp.where(zero, 1.0, 0.0).astype(bf) + jnp.where(one, 1.0, 0.0).astype(bf)
            rows_of, sums = ((inp, pre_s), (ups, prj_s))[a]
            picked(a, rows_of, g)

            def expert(l):
                out = dot(rows_of[l, group(g), :], weights[l, :, wide[a]], ((1,), (0,)))
                sums[g, at(l), :] = out.astype(bf)

                @pl.when(g == f)
                def _():
                    own[at(l), wide[a]] = out

            loop(local, expert)

    def rs_copy(a, g, sign):
        sent, got = ((pre_s, pre_r), (prj_s, prj_r))[a]
        spot = jnp.where((sign < 0) & (g == f - 1), nf, g)
        return put(sent.at[g], got.at[spot], sp.at[a, g], rp.at[a, spot], (k, e, f + sign))

    def rs_wait(a, spot):
        got = (pre_r, prj_r)[a]
        put(got.at[spot], got.at[spot], sp.at[a, 0], rp.at[a, spot], (k, e, f_at(1))).wait_recv()

    def rs_step(a, g, sign):
        sent, got = ((pre_s, pre_r), (prj_s, prj_r))[a]
        behind = f - sign

        @pl.when((g - f) * sign > 0)
        def _():
            @pl.when((behind >= 0) & (behind < nf))
            def _():
                with scope("wait_rs"):
                    rs_wait(a, g)

                def add(l):
                    sent[g, at(l), :] = (sent[g, at(l), :].astype(f32) + got[g, at(l), :].astype(f32)).astype(bf)

                loop(local, add)

            rs_copy(a, g, sign).start()

    near = jnp.where(f < nf // 2, 1, -1)

    def rs_chain(a, first=0):
        def steps(n):
            t = n + first
            for sign in (near, -near):
                rs_step(a, jnp.where(sign > 0, nf - 1 - t, t), sign)

        loop(nf - 1 - first, steps)

    at_edge = (f == 0) | (f == nf - 1)

    def both(t, work):
        def side(n):
            g = f + (1 - 2 * n) * t

            @pl.when((g >= 0) & (g < nf))
            def _():
                work(g)

        loop(2, side)

    w_pass(0)
    w_done(0)
    partial_sum(0, f)
    for t in range(1, nf):
        both(t, functools.partial(partial_sum, 0))
        if t == min(2, nf - 1):
            sides(1, functools.partial(z_pass, 1))

    @pl.when(at_edge)
    def _():
        rs_chain(0)

    w_pass(1)
    for t in range(2, nf):
        sides(t, functools.partial(z_pass, 1))
    w_done(1)

    @pl.when(jnp.logical_not(at_edge))
    def _():
        rs_step(0, jnp.where(near > 0, nf - 1, 0), near)

    partial_sum(1, f)
    for t in range(1, nf):
        both(t, functools.partial(partial_sum, 1))

    @pl.when(jnp.logical_not(at_edge))
    def _():
        rs_step(0, jnp.where(near > 0, 0, nf - 1), -near)
        rs_chain(0, 1)

    rs_chain(1)

    for a, got in enumerate((pre_r, prj_r)):
        for spot, edge in ((f, 0), (nf, nf - 1)):

            @pl.when(f == edge)
            def _():
                got[spot] = jnp.zeros(got.shape[1:], bf)

            @pl.when(f != edge)
            def _():
                with scope("wait_own"):
                    rs_wait(a, spot)

    def middle(l, carry):
        here = at(l)
        gate = own[here, :units] + pre_r[f, here, :units].astype(f32) + pre_r[nf, here, :units].astype(f32)
        up = own[here, units : 2 * units] + pre_r[f, here, units:].astype(f32) + pre_r[nf, here, units:].astype(f32)
        proj = own[here, 2 * units :] + prj_r[f, here, :].astype(f32) + prj_r[nf, here, :].astype(f32)
        zero, one = choose(f, (l * span).astype(f32), span)
        scale = jnp.sum(
            jnp.where(zero, codes(f, 2), 0.0) + jnp.where(one, codes(f, 3), 0.0), axis=1, keepdims=True
        )
        sig = jax.nn.sigmoid(gate)
        act = gate * sig
        hidden = act * up
        slot_gate = jnp.sum(hidden * proj, axis=1, keepdims=True)
        delta = scale * proj
        dl[l, group(f), :units] = (delta * up * sig * (1.0 + gate * (1.0 - sig))).astype(bf)
        dl[l, group(f), units : 2 * units] = (delta * act).astype(bf)
        dl[l, group(f), 2 * units :] = (scale * hidden).astype(bf)
        return (
            carry[0] + jnp.sum(jnp.where(zero, slot_gate, 0.0), axis=0, keepdims=True),
            carry[1] + jnp.sum(jnp.where(one, slot_gate, 0.0), axis=0, keepdims=True),
        )

    def ag_copy(h, g, sign, spot):
        held = dl.at[h, group(g), :]
        return put(held, held, sa.at[h, spot], ra.at[h, g], (k, e, f + sign))

    def has(sign):
        return (f + sign >= 0) & (f + sign < nf)

    def ag_own(h):
        for sign, spot in ((1, f), (-1, nf)):

            @pl.when(has(sign))
            def _():
                ag_copy(h, f, sign, spot).start()

    def ag_step(h, t, sign):
        g = f - sign * t

        @pl.when((g >= 0) & (g < nf))
        def _():
            with scope("wait_ag"):
                ag_copy(h, g, sign, g).wait_recv()

            @pl.when(has(sign))
            def _():
                ag_copy(h, g, sign, g).start()

    nothing = jnp.zeros((1, ne * tcount), f32)
    parts = (nothing, nothing)
    ahead = 2
    for h in range(local):
        with scope("middle"):
            parts = middle(jnp.int32(h), parts)
        if h < ahead:
            ag_own(h)

    for ee in range(ne):
        for j in range(2):
            gg_s[ee, j : j + 1, :] = parts[j][:, ee * tcount : (ee + 1) * tcount]

    def gg_copy(de):
        return put(gg_s.at[e_at(de)], gg_r.at[de], sg_sem.at[de], rg_sem.at[de], (k, e_at(de), f))

    for de in range(1, ne):
        gg_copy(de).start()

    for de in range(1, ne):
        for g in range(nf):
            y_whole(0, g, de, e).wait_send()

    def ret_copy(g, de, kk):
        return put(
            tokb.at[g, mine(e_at(de)), cut(kk)], ret_r.at[g, de - 1, :, cut(kk)], st.at[g, de, kk],
            rt.at[g, de, kk], (k, e_at(de), f),
        )

    def slot_rows(l, g):
        with scope("slot_rows"):
            sg[g, at(l), :] = dot(dl[l, group(g), : 2 * units], weights[l, :, : 2 * units], ((1,), (1,))).astype(bf)

    def returned(g):
        with scope("returned"):

            def column(kk):
                tokb[g, :, cut(kk)] = dot(place[g], sg[g, :, cut(kk)], ((0,), (0,))).astype(bf)
                for de in range(1, ne):
                    ret_copy(g, de, kk).start()

            loop(nk, column)

    def final(g):
        with scope("final"):
            d = lax.rem(g - f + nf, nf)

            def column(kk):
                total = tokb[g, mine(e), cut(kk)].astype(f32)
                for de in range(1, ne):
                    with scope("wait_ret"):
                        ret_copy(g, de, kk).wait_recv()
                    total += ret_r[g, de - 1, :, cut(kk)].astype(f32)
                tg_s[g, :, cut(kk)] = total.astype(bf)
                there = tg_ref.at[:, strip(kk, f)]

                @pl.when(d > 0)
                def _():
                    put(tg_s.at[g, :, cut(kk)], there, so.at[d], ro.at[d], (k, e, g)).start()

                @pl.when(d == 0)
                def _():
                    pltpu.make_async_copy(tg_s.at[g, :, cut(kk)], there, own_sems.at[3]).start()

            loop(nk, column)

    def gradient(kk, l):
        ahead = dot(inp[l, :, cut(kk)], dl[l, :, : 2 * units], ((0,), (0,)))
        down = dot(ups[l, :, cut(kk)], dl[l, :, 2 * units :], ((0,), (0,)))
        return ahead, down

    def g1_copy(dx, l):
        return put(g1_out.at[dx, l], g1_in.at[dx, l], s1.at[dx, l], r1.at[dx, l], (partner, e, f))

    def g2_copy(dx, l):
        return put(g2_out.at[dx - 1, l], g2_in.at[dx - 1, l], s2.at[dx, l], r2.at[dx, l], (chip_at(dx, c), e, f))

    def to_core(l):
        with scope("to_core"):
            for dx in [*range(1, chips), 0]:
                ahead, down = gradient(chip_at(dx, 1 - c), l)
                g1_out[dx, l, :, : 2 * units] = ahead.astype(bf)
                g1_out[dx, l, :, 2 * units :] = down.astype(bf)
                g1_copy(dx, l).start()

    def summed(dx, l):
        ahead, down = gradient(chip_at(dx, c), l)
        with scope("wait_g1"):
            g1_copy(dx, l).wait_recv()
        ahead += g1_in[dx, l, :, : 2 * units].astype(f32)
        down += g1_in[dx, l, :, 2 * units :].astype(f32)
        return ahead, down

    def to_chip(l):
        with scope("to_chip"):
            for dx in range(1, chips):
                ahead, down = summed(dx, l)
                g2_out[dx - 1, l, :, : 2 * units] = ahead.astype(bf)
                g2_out[dx - 1, l, :, 2 * units :] = down.astype(bf)
                g2_copy(dx, l).start()

    def keep(l):
        ahead, down = summed(0, l)
        grad_ref[0, l] = ahead[:, :units]
        grad_ref[1, l] = ahead[:, units:]
        grad_ref[2, l] = down

    last = local - 1
    for l in range(local):
        for t in range(1, nf):
            for sign in (1, -1):
                ag_step(l, t, sign)
            if t == 1 and l + ahead < local:
                ag_own(l + ahead)
            if t == nf - 1:
                to_core(jnp.int32(l))
            if t == 1:
                slot_rows(jnp.int32(l), f)
                if l == last:
                    returned(f)
            if l < last:
                if t == 2 and l:
                    to_chip(jnp.int32(l - 1))
                if t == nf - 1:
                    for near_t in range(1, nf):
                        both(near_t, functools.partial(slot_rows, jnp.int32(l)))
            else:
                both(t, functools.partial(slot_rows, jnp.int32(l)))
                both(t, returned)
                if t == 1 and l:
                    to_chip(jnp.int32(l - 1))
                if t == 2:
                    final(f)
                if t > 2:
                    both(t - 2, final)
    to_chip(jnp.int32(last))
    for t in range(max(1, nf - 2), nf):
        both(t, final)
    with scope("keep"):
        loop(local, keep)

    total = [gg_s[e, j : j + 1, :] for j in range(2)]
    for de in range(1, ne):
        gg_copy(de).wait_recv()
        for j in range(2):
            total[j] += gg_r[de, j : j + 1, :]
    for j in range(2):
        gg_ref[j : j + 1, :] = total[j].astype(bf)

    def collect(l):
        for dx in range(1, chips):
            with scope("wait_g2"):
                g2_copy(dx, l).wait_recv()
            got = g2_in[dx - 1, l].astype(f32)
            for n in range(3):
                grad_ref[n, l] += got[:, n * units : (n + 1) * units]

    loop(local, collect)

    for d in range(1, nf):
        with scope("wait_tg"):
            put(tg_s.at[0], tg_s.at[0], so.at[d], ro.at[d], (k, e, f_at(d))).wait()
    pltpu.make_async_copy(tg_s.at[0], tg_s.at[0], own_sems.at[3]).wait()

    for de in range(ne):
        for d in range(nf):
            if de or d:
                info_copy(de, d).wait_send()
    for g in range(nf):

        @pl.when(f != g)
        def _():
            for a in range(2):
                z_whole(a, g).wait_send()
                rs_copy(a, g, 1).wait_send()

    for h in range(local):
        for g in range(nf):
            sign = jnp.where(f >= g, 1, -1)

            @pl.when(has(sign))
            def _():
                ag_copy(h, g, sign, g).wait_send()

        @pl.when(f > 0)
        def _():
            ag_copy(h, f, -1, nf).wait_send()

    for de in range(1, ne):
        gg_copy(de).wait_send()
        for g in range(nf):
            y_whole(1, g, de, e).wait_send()
            for kk in range(nk):
                ret_copy(g, de, kk).wait_send()
    for dx in range(chips):
        for a in range(2):
            w_core(a, dx, k).wait_send()
            if dx:
                w_chip(a, dx, k).wait_send()

        def sent(l):
            g1_copy(dx, l).wait_send()
            if dx:
                g2_copy(dx, l).wait_send()

        loop(local, sent)


def per_device(mesh_shape, tokens, out_grad, expert_ids, gate_probs, params, moment_first, moment_second):
    nk, ne, nf = mesh_shape["cuts"], mesh_shape["exp"], mesh_shape["fsdp"]
    token_count, width = tokens.shape
    local, rows, units = params.shape[1:]
    cap = 10 * token_count // 32
    chips = nk // CORES
    span = ne * cap
    slots = local * span
    depth = nk * rows
    bf, f32 = jnp.bfloat16, jnp.float32

    sizes = (nk, ne, nf, local, cap, token_count, rows, units)

    def vm(*shape, kind=bf):
        return pltpu.VMEM(shape, kind)

    def sem(*shape):
        return pltpu.SemaphoreType.DMA(shape)

    scratch = [
        vm(token_count, width),
        vm(token_count, width),
        vm(nf, ne, 8, token_count, kind=f32),
        vm(local, depth, 3 * units),
        vm(nf, ne * token_count, depth),
        vm(nf, ne * token_count, depth),
        vm(nf, slots, ne * token_count),
        vm(local, nf * span, depth),
        vm(local, nf * span, depth),
        vm(nf, slots, 2 * units),
        vm(nf, slots, units),
        vm(nf + 1, slots, 2 * units),
        vm(nf + 1, slots, units),
        vm(slots, 3 * units, kind=f32),
        vm(local, nf * span, 3 * units),
        vm(nf, slots, depth),
        vm(nf, ne - 1, token_count, depth),
        vm(nf, token_count, depth),
        vm(ne, 8, token_count, kind=f32),
        vm(ne, 8, token_count, kind=f32),
        vm(chips, local, rows, 3 * units),
        vm(chips, local, rows, 3 * units),
        vm(chips - 1, local, rows, 3 * units),
        vm(chips - 1, local, rows, 3 * units),
        sem(ne, nf), sem(ne, nf),
        sem(2, nf), sem(2, nf),
        sem(2, nf, ne), sem(2, nf, ne),
        sem(2, chips), sem(2, chips),
        sem(2, chips), sem(2, chips),
        sem(2, nf), sem(2, nf + 1),
        sem(local, nf + 1), sem(local, nf),
        sem(nf, ne, nk), sem(nf, ne, nk),
        sem(nf), sem(nf),
        sem(ne), sem(ne),
        sem(chips, local), sem(chips, local),
        sem(chips, local), sem(chips, local),
        sem(4),
    ]
    vmem = pl.BlockSpec(memory_space=pltpu.VMEM)
    hbm = pl.BlockSpec(memory_space=pl.ANY)
    token_grad, gates, gradient = pl.pallas_call(
        functools.partial(kernel, sizes),
        out_shape=(
            jax.ShapeDtypeStruct((token_count, width), bf),
            jax.ShapeDtypeStruct((2, token_count), bf),
            jax.ShapeDtypeStruct((3, local, rows, units), f32),
        ),
        in_specs=[vmem, vmem, hbm, hbm, hbm],
        out_specs=(hbm, vmem, vmem),
        scratch_shapes=scratch,
        compiler_params=pltpu.CompilerParams(
            collective_id=0, has_side_effects=True, vmem_limit_bytes=67043328
        ),
    )(expert_ids.T, gate_probs.T, tokens, out_grad, params)
    new_params, new_first, new_second = adam_update(params, gradient, moment_first, moment_second)
    return (token_grad, gates.T, new_params, new_first, new_second)


def solution(mesh):
    tokens_spec = P(("cuts", "exp", "fsdp"), None)
    weights_spec = P(None, "exp", ("cuts", "fsdp"), None)
    return jax.shard_map(
        functools.partial(per_device, dict(mesh.shape)),
        mesh=mesh,
        in_specs=(tokens_spec,) * 4 + (weights_spec,) * 3,
        out_specs=(tokens_spec,) * 2 + (weights_spec,) * 3,
        check_vma=False,
    )
```

```python
import functools
import math

import jax
import jax.numpy as jnp
from jax import lax
from jax.experimental import pallas as pl
from jax.experimental.pallas import tpu as pltpu
from jax.sharding import PartitionSpec as P

CORES = 2
VMEM_ALL = 67043328
MARGIN = 2 * 1024 * 1024
MESH = pl.DeviceIdType.MESH

decay_first = 0.9
decay_second = 0.95
correct_first = 1.0 - 0.9**10
correct_second = 1.0 - 0.95**10
epsilon = 1e-08
learn_rate = 0.0003
weight_decay = 0.1


def adam_update(params, gradient, moment_first, moment_second):
    new_first = decay_first * moment_first + (1.0 - decay_first) * gradient
    new_second = decay_second * moment_second + (1.0 - decay_second) * gradient * gradient
    stepped = new_first / correct_first / (jnp.sqrt(new_second / correct_second) + epsilon)
    new_params = params - learn_rate * (stepped + weight_decay * params)
    return (new_params, new_first, new_second)


def loop(count, body):
    def step(i, carry):
        body(i)
        return carry

    lax.fori_loop(0, count, step, 0)


def dot(a, b, dims):
    return lax.dot_general(a, b, (dims, ((), ())), preferred_element_type=jnp.float32)


def kernel(
    sizes,
    ids_ref, gates_ref, tok_ref, og_ref, params_hbm, first_hbm, second_hbm,
    tg_ref, gg_ref, grad_ref, par_ref, first_ref, second_ref,
    info, weights, tokb, ogb, place, inp, ups, pre_s, prj_s, pre_r, prj_r, own, dl, sg,
    ret_r, tg_s, gg_s, gg_r, g1_out, g1_in, g2_out, g2_in,
    si, ri, sz, rz, sy, ry, sw, rw, sv, rv, sp, rp, sa, ra, st, rt, so, ro, sg_sem, rg_sem, s1, r1, s2, r2,
    own_sems,
):
    nk, ne, nf, local, cap, tcount, rows, units = sizes
    chips = nk // CORES
    span = ne * cap
    slots = local * span
    bf = jnp.bfloat16
    f32 = jnp.float32
    k, e, f = lax.axis_index("cuts"), lax.axis_index("exp"), lax.axis_index("fsdp")
    x, c = k // CORES, lax.rem(k, CORES)
    scope = jax.named_scope

    def f_at(d):
        return lax.rem(f + d, nf)

    def e_at(d):
        return lax.rem(e + d, ne)

    def chip_at(d, core):
        return lax.rem(x + d, chips) * CORES + core

    partner = x * CORES + 1 - c

    def put(src, dst, send, recv, device):
        return pltpu.make_async_remote_copy(
            src_ref=src, dst_ref=dst, send_sem=send, recv_sem=recv, device_id=device, device_id_type=MESH
        )

    def strip(kk, ff):
        return pl.ds(pl.multiple_of((kk * nf + ff) * rows, rows), rows)

    def cut(kk):
        return pl.ds(pl.multiple_of(kk * rows, rows), rows)

    def mine(ee):
        return pl.ds(pl.multiple_of(ee * tcount, tcount), tcount)

    def group(g):
        return pl.ds(pl.multiple_of(g * span, span), span)

    barrier = pltpu.get_barrier_semaphore()
    partners = 0
    for de in range(ne):
        for d in range(nf):
            if de or d:
                pl.semaphore_signal(barrier, inc=1, device_id=(k, e_at(de), f_at(d)), device_id_type=MESH)
                partners += 1
    pl.semaphore_signal(barrier, inc=1, device_id=(partner, e, f), device_id_type=MESH)
    partners += 1
    for dx in range(1, chips):
        pl.semaphore_signal(barrier, inc=1, device_id=(chip_at(dx, c), e, f), device_id_type=MESH)
        partners += 1

    staged = ((params_hbm, par_ref), (first_hbm, first_ref), (second_hbm, second_ref))
    copies = [pltpu.make_async_copy(src, dst, own_sems.at[n]) for n, (src, dst) in enumerate(staged)]
    copies[0].start()

    def iota(shape, dim):
        return lax.broadcasted_iota(jnp.int32, shape, dim)

    experts = iota((local * ne, tcount), 0)
    named = [jnp.where(experts == ids_ref[j : j + 1, :], 1.0, 0.0).astype(f32) for j in range(2)]
    earlier = jnp.where(iota((tcount, tcount), 0) < iota((tcount, tcount), 1), 1.0, 0.0).astype(bf)
    before = dot((named[0] + named[1]).astype(bf), earlier, ((1,), (0,)))
    info[f, e] = jnp.zeros((8, tcount), f32)
    for j in range(2):
        position = jnp.sum(named[j] * before, axis=0, keepdims=True)
        info[f, e, j : j + 1, :] = (ids_ref[j : j + 1, :] * span + e * cap).astype(f32) + position
        info[f, e, j + 2 : j + 3, :] = gates_ref[j : j + 1, :].astype(f32)

    copies[0].wait()
    for l in range(local):
        for n in range(3):
            weights[l, cut(k), n * units : (n + 1) * units] = par_ref[n, l].astype(bf)
    with scope("barrier"):
        pl.semaphore_wait(barrier, partners)

    def info_copy(de, d):
        mark = info.at[f, e]
        return put(mark, mark, si.at[de, d], ri.at[de, d], (k, e_at(de), f_at(d)))

    at_edge = (f == 0) | (f == nf - 1)

    def far(n):
        return jnp.where(at_edge, nf + 1 - n, n) if n > 1 else 1

    arrays = ((tok_ref, tokb), (og_ref, ogb))
    wide = (pl.ds(0, 2 * units), pl.ds(2 * units, units))

    def sides(t, work):
        for sign in (1, -1):
            g = f + sign * t

            @pl.when((g >= 0) & (g < nf))
            def _():
                work(g)

    def z_start(a, g):
        src, dst = arrays[a]
        for kk in range(nk):
            put(
                src.at[:, strip(kk, g)], dst.at[f, mine(e), cut(kk)], sz.at[a, g], rz.at[a, f], (k, e, g)
            ).start()

    def y_own_start(a):
        src, dst = arrays[a]
        for de in range(1, ne):
            for kk in range(nk):
                put(
                    src.at[:, strip(kk, f)], dst.at[f, mine(e), cut(kk)], sy.at[a, f, de], ry.at[a, f, de],
                    (k, e_at(de), f),
                ).start()

    def w_chip(a, dx, owner):
        held = weights.at[:, cut(owner), wide[a]]
        return put(held, held, sw.at[a, dx], rw.at[a, dx], (chip_at(dx, c), e, f))

    def w_core(a, dx, owner):
        held = weights.at[:, cut(owner), wide[a]]
        return put(held, held, sv.at[a, dx], rv.at[a, dx], (partner, e, f))

    def whole(dst, g, ee, send, recv, device):
        return put(dst.at[g, mine(ee), :], dst.at[g, mine(ee), :], send, recv, device)

    def z_whole(a, g):
        return whole(arrays[a][1], g, e, sz.at[a, g], rz.at[a, g], (k, e, g))

    def y_whole(a, g, de, ee):
        return whole(arrays[a][1], g, ee, sy.at[a, g, de], ry.at[a, g, de], (k, e_at(de), f))

    def z_pass(a, g):
        with scope("wait_z"):
            z_whole(a, g).wait_recv()
        for de in range(1, ne):
            y_whole(a, g, de, e).start()

    for de in range(ne):
        for d in range(nf):
            if de or d:
                info_copy(de, d).start()
    for t in range(1, nf):
        sides(far(t), functools.partial(z_start, 0))
    y_own_start(0)
    for a in range(2):
        for dx in range(1, chips):
            w_chip(a, dx, k).start()
        w_core(a, 0, k).start()
        if a == 0:
            for t in range(1, nf):
                sides(far(t), functools.partial(z_start, 1))

    copies[1].start()
    copies[2].start()
    for src, dst in arrays:
        for kk in range(nk):
            dst[f, mine(e), cut(kk)] = src[:, strip(kk, f)]

    for t in range(1, nf):
        sides(far(t), functools.partial(z_pass, 0))
        if t == 1:
            y_own_start(1)
    for de in range(ne):
        for d in range(nf):
            if de or d:
                info_copy(de, d).wait_recv()

    def w_pass(a):
        with scope("wait_w"):
            for dx in range(1, chips):
                owner = chip_at(chips - dx, c)
                w_chip(a, dx, owner).wait_recv()
                w_core(a, dx, owner).start()

    def w_done(a):
        with scope("wait_w2"):
            for dx in range(chips):
                w_core(a, dx, chip_at(chips - dx, 1 - c)).wait_recv()

    def codes(g, row):
        return jnp.concatenate([info[g, ee, row : row + 1, :] for ee in range(ne)], axis=1)

    first_slot = (e * slots).astype(f32)

    def choose(g, base, count):
        ids = iota((count, ne * tcount), 0).astype(f32) + base
        return [codes(g, j) - first_slot == ids for j in range(2)]

    def at(l):
        return pl.ds(pl.multiple_of(l * span, span), span)

    def picked(a, dst, g):
        src = arrays[a][1]
        for de in range(1, ne):
            with scope("wait_y"):
                y_whole(a, g, de, e_at(ne - de)).wait_recv()

        def column(kk):
            out = dot(place[g], src[g, :, cut(kk)], ((1,), (0,))).astype(bf)
            for l in range(local):
                dst[l, group(g), cut(kk)] = out[l * span : (l + 1) * span]

        loop(nk, column)

    def partial_sum(a, g):
        with scope("partial"):
            if a == 0:
                zero, one = choose(g, 0.0, slots)
                place[g] = jnp.where(zero, 1.0, 0.0).astype(bf) + jnp.where(one, 1.0, 0.0).astype(bf)
            rows_of, sums = ((inp, pre_s), (ups, prj_s))[a]
            picked(a, rows_of, g)

            def expert(l):
                out = dot(rows_of[l, group(g), :], weights[l, :, wide[a]], ((1,), (0,)))
                sums[g, at(l), :] = out.astype(bf)

                @pl.when(g == f)
                def _():
                    own[at(l), wide[a]] = out

            loop(local, expert)

    def rs_copy(a, g, sign):
        sent, got = ((pre_s, pre_r), (prj_s, prj_r))[a]
        spot = jnp.where((sign < 0) & (g == f - 1), nf, g)
        return put(sent.at[g], got.at[spot], sp.at[a, g], rp.at[a, spot], (k, e, f + sign))

    def rs_wait(a, spot):
        got = (pre_r, prj_r)[a]
        put(got.at[spot], got.at[spot], sp.at[a, 0], rp.at[a, spot], (k, e, f_at(1))).wait_recv()

    def rs_step(a, g, sign):
        sent, got = ((pre_s, pre_r), (prj_s, prj_r))[a]
        behind = f - sign

        @pl.when((g - f) * sign > 0)
        def _():
            @pl.when((behind >= 0) & (behind < nf))
            def _():
                with scope("wait_rs"):
                    rs_wait(a, g)

                def add(l):
                    sent[g, at(l), :] = (sent[g, at(l), :].astype(f32) + got[g, at(l), :].astype(f32)).astype(bf)

                loop(local, add)

            rs_copy(a, g, sign).start()

    near = jnp.where(f < nf // 2, 1, -1)

    def rs_chain(a, first=0):
        def steps(n):
            t = n + first
            for sign in (near, -near):
                rs_step(a, jnp.where(sign > 0, nf - 1 - t, t), sign)

        loop(nf - 1 - first, steps)

    def both(t, work):
        def side(n):
            g = f + (1 - 2 * n) * t

            @pl.when((g >= 0) & (g < nf))
            def _():
                work(g)

        loop(2, side)

    w_pass(0)
    w_done(0)
    partial_sum(0, f)
    for t in range(1, nf):
        both(far(t), functools.partial(partial_sum, 0))
        if t == min(2, nf - 1):
            sides(1, functools.partial(z_pass, 1))

    @pl.when(at_edge)
    def _():
        rs_chain(0)

    w_pass(1)
    for t in range(2, nf):
        sides(far(t), functools.partial(z_pass, 1))
    w_done(1)

    @pl.when(jnp.logical_not(at_edge))
    def _():
        rs_step(0, jnp.where(near > 0, nf - 1, 0), near)

    partial_sum(1, f)
    for t in range(1, nf):
        both(far(t), functools.partial(partial_sum, 1))
        if t == 1:

            @pl.when(jnp.logical_not(at_edge))
            def _():
                rs_step(0, jnp.where(near > 0, 0, nf - 1), -near)

    @pl.when(jnp.logical_not(at_edge))
    def _():
        rs_chain(0, 1)

    rs_chain(1)

    for a, got in enumerate((pre_r, prj_r)):
        for spot, edge in ((f, 0), (nf, nf - 1)):

            @pl.when(f == edge)
            def _():
                got[spot] = jnp.zeros(got.shape[1:], bf)

            @pl.when(f != edge)
            def _():
                with scope("wait_own"):
                    rs_wait(a, spot)

    def middle(l, carry):
        here = at(l)
        gate = own[here, :units] + pre_r[f, here, :units].astype(f32) + pre_r[nf, here, :units].astype(f32)
        up = own[here, units : 2 * units] + pre_r[f, here, units:].astype(f32) + pre_r[nf, here, units:].astype(f32)
        proj = own[here, 2 * units :] + prj_r[f, here, :].astype(f32) + prj_r[nf, here, :].astype(f32)
        zero, one = choose(f, (l * span).astype(f32), span)
        scale = jnp.sum(
            jnp.where(zero, codes(f, 2), 0.0) + jnp.where(one, codes(f, 3), 0.0), axis=1, keepdims=True
        )
        sig = jax.nn.sigmoid(gate)
        act = gate * sig
        hidden = act * up
        slot_gate = jnp.sum(hidden * proj, axis=1, keepdims=True)
        delta = scale * proj
        dl[l, group(f), :units] = (delta * up * sig * (1.0 + gate * (1.0 - sig))).astype(bf)
        dl[l, group(f), units : 2 * units] = (delta * act).astype(bf)
        dl[l, group(f), 2 * units :] = (scale * hidden).astype(bf)
        return (
            carry[0] + jnp.sum(jnp.where(zero, slot_gate, 0.0), axis=0, keepdims=True),
            carry[1] + jnp.sum(jnp.where(one, slot_gate, 0.0), axis=0, keepdims=True),
        )

    def ag_copy(h, g, sign, spot):
        held = dl.at[h, group(g), :]
        return put(held, held, sa.at[h, spot], ra.at[h, g], (k, e, f + sign))

    def has(sign):
        return (f + sign >= 0) & (f + sign < nf)

    def ag_own(h):
        for sign, spot in ((1, f), (-1, nf)):

            @pl.when(has(sign))
            def _():
                ag_copy(h, f, sign, spot).start()

    def ag_step(h, t, sign):
        g = f - sign * t

        @pl.when((g >= 0) & (g < nf))
        def _():
            with scope("wait_ag"):
                ag_copy(h, g, sign, g).wait_recv()

            @pl.when(has(sign))
            def _():
                ag_copy(h, g, sign, g).start()

    nothing = jnp.zeros((1, ne * tcount), f32)
    parts = (nothing, nothing)
    ahead = 2
    for h in range(local):
        with scope("middle"):
            parts = middle(jnp.int32(h), parts)
        if h < ahead:
            ag_own(h)

    for ee in range(ne):
        for j in range(2):
            gg_s[ee, j : j + 1, :] = parts[j][:, ee * tcount : (ee + 1) * tcount]

    def gg_copy(de):
        return put(gg_s.at[e_at(de)], gg_r.at[de], sg_sem.at[de], rg_sem.at[de], (k, e_at(de), f))

    for de in range(1, ne):
        gg_copy(de).start()

    for de in range(1, ne):
        for g in range(nf):
            y_whole(0, g, de, e).wait_send()

    def ret_copy(g, de, kk):
        return put(
            tokb.at[g, mine(e_at(de)), cut(kk)], ret_r.at[g, de - 1, :, cut(kk)], st.at[g, de, kk],
            rt.at[g, de, kk], (k, e_at(de), f),
        )

    def slot_rows(l, g):
        with scope("slot_rows"):
            sg[g, at(l), :] = dot(dl[l, group(g), : 2 * units], weights[l, :, : 2 * units], ((1,), (1,))).astype(bf)

    def returned(g):
        with scope("returned"):

            def column(kk):
                tokb[g, :, cut(kk)] = dot(place[g], sg[g, :, cut(kk)], ((0,), (0,))).astype(bf)
                for de in range(1, ne):
                    ret_copy(g, de, kk).start()

            loop(nk, column)

    def final(g):
        with scope("final"):
            d = lax.rem(g - f + nf, nf)

            def column(kk):
                total = tokb[g, mine(e), cut(kk)].astype(f32)
                for de in range(1, ne):
                    with scope("wait_ret"):
                        ret_copy(g, de, kk).wait_recv()
                    total += ret_r[g, de - 1, :, cut(kk)].astype(f32)
                tg_s[g, :, cut(kk)] = total.astype(bf)
                there = tg_ref.at[:, strip(kk, f)]

                @pl.when(d > 0)
                def _():
                    put(tg_s.at[g, :, cut(kk)], there, so.at[d], ro.at[d], (k, e, g)).start()

                @pl.when(d == 0)
                def _():
                    pltpu.make_async_copy(tg_s.at[g, :, cut(kk)], there, own_sems.at[3]).start()

            loop(nk, column)

    def gradient(kk, l):
        ahead = dot(inp[l, :, cut(kk)], dl[l, :, : 2 * units], ((0,), (0,)))
        down = dot(ups[l, :, cut(kk)], dl[l, :, 2 * units :], ((0,), (0,)))
        return ahead, down

    def g1_copy(dx, l):
        return put(g1_out.at[dx, l], g1_in.at[dx, l], s1.at[dx, l], r1.at[dx, l], (partner, e, f))

    def g2_copy(dx, l):
        return put(g2_out.at[dx - 1, l], g2_in.at[dx - 1, l], s2.at[dx, l], r2.at[dx, l], (chip_at(dx, c), e, f))

    def to_core(l):
        with scope("to_core"):
            for dx in [*range(1, chips), 0]:
                ahead, down = gradient(chip_at(dx, 1 - c), l)
                g1_out[dx, l, :, : 2 * units] = ahead.astype(bf)
                g1_out[dx, l, :, 2 * units :] = down.astype(bf)
                g1_copy(dx, l).start()

    def summed(dx, l):
        ahead, down = gradient(chip_at(dx, c), l)
        with scope("wait_g1"):
            g1_copy(dx, l).wait_recv()
        ahead += g1_in[dx, l, :, : 2 * units].astype(f32)
        down += g1_in[dx, l, :, 2 * units :].astype(f32)
        return ahead, down

    def to_chip(l):
        with scope("to_chip"):
            for dx in range(1, chips):
                ahead, down = summed(dx, l)
                g2_out[dx - 1, l, :, : 2 * units] = ahead.astype(bf)
                g2_out[dx - 1, l, :, 2 * units :] = down.astype(bf)
                g2_copy(dx, l).start()

    def keep(l):
        ahead, down = summed(0, l)
        grad_ref[0, l] = ahead[:, :units]
        grad_ref[1, l] = ahead[:, units:]
        grad_ref[2, l] = down

    def collect(l):
        for dx in range(1, chips):
            with scope("wait_g2"):
                g2_copy(dx, l).wait_recv()
            got = g2_in[dx - 1, l].astype(f32)
            for n in range(3):
                grad_ref[n, l] += got[:, n * units : (n + 1) * units]

    def own_rows(l):
        slot_rows(l, f)

    loop(local, own_rows)
    returned(f)
    tail = min(2, local)
    head = local - tail
    for l in range(head):
        for t in range(1, nf):
            for sign in (1, -1):
                ag_step(l, t, sign)
            if t == 1 and l + ahead < local:
                ag_own(l + ahead)
            if t == 2 and l:
                to_chip(jnp.int32(l - 1))
        to_core(jnp.int32(l))
        for t in range(1, nf):
            both(t, functools.partial(slot_rows, jnp.int32(l)))
        if l == 0:
            final(f)
        else:
            keep(jnp.int32(l - 1))
    for t in range(1, nf):
        for l in range(head, local):
            for sign in (1, -1):
                ag_step(l, t, sign)
        if t == 1 and head:
            to_chip(jnp.int32(head - 1))
        if t == nf - 1:
            for l in range(head, local):
                to_core(jnp.int32(l))

        def rows_back(g):
            for l in range(head, local):
                slot_rows(jnp.int32(l), g)
            returned(g)

        both(t, rows_back)
    if not head:
        final(f)
    for n in range(max(tail, nf - 1)):
        if n < tail:
            to_chip(jnp.int32(head + n))
        if n < nf - 1:
            both(n + 1, final)
    with scope("keep"):
        for l in range(max(head - 1, 0), local):
            keep(jnp.int32(l))

    total = [gg_s[e, j : j + 1, :] for j in range(2)]
    for de in range(1, ne):
        gg_copy(de).wait_recv()
        for j in range(2):
            total[j] += gg_r[de, j : j + 1, :]
    for j in range(2):
        gg_ref[j : j + 1, :] = total[j].astype(bf)

    loop(local, collect)

    for d in range(1, nf):
        with scope("wait_tg"):
            put(tg_s.at[0], tg_s.at[0], so.at[d], ro.at[d], (k, e, f_at(d))).wait()
    pltpu.make_async_copy(tg_s.at[0], tg_s.at[0], own_sems.at[3]).wait()
    copies[1].wait()
    copies[2].wait()

    for de in range(ne):
        for d in range(nf):
            if de or d:
                info_copy(de, d).wait_send()
    for g in range(nf):

        @pl.when(f != g)
        def _():
            for a in range(2):
                z_whole(a, g).wait_send()
                rs_copy(a, g, 1).wait_send()

    for h in range(local):
        for g in range(nf):
            sign = jnp.where(f >= g, 1, -1)

            @pl.when(has(sign))
            def _():
                ag_copy(h, g, sign, g).wait_send()

        @pl.when(f > 0)
        def _():
            ag_copy(h, f, -1, nf).wait_send()

    for de in range(1, ne):
        gg_copy(de).wait_send()
        for g in range(nf):
            y_whole(1, g, de, e).wait_send()
            for kk in range(nk):
                ret_copy(g, de, kk).wait_send()
    for dx in range(chips):
        for a in range(2):
            w_core(a, dx, k).wait_send()
            if dx:
                w_chip(a, dx, k).wait_send()

        def sent(l):
            g1_copy(dx, l).wait_send()
            if dx:
                g2_copy(dx, l).wait_send()

        loop(local, sent)


def per_device(mesh_shape, tokens, out_grad, expert_ids, gate_probs, params, moment_first, moment_second):
    nk, ne, nf = mesh_shape["cuts"], mesh_shape["exp"], mesh_shape["fsdp"]
    token_count, width = tokens.shape
    local, rows, units = params.shape[1:]
    cap = 10 * token_count // 32
    chips = nk // CORES
    span = ne * cap
    slots = local * span
    depth = nk * rows
    bf, f32 = jnp.bfloat16, jnp.float32

    sizes = (nk, ne, nf, local, cap, token_count, rows, units)

    held = []

    def vm(*shape, kind=bf):
        held.append(math.prod(shape) * jnp.dtype(kind).itemsize)
        return pltpu.VMEM(shape, kind)

    def sem(*shape):
        return pltpu.SemaphoreType.DMA(shape)

    scratch = [
        vm(nf, ne, 8, token_count, kind=f32),
        vm(local, depth, 3 * units),
        vm(nf, ne * token_count, depth),
        vm(nf, ne * token_count, depth),
        vm(nf, slots, ne * token_count),
        vm(local, nf * span, depth),
        vm(local, nf * span, depth),
        vm(nf, slots, 2 * units),
        vm(nf, slots, units),
        vm(nf + 1, slots, 2 * units),
        vm(nf + 1, slots, units),
        vm(slots, 3 * units, kind=f32),
        vm(local, nf * span, 3 * units),
        vm(nf, slots, depth),
        vm(nf, ne - 1, token_count, depth),
        vm(nf, token_count, depth),
        vm(ne, 8, token_count, kind=f32),
        vm(ne, 8, token_count, kind=f32),
        vm(chips, local, rows, 3 * units),
        vm(chips, local, rows, 3 * units),
        vm(chips - 1, local, rows, 3 * units),
        vm(chips - 1, local, rows, 3 * units),
        sem(ne, nf), sem(ne, nf),
        sem(2, nf), sem(2, nf),
        sem(2, nf, ne), sem(2, nf, ne),
        sem(2, chips), sem(2, chips),
        sem(2, chips), sem(2, chips),
        sem(2, nf), sem(2, nf + 1),
        sem(local, nf + 1), sem(local, nf),
        sem(nf, ne, nk), sem(nf, ne, nk),
        sem(nf), sem(nf),
        sem(ne), sem(ne),
        sem(chips, local), sem(chips, local),
        sem(chips, local), sem(chips, local),
        sem(4),
    ]
    grant = sum(held) + MARGIN
    if 3 * grant > 2 * VMEM_ALL:
        grant = VMEM_ALL
    state = jax.ShapeDtypeStruct((3, local, rows, units), f32)
    vmem = pl.BlockSpec(memory_space=pltpu.VMEM)
    hbm = pl.BlockSpec(memory_space=pltpu.HBM)
    anywhere = pl.BlockSpec(memory_space=pl.ANY)
    token_grad, gates, gradient, params, moment_first, moment_second = pl.pallas_call(
        functools.partial(kernel, sizes),
        out_shape=(
            jax.ShapeDtypeStruct((token_count, width), bf),
            jax.ShapeDtypeStruct((2, token_count), bf),
            state, state, state, state,
        ),
        in_specs=[vmem, vmem, vmem, vmem, hbm, hbm, hbm],
        out_specs=(anywhere, vmem, vmem, vmem, vmem, vmem),
        scratch_shapes=scratch,
        compiler_params=pltpu.CompilerParams(
            collective_id=0, has_side_effects=True, vmem_limit_bytes=grant
        ),
    )(expert_ids.T, gate_probs.T, tokens, out_grad, params, moment_first, moment_second)
    new_params, new_first, new_second = adam_update(params, gradient, moment_first, moment_second)
    return (token_grad, gates.T, new_params, new_first, new_second)


def solution(mesh):
    tokens_spec = P(("cuts", "exp", "fsdp"), None)
    weights_spec = P(None, "exp", ("cuts", "fsdp"), None)
    return jax.shard_map(
        functools.partial(per_device, dict(mesh.shape)),
        mesh=mesh,
        in_specs=(tokens_spec,) * 4 + (weights_spec,) * 3,
        out_specs=(tokens_spec,) * 2 + (weights_spec,) * 3,
        check_vma=False,
    )
```

```python
import functools
import math

import jax
import jax.numpy as jnp
from jax import lax
from jax.experimental import pallas as pl
from jax.experimental.pallas import tpu as pltpu
from jax.sharding import PartitionSpec as P

CORES = 2
VMEM_ALL = 67043328
MARGIN = 2 * 1024 * 1024
MESH = pl.DeviceIdType.MESH

decay_first = 0.9
decay_second = 0.95
correct_first = 1.0 - 0.9**10
correct_second = 1.0 - 0.95**10
epsilon = 1e-08
learn_rate = 0.0003
weight_decay = 0.1


def adam_update(params, gradient, moment_first, moment_second):
    new_first = decay_first * moment_first + (1.0 - decay_first) * gradient
    new_second = decay_second * moment_second + (1.0 - decay_second) * gradient * gradient
    stepped = new_first / correct_first / (jnp.sqrt(new_second / correct_second) + epsilon)
    new_params = params - learn_rate * (stepped + weight_decay * params)
    return (new_params, new_first, new_second)


def loop(count, body):
    def step(i, carry):
        body(i)
        return carry

    lax.fori_loop(0, count, step, 0)


def dot(a, b, dims):
    return lax.dot_general(a, b, (dims, ((), ())), preferred_element_type=jnp.float32)


def kernel(
    sizes,
    ids_ref, gates_ref, tok_ref, og_ref, params_hbm, first_hbm, second_hbm,
    tg_ref, gg_ref, grad_ref, par_ref, first_ref, second_ref,
    info, weights, tokb, ogb, place, inp, ups, pre_s, prj_s, pre_r, prj_r, own, dl, sg,
    ret_r, tg_s, gg_s, gg_r, g1_out, g1_in, g2_out, g2_in,
    si, ri, sz, rz, sy, ry, sw, rw, sv, rv, sp, rp, sa, ra, st, rt, so, ro, sg_sem, rg_sem, s1, r1, s2, r2,
    own_sems,
):
    nk, ne, nf, local, cap, tcount, rows, units = sizes
    chips = nk // CORES
    span = ne * cap
    slots = local * span
    bf = jnp.bfloat16
    f32 = jnp.float32
    k, e, f = lax.axis_index("cuts"), lax.axis_index("exp"), lax.axis_index("fsdp")
    x, c = k // CORES, lax.rem(k, CORES)
    scope = jax.named_scope

    def f_at(d):
        return lax.rem(f + d, nf)

    def e_at(d):
        return lax.rem(e + d, ne)

    def chip_at(d, core):
        return lax.rem(x + d, chips) * CORES + core

    partner = x * CORES + 1 - c

    def put(src, dst, send, recv, device):
        return pltpu.make_async_remote_copy(
            src_ref=src, dst_ref=dst, send_sem=send, recv_sem=recv, device_id=device, device_id_type=MESH
        )

    def strip(kk, ff):
        return pl.ds(pl.multiple_of((kk * nf + ff) * rows, rows), rows)

    def cut(kk):
        return pl.ds(pl.multiple_of(kk * rows, rows), rows)

    def mine(ee):
        return pl.ds(pl.multiple_of(ee * tcount, tcount), tcount)

    def group(g):
        return pl.ds(pl.multiple_of(g * span, span), span)

    barrier = pltpu.get_barrier_semaphore()
    partners = 0
    for de in range(ne):
        for d in range(nf):
            if de or d:
                pl.semaphore_signal(barrier, inc=1, device_id=(k, e_at(de), f_at(d)), device_id_type=MESH)
                partners += 1
    pl.semaphore_signal(barrier, inc=1, device_id=(partner, e, f), device_id_type=MESH)
    partners += 1
    for dx in range(1, chips):
        pl.semaphore_signal(barrier, inc=1, device_id=(chip_at(dx, c), e, f), device_id_type=MESH)
        partners += 1

    staged = ((params_hbm, par_ref), (first_hbm, first_ref), (second_hbm, second_ref))
    copies = [pltpu.make_async_copy(src, dst, own_sems.at[n]) for n, (src, dst) in enumerate(staged)]
    copies[0].start()

    def iota(shape, dim):
        return lax.broadcasted_iota(jnp.int32, shape, dim)

    experts = iota((local * ne, tcount), 0)
    named = [jnp.where(experts == ids_ref[j : j + 1, :], 1.0, 0.0).astype(f32) for j in range(2)]
    earlier = jnp.where(iota((tcount, tcount), 0) < iota((tcount, tcount), 1), 1.0, 0.0).astype(bf)
    before = dot((named[0] + named[1]).astype(bf), earlier, ((1,), (0,)))
    info[f, e] = jnp.zeros((8, tcount), f32)
    for j in range(2):
        position = jnp.sum(named[j] * before, axis=0, keepdims=True)
        info[f, e, j : j + 1, :] = (ids_ref[j : j + 1, :] * span + e * cap).astype(f32) + position
        info[f, e, j + 2 : j + 3, :] = gates_ref[j : j + 1, :].astype(f32)

    copies[0].wait()
    for l in range(local):
        for n in range(3):
            weights[l, cut(k), n * units : (n + 1) * units] = par_ref[n, l].astype(bf)
    with scope("barrier"):
        pl.semaphore_wait(barrier, partners)

    def info_copy(de, d):
        mark = info.at[f, e]
        return put(mark, mark, si.at[de, d], ri.at[de, d], (k, e_at(de), f_at(d)))

    at_edge = (f == 0) | (f == nf - 1)

    def arrivals(a, place):
        if place == 0:
            return [1, *range(nf - 1, 1, -1)]
        ends = [nf - 1, 0] if a == 0 else [0, nf - 1]
        inner = sorted(set(range(1, nf - 1)) - {place}, key=lambda g: abs(g - place))
        return ends + inner

    def arriving(a, n):
        place = jnp.where(f < nf // 2, f, nf - 1 - f)
        g = jnp.int32(arrivals(a, 0)[n])
        for p in range(1, nf // 2):
            g = jnp.where(place == p, arrivals(a, p)[n], g)
        return jnp.where(f < nf // 2, g, nf - 1 - g)

    arrays = ((tok_ref, tokb), (og_ref, ogb))
    wide = (pl.ds(0, 2 * units), pl.ds(2 * units, units))

    def sides(t, work):
        for sign in (1, -1):
            g = f + sign * t

            @pl.when((g >= 0) & (g < nf))
            def _():
                work(g)

    def z_start(a, g):
        src, dst = arrays[a]
        for kk in range(nk):
            put(
                src.at[:, strip(kk, g)], dst.at[f, mine(e), cut(kk)], sz.at[a, g], rz.at[a, f], (k, e, g)
            ).start()

    def y_own_start(a):
        src, dst = arrays[a]
        for de in range(1, ne):
            for kk in range(nk):
                put(
                    src.at[:, strip(kk, f)], dst.at[f, mine(e), cut(kk)], sy.at[a, f, de], ry.at[a, f, de],
                    (k, e_at(de), f),
                ).start()

    def w_chip(a, dx, owner):
        held = weights.at[:, cut(owner), wide[a]]
        return put(held, held, sw.at[a, dx], rw.at[a, dx], (chip_at(dx, c), e, f))

    def w_core(a, dx, owner):
        held = weights.at[:, cut(owner), wide[a]]
        return put(held, held, sv.at[a, dx], rv.at[a, dx], (partner, e, f))

    def whole(dst, g, ee, send, recv, device):
        return put(dst.at[g, mine(ee), :], dst.at[g, mine(ee), :], send, recv, device)

    def z_whole(a, g):
        return whole(arrays[a][1], g, e, sz.at[a, g], rz.at[a, g], (k, e, g))

    def y_whole(a, g, de, ee):
        return whole(arrays[a][1], g, ee, sy.at[a, g, de], ry.at[a, g, de], (k, e_at(de), f))

    def z_pass(a, g):
        with scope("wait_z"):
            z_whole(a, g).wait_recv()
        for de in range(1, ne):
            y_whole(a, g, de, e).start()

    for de in range(ne):
        for d in range(nf):
            if de or d:
                info_copy(de, d).start()
    def z_starts(a, distances):
        for t in distances:
            sides(t, functools.partial(z_start, a))

    @pl.when(at_edge)
    def _():
        z_starts(0, range(nf - 1, 0, -1))
        z_starts(1, [1])

    @pl.when(jnp.logical_not(at_edge))
    def _():
        z_starts(0, range(1, nf))
        z_starts(1, range(1, nf))

    y_own_start(0)
    for a in range(2):
        for dx in range(1, chips):
            w_chip(a, dx, k).start()
        w_core(a, 0, k).start()

    copies[1].start()
    copies[2].start()
    for src, dst in arrays:
        for kk in range(nk):
            dst[f, mine(e), cut(kk)] = src[:, strip(kk, f)]

    for n in range(nf - 1):
        z_pass(0, arriving(0, n))
        if n == 0:
            y_own_start(1)

    @pl.when(at_edge)
    def _():
        z_starts(1, range(nf - 1, 1, -1))

    z_pass(1, arriving(1, 0))
    for de in range(ne):
        for d in range(nf):
            if de or d:
                info_copy(de, d).wait_recv()

    def w_pass(a):
        with scope("wait_w"):
            for dx in range(1, chips):
                owner = chip_at(chips - dx, c)
                w_chip(a, dx, owner).wait_recv()
                w_core(a, dx, owner).start()

    def w_done(a):
        with scope("wait_w2"):
            for dx in range(chips):
                w_core(a, dx, chip_at(chips - dx, 1 - c)).wait_recv()

    def codes(g, row):
        return jnp.concatenate([info[g, ee, row : row + 1, :] for ee in range(ne)], axis=1)

    first_slot = (e * slots).astype(f32)

    def choose(g, base, count):
        ids = iota((count, ne * tcount), 0).astype(f32) + base
        return [codes(g, j) - first_slot == ids for j in range(2)]

    def at(l):
        return pl.ds(pl.multiple_of(l * span, span), span)

    def picked(a, dst, g):
        src = arrays[a][1]
        for de in range(1, ne):
            with scope("wait_y"):
                y_whole(a, g, de, e_at(ne - de)).wait_recv()

        def column(kk):
            out = dot(place[g], src[g, :, cut(kk)], ((1,), (0,))).astype(bf)
            for l in range(local):
                dst[l, group(g), cut(kk)] = out[l * span : (l + 1) * span]

        loop(nk, column)

    def partial_sum(a, g):
        with scope("partial"):
            if a == 0:
                zero, one = choose(g, 0.0, slots)
                place[g] = jnp.where(zero, 1.0, 0.0).astype(bf) + jnp.where(one, 1.0, 0.0).astype(bf)
            rows_of, sums = ((inp, pre_s), (ups, prj_s))[a]
            picked(a, rows_of, g)

            def expert(l):
                out = dot(rows_of[l, group(g), :], weights[l, :, wide[a]], ((1,), (0,)))
                sums[g, at(l), :] = out.astype(bf)

                @pl.when(g == f)
                def _():
                    own[at(l), wide[a]] = out

            loop(local, expert)

    def rs_copy(a, g, sign):
        sent, got = ((pre_s, pre_r), (prj_s, prj_r))[a]
        spot = jnp.where((sign < 0) & (g == f - 1), nf, g)
        return put(sent.at[g], got.at[spot], sp.at[a, g], rp.at[a, spot], (k, e, f + sign))

    def rs_wait(a, spot):
        got = (pre_r, prj_r)[a]
        put(got.at[spot], got.at[spot], sp.at[a, 0], rp.at[a, spot], (k, e, f_at(1))).wait_recv()

    def rs_step(a, g, sign):
        sent, got = ((pre_s, pre_r), (prj_s, prj_r))[a]
        behind = f - sign

        @pl.when((g - f) * sign > 0)
        def _():
            @pl.when((behind >= 0) & (behind < nf))
            def _():
                with scope("wait_rs"):
                    rs_wait(a, g)

                def add(l):
                    sent[g, at(l), :] = (sent[g, at(l), :].astype(f32) + got[g, at(l), :].astype(f32)).astype(bf)

                loop(local, add)

            rs_copy(a, g, sign).start()

    near = jnp.where(f < nf // 2, 1, -1)

    def rs_chain(a, sign, first=0):
        def steps(n):
            t = n + first
            rs_step(a, jnp.where(sign > 0, nf - 1 - t, t), sign)

        loop(nf - 1 - first, steps)

    def both(t, work):
        def side(n):
            g = f + (1 - 2 * n) * t

            @pl.when((g >= 0) & (g < nf))
            def _():
                work(g)

        loop(2, side)

    w_pass(0)
    w_done(0)
    partial_sum(0, f)
    for n in range(nf - 1):
        partial_sum(0, arriving(0, n))

    @pl.when(at_edge)
    def _():
        rs_chain(0, near)

    for n in range(1, nf - 1):
        z_pass(1, arriving(1, n))
        if n == 1:
            w_pass(1)
    w_done(1)

    @pl.when(jnp.logical_not(at_edge))
    def _():
        rs_step(0, jnp.where(near > 0, nf - 1, 0), near)

    partial_sum(1, f)
    for n in range(nf - 1):
        partial_sum(1, arriving(1, n))

    @pl.when(jnp.logical_not(at_edge))
    def _():
        rs_chain(0, near, 1)
        rs_chain(0, -near)

    rs_chain(1, near)
    rs_chain(1, -near)

    for a, got in enumerate((pre_r, prj_r)):
        for spot, edge in ((f, 0), (nf, nf - 1)):

            @pl.when(f == edge)
            def _():
                got[spot] = jnp.zeros(got.shape[1:], bf)

            @pl.when(f != edge)
            def _():
                with scope("wait_own"):
                    rs_wait(a, spot)

    def middle(l, carry):
        here = at(l)
        gate = own[here, :units] + pre_r[f, here, :units].astype(f32) + pre_r[nf, here, :units].astype(f32)
        up = own[here, units : 2 * units] + pre_r[f, here, units:].astype(f32) + pre_r[nf, here, units:].astype(f32)
        proj = own[here, 2 * units :] + prj_r[f, here, :].astype(f32) + prj_r[nf, here, :].astype(f32)
        zero, one = choose(f, (l * span).astype(f32), span)
        scale = jnp.sum(
            jnp.where(zero, codes(f, 2), 0.0) + jnp.where(one, codes(f, 3), 0.0), axis=1, keepdims=True
        )
        sig = jax.nn.sigmoid(gate)
        act = gate * sig
        hidden = act * up
        slot_gate = jnp.sum(hidden * proj, axis=1, keepdims=True)
        delta = scale * proj
        dl[l, group(f), :units] = (delta * up * sig * (1.0 + gate * (1.0 - sig))).astype(bf)
        dl[l, group(f), units : 2 * units] = (delta * act).astype(bf)
        dl[l, group(f), 2 * units :] = (scale * hidden).astype(bf)
        return (
            carry[0] + jnp.sum(jnp.where(zero, slot_gate, 0.0), axis=0, keepdims=True),
            carry[1] + jnp.sum(jnp.where(one, slot_gate, 0.0), axis=0, keepdims=True),
        )

    def ag_copy(h, g, sign, spot):
        held = dl.at[h, group(g), :]
        return put(held, held, sa.at[h, spot], ra.at[h, g], (k, e, f + sign))

    def has(sign):
        return (f + sign >= 0) & (f + sign < nf)

    def ag_first():
        held = dl.at[0, group(f), :]

        def direct(g):
            put(held, held, sa.at[0, g], ra.at[0, f], (k, e, g)).start()

        @pl.when(at_edge)
        def _():
            for t in range(nf - 1, 0, -1):
                sides(t, direct)

        @pl.when(jnp.logical_not(at_edge))
        def _():
            for t in range(1, nf):
                sides(t, direct)

    def ag_own(h):
        for sign, spot in ((1, f), (-1, nf)):

            @pl.when(has(sign))
            def _():
                ag_copy(h, f, sign, spot).start()

    def ag_step(h, t, sign):
        g = f - sign * t

        @pl.when((g >= 0) & (g < nf))
        def _():
            with scope("wait_ag"):
                ag_copy(h, g, sign, g).wait_recv()

            if h:

                @pl.when(has(sign))
                def _():
                    ag_copy(h, g, sign, g).start()

    nothing = jnp.zeros((1, ne * tcount), f32)
    parts = (nothing, nothing)
    ahead = 2
    for h in range(local):
        with scope("middle"):
            parts = middle(jnp.int32(h), parts)
        if h == 0:
            ag_first()
        elif h < ahead:
            ag_own(h)

    for ee in range(ne):
        for j in range(2):
            gg_s[ee, j : j + 1, :] = parts[j][:, ee * tcount : (ee + 1) * tcount]

    def gg_copy(de):
        return put(gg_s.at[e_at(de)], gg_r.at[de], sg_sem.at[de], rg_sem.at[de], (k, e_at(de), f))

    for de in range(1, ne):
        gg_copy(de).start()

    for de in range(1, ne):
        for g in range(nf):
            y_whole(0, g, de, e).wait_send()

    def ret_copy(g, de, kk):
        return put(
            tokb.at[g, mine(e_at(de)), cut(kk)], ret_r.at[g, de - 1, :, cut(kk)], st.at[g, de, kk],
            rt.at[g, de, kk], (k, e_at(de), f),
        )

    def slot_rows(l, g):
        with scope("slot_rows"):
            sg[g, at(l), :] = dot(dl[l, group(g), : 2 * units], weights[l, :, : 2 * units], ((1,), (1,))).astype(bf)

    def returned(g):
        with scope("returned"):

            def column(kk):
                tokb[g, :, cut(kk)] = dot(place[g], sg[g, :, cut(kk)], ((0,), (0,))).astype(bf)
                for de in range(1, ne):
                    ret_copy(g, de, kk).start()

            loop(nk, column)

    def final(g):
        with scope("final"):
            d = lax.rem(g - f + nf, nf)

            def column(kk):
                total = tokb[g, mine(e), cut(kk)].astype(f32)
                for de in range(1, ne):
                    with scope("wait_ret"):
                        ret_copy(g, de, kk).wait_recv()
                    total += ret_r[g, de - 1, :, cut(kk)].astype(f32)
                tg_s[g, :, cut(kk)] = total.astype(bf)
                there = tg_ref.at[:, strip(kk, f)]

                @pl.when(d > 0)
                def _():
                    put(tg_s.at[g, :, cut(kk)], there, so.at[d], ro.at[d], (k, e, g)).start()

                @pl.when(d == 0)
                def _():
                    pltpu.make_async_copy(tg_s.at[g, :, cut(kk)], there, own_sems.at[3]).start()

            loop(nk, column)

    def gradient(kk, l):
        ahead = dot(inp[l, :, cut(kk)], dl[l, :, : 2 * units], ((0,), (0,)))
        down = dot(ups[l, :, cut(kk)], dl[l, :, 2 * units :], ((0,), (0,)))
        return ahead, down

    def g1_copy(dx, l):
        return put(g1_out.at[dx, l], g1_in.at[dx, l], s1.at[dx, l], r1.at[dx, l], (partner, e, f))

    def g2_copy(dx, l):
        return put(g2_out.at[dx - 1, l], g2_in.at[dx - 1, l], s2.at[dx, l], r2.at[dx, l], (chip_at(dx, c), e, f))

    def to_core(l):
        with scope("to_core"):
            for dx in [*range(1, chips), 0]:
                ahead, down = gradient(chip_at(dx, 1 - c), l)
                g1_out[dx, l, :, : 2 * units] = ahead.astype(bf)
                g1_out[dx, l, :, 2 * units :] = down.astype(bf)
                g1_copy(dx, l).start()

    def summed(dx, l):
        ahead, down = gradient(chip_at(dx, c), l)
        with scope("wait_g1"):
            g1_copy(dx, l).wait_recv()
        ahead += g1_in[dx, l, :, : 2 * units].astype(f32)
        down += g1_in[dx, l, :, 2 * units :].astype(f32)
        return ahead, down

    def to_chip(l):
        with scope("to_chip"):
            for dx in range(1, chips):
                ahead, down = summed(dx, l)
                g2_out[dx - 1, l, :, : 2 * units] = ahead.astype(bf)
                g2_out[dx - 1, l, :, 2 * units :] = down.astype(bf)
                g2_copy(dx, l).start()

    def keep(l):
        ahead, down = summed(0, l)
        grad_ref[0, l] = ahead[:, :units]
        grad_ref[1, l] = ahead[:, units:]
        grad_ref[2, l] = down

    def collect(l):
        for dx in range(1, chips):
            with scope("wait_g2"):
                g2_copy(dx, l).wait_recv()
            got = g2_in[dx - 1, l].astype(f32)
            for n in range(3):
                grad_ref[n, l] += got[:, n * units : (n + 1) * units]

    def own_rows(l):
        slot_rows(l, f)

    loop(local, own_rows)
    returned(f)
    tail = 1
    head = local - tail
    for l in range(head):
        for t in range(1, nf):
            for sign in (1, -1):
                ag_step(l, t, sign)
            if t == 1 and l + ahead < local:
                ag_own(l + ahead)
        to_core(jnp.int32(l))
        for t in range(1, nf):
            both(t, functools.partial(slot_rows, jnp.int32(l)))
        to_chip(jnp.int32(l))
        if l == 0:
            final(f)
        else:
            keep(jnp.int32(l - 1))
    for t in range(1, nf):
        for l in range(head, local):
            for sign in (1, -1):
                ag_step(l, t, sign)
        if t == nf - 1:
            for l in range(head, local):
                to_core(jnp.int32(l))

        def rows_back(g):
            for l in range(head, local):
                slot_rows(jnp.int32(l), g)
            returned(g)

        both(t, rows_back)
    if not head:
        final(f)
    for n in range(max(tail, nf - 1)):
        if n < tail:
            to_chip(jnp.int32(head + n))
        if n < nf - 1:
            both(n + 1, final)
    with scope("keep"):
        for l in range(max(head - 1, 0), local):
            keep(jnp.int32(l))

    total = [gg_s[e, j : j + 1, :] for j in range(2)]
    for de in range(1, ne):
        gg_copy(de).wait_recv()
        for j in range(2):
            total[j] += gg_r[de, j : j + 1, :]
    for j in range(2):
        gg_ref[j : j + 1, :] = total[j].astype(bf)

    loop(local, collect)

    for d in range(1, nf):
        with scope("wait_tg"):
            put(tg_s.at[0], tg_s.at[0], so.at[d], ro.at[d], (k, e, f_at(d))).wait()
    pltpu.make_async_copy(tg_s.at[0], tg_s.at[0], own_sems.at[3]).wait()
    copies[1].wait()
    copies[2].wait()

    for de in range(ne):
        for d in range(nf):
            if de or d:
                info_copy(de, d).wait_send()
    for g in range(nf):

        @pl.when(f != g)
        def _():
            for a in range(2):
                z_whole(a, g).wait_send()
                rs_copy(a, g, 1).wait_send()

    for g in range(nf):

        @pl.when(f != g)
        def _():
            put(dl.at[0, group(f), :], dl.at[0, group(f), :], sa.at[0, g], ra.at[0, f], (k, e, g)).wait_send()

    for h in range(1, local):
        for g in range(nf):
            sign = jnp.where(f >= g, 1, -1)

            @pl.when(has(sign))
            def _():
                ag_copy(h, g, sign, g).wait_send()

        @pl.when(f > 0)
        def _():
            ag_copy(h, f, -1, nf).wait_send()

    for de in range(1, ne):
        gg_copy(de).wait_send()
        for g in range(nf):
            y_whole(1, g, de, e).wait_send()
            for kk in range(nk):
                ret_copy(g, de, kk).wait_send()
    for dx in range(chips):
        for a in range(2):
            w_core(a, dx, k).wait_send()
            if dx:
                w_chip(a, dx, k).wait_send()

        def sent(l):
            g1_copy(dx, l).wait_send()
            if dx:
                g2_copy(dx, l).wait_send()

        loop(local, sent)


def per_device(mesh_shape, tokens, out_grad, expert_ids, gate_probs, params, moment_first, moment_second):
    nk, ne, nf = mesh_shape["cuts"], mesh_shape["exp"], mesh_shape["fsdp"]
    token_count, width = tokens.shape
    local, rows, units = params.shape[1:]
    cap = 10 * token_count // 32
    chips = nk // CORES
    span = ne * cap
    slots = local * span
    depth = nk * rows
    bf, f32 = jnp.bfloat16, jnp.float32

    sizes = (nk, ne, nf, local, cap, token_count, rows, units)

    held = []

    def vm(*shape, kind=bf):
        held.append(math.prod(shape) * jnp.dtype(kind).itemsize)
        return pltpu.VMEM(shape, kind)

    def sem(*shape):
        return pltpu.SemaphoreType.DMA(shape)

    scratch = [
        vm(nf, ne, 8, token_count, kind=f32),
        vm(local, depth, 3 * units),
        vm(nf, ne * token_count, depth),
        vm(nf, ne * token_count, depth),
        vm(nf, slots, ne * token_count),
        vm(local, nf * span, depth),
        vm(local, nf * span, depth),
        vm(nf, slots, 2 * units),
        vm(nf, slots, units),
        vm(nf + 1, slots, 2 * units),
        vm(nf + 1, slots, units),
        vm(slots, 3 * units, kind=f32),
        vm(local, nf * span, 3 * units),
        vm(nf, slots, depth),
        vm(nf, ne - 1, token_count, depth),
        vm(nf, token_count, depth),
        vm(ne, 8, token_count, kind=f32),
        vm(ne, 8, token_count, kind=f32),
        vm(chips, local, rows, 3 * units),
        vm(chips, local, rows, 3 * units),
        vm(chips - 1, local, rows, 3 * units),
        vm(chips - 1, local, rows, 3 * units),
        sem(ne, nf), sem(ne, nf),
        sem(2, nf), sem(2, nf),
        sem(2, nf, ne), sem(2, nf, ne),
        sem(2, chips), sem(2, chips),
        sem(2, chips), sem(2, chips),
        sem(2, nf), sem(2, nf + 1),
        sem(local, nf + 1), sem(local, nf),
        sem(nf, ne, nk), sem(nf, ne, nk),
        sem(nf), sem(nf),
        sem(ne), sem(ne),
        sem(chips, local), sem(chips, local),
        sem(chips, local), sem(chips, local),
        sem(4),
    ]
    grant = sum(held) + MARGIN
    if 3 * grant > 2 * VMEM_ALL:
        grant = VMEM_ALL
    state = jax.ShapeDtypeStruct((3, local, rows, units), f32)
    vmem = pl.BlockSpec(memory_space=pltpu.VMEM)
    hbm = pl.BlockSpec(memory_space=pltpu.HBM)
    anywhere = pl.BlockSpec(memory_space=pl.ANY)
    token_grad, gates, gradient, params, moment_first, moment_second = pl.pallas_call(
        functools.partial(kernel, sizes),
        out_shape=(
            jax.ShapeDtypeStruct((token_count, width), bf),
            jax.ShapeDtypeStruct((2, token_count), bf),
            state, state, state, state,
        ),
        in_specs=[vmem, vmem, vmem, vmem, hbm, hbm, hbm],
        out_specs=(anywhere, vmem, vmem, vmem, vmem, vmem),
        scratch_shapes=scratch,
        compiler_params=pltpu.CompilerParams(
            collective_id=0, has_side_effects=True, vmem_limit_bytes=grant
        ),
    )(expert_ids.T, gate_probs.T, tokens, out_grad, params, moment_first, moment_second)
    new_params, new_first, new_second = adam_update(params, gradient, moment_first, moment_second)
    return (token_grad, gates.T, new_params, new_first, new_second)


def solution(mesh):
    tokens_spec = P(("cuts", "exp", "fsdp"), None)
    weights_spec = P(None, "exp", ("cuts", "fsdp"), None)
    return jax.shard_map(
        functools.partial(per_device, dict(mesh.shape)),
        mesh=mesh,
        in_specs=(tokens_spec,) * 4 + (weights_spec,) * 3,
        out_specs=(tokens_spec,) * 2 + (weights_spec,) * 3,
        check_vma=False,
    )
```

```python
import functools
import math

import jax
import jax.numpy as jnp
from jax import lax
from jax.experimental import pallas as pl
from jax.experimental.pallas import tpu as pltpu
from jax.sharding import PartitionSpec as P

CORES = 2
VMEM_ALL = 67043328
MARGIN = 2 * 1024 * 1024
MESH = pl.DeviceIdType.MESH

decay_first = 0.9
decay_second = 0.95
correct_first = 1.0 - 0.9**10
correct_second = 1.0 - 0.95**10
epsilon = 1e-08
learn_rate = 0.0003
weight_decay = 0.1


def adam_update(params, gradient, moment_first, moment_second):
    new_first = decay_first * moment_first + (1.0 - decay_first) * gradient
    new_second = decay_second * moment_second + (1.0 - decay_second) * gradient * gradient
    stepped = new_first / correct_first / (jnp.sqrt(new_second / correct_second) + epsilon)
    new_params = params - learn_rate * (stepped + weight_decay * params)
    return (new_params, new_first, new_second)


def loop(count, body):
    def step(i, carry):
        body(i)
        return carry

    lax.fori_loop(0, count, step, 0)


def dot(a, b, dims):
    return lax.dot_general(a, b, (dims, ((), ())), preferred_element_type=jnp.float32)


def kernel(
    sizes,
    ids_ref, gates_ref, tok_hbm, og_hbm, params_hbm, first_hbm, second_hbm,
    tg_ref, gg_ref, grad_ref, par_ref, first_ref, second_ref,
    tok_ref, og_ref, info, weights, tokb, ogb, place, inp, ups, pre_s, prj_s, pre_r, prj_r, own, dl, sg,
    ret_r, tg_s, gg_s, gg_r, g1_out, g1_in, g2_out, g2_in,
    si, ri, sz, rz, sy, ry, sw, rw, sv, rv, sp, rp, sa, ra, st, rt, so, ro, sg_sem, rg_sem, s1, r1, s2, r2,
    own_sems,
):
    nk, ne, nf, local, cap, tcount, rows, units = sizes
    chips = nk // CORES
    span = ne * cap
    slots = local * span
    bf = jnp.bfloat16
    f32 = jnp.float32
    k, e, f = lax.axis_index("cuts"), lax.axis_index("exp"), lax.axis_index("fsdp")
    x, c = k // CORES, lax.rem(k, CORES)
    scope = jax.named_scope

    def f_at(d):
        return lax.rem(f + d, nf)

    def e_at(d):
        return lax.rem(e + d, ne)

    def chip_at(d, core):
        return lax.rem(x + d, chips) * CORES + core

    partner = x * CORES + 1 - c

    def put(src, dst, send, recv, device):
        return pltpu.make_async_remote_copy(
            src_ref=src, dst_ref=dst, send_sem=send, recv_sem=recv, device_id=device, device_id_type=MESH
        )

    def strip(kk, ff):
        return pl.ds(pl.multiple_of((kk * nf + ff) * rows, rows), rows)

    def cut(kk):
        return pl.ds(pl.multiple_of(kk * rows, rows), rows)

    def mine(ee):
        return pl.ds(pl.multiple_of(ee * tcount, tcount), tcount)

    def group(g):
        return pl.ds(pl.multiple_of(g * span, span), span)

    barrier = pltpu.get_barrier_semaphore()
    partners = 0
    for de in range(ne):
        for d in range(nf):
            if de or d:
                pl.semaphore_signal(barrier, inc=1, device_id=(k, e_at(de), f_at(d)), device_id_type=MESH)
                partners += 1
    pl.semaphore_signal(barrier, inc=1, device_id=(partner, e, f), device_id_type=MESH)
    partners += 1
    for dx in range(1, chips):
        pl.semaphore_signal(barrier, inc=1, device_id=(chip_at(dx, c), e, f), device_id_type=MESH)
        partners += 1

    staged = (
        (params_hbm, par_ref), (first_hbm, first_ref), (second_hbm, second_ref), (tok_hbm, tok_ref), (og_hbm, og_ref)
    )
    copies = [pltpu.make_async_copy(src, dst, own_sems.at[n]) for n, (src, dst) in enumerate(staged)]
    for n in (0, 3, 4):
        copies[n].start()

    def iota(shape, dim):
        return lax.broadcasted_iota(jnp.int32, shape, dim)

    experts = iota((local * ne, tcount), 0)
    named = [jnp.where(experts == ids_ref[j : j + 1, :], 1.0, 0.0).astype(f32) for j in range(2)]
    earlier = jnp.where(iota((tcount, tcount), 0) < iota((tcount, tcount), 1), 1.0, 0.0).astype(bf)
    before = dot((named[0] + named[1]).astype(bf), earlier, ((1,), (0,)))
    info[f, e] = jnp.zeros((8, tcount), f32)
    for j in range(2):
        position = jnp.sum(named[j] * before, axis=0, keepdims=True)
        info[f, e, j : j + 1, :] = (ids_ref[j : j + 1, :] * span + e * cap).astype(f32) + position
        info[f, e, j + 2 : j + 3, :] = gates_ref[j : j + 1, :].astype(f32)

    copies[0].wait()
    for l in range(local):
        for n in range(3):
            weights[l, cut(k), n * units : (n + 1) * units] = par_ref[n, l].astype(bf)
    copies[3].wait()
    copies[4].wait()
    with scope("barrier"):
        pl.semaphore_wait(barrier, partners)

    def info_copy(de, d):
        mark = info.at[f, e]
        return put(mark, mark, si.at[de, d], ri.at[de, d], (k, e_at(de), f_at(d)))

    at_edge = (f == 0) | (f == nf - 1)

    def arrivals(a, place):
        if place == 0:
            return [1, *range(nf - 1, 1, -1)]
        ends = [nf - 1, 0] if a == 0 else [0, nf - 1]
        inner = sorted(set(range(1, nf - 1)) - {place}, key=lambda g: abs(g - place))
        return ends + inner

    def arriving(a, n):
        place = jnp.where(f < nf // 2, f, nf - 1 - f)
        g = jnp.int32(arrivals(a, 0)[n])
        for p in range(1, nf // 2):
            g = jnp.where(place == p, arrivals(a, p)[n], g)
        return jnp.where(f < nf // 2, g, nf - 1 - g)

    arrays = ((tok_ref, tokb), (og_ref, ogb))
    wide = (pl.ds(0, 2 * units), pl.ds(2 * units, units))

    def sides(t, work):
        for sign in (1, -1):
            g = f + sign * t

            @pl.when((g >= 0) & (g < nf))
            def _():
                work(g)

    def z_start(a, g):
        src, dst = arrays[a]
        for kk in range(nk):
            put(
                src.at[:, strip(kk, g)], dst.at[f, mine(e), cut(kk)], sz.at[a, g], rz.at[a, f], (k, e, g)
            ).start()

    def y_own_start(a):
        src, dst = arrays[a]
        for de in range(1, ne):
            for kk in range(nk):
                put(
                    src.at[:, strip(kk, f)], dst.at[f, mine(e), cut(kk)], sy.at[a, f, de], ry.at[a, f, de],
                    (k, e_at(de), f),
                ).start()

    def w_chip(a, dx, owner):
        held = weights.at[:, cut(owner), wide[a]]
        return put(held, held, sw.at[a, dx], rw.at[a, dx], (chip_at(dx, c), e, f))

    def w_core(a, dx, owner):
        held = weights.at[:, cut(owner), wide[a]]
        return put(held, held, sv.at[a, dx], rv.at[a, dx], (partner, e, f))

    def whole(dst, g, ee, send, recv, device):
        return put(dst.at[g, mine(ee), :], dst.at[g, mine(ee), :], send, recv, device)

    def z_whole(a, g):
        return whole(arrays[a][1], g, e, sz.at[a, g], rz.at[a, g], (k, e, g))

    def y_whole(a, g, de, ee):
        return whole(arrays[a][1], g, ee, sy.at[a, g, de], ry.at[a, g, de], (k, e_at(de), f))

    def z_pass(a, g):
        with scope("wait_z"):
            z_whole(a, g).wait_recv()
        for de in range(1, ne):
            y_whole(a, g, de, e).start()

    for de in range(ne):
        for d in range(nf):
            if de or d:
                info_copy(de, d).start()
    def z_starts(a, distances):
        for t in distances:
            sides(t, functools.partial(z_start, a))

    @pl.when(at_edge)
    def _():
        z_starts(0, range(nf - 1, 0, -1))
        z_starts(1, [1])

    @pl.when(jnp.logical_not(at_edge))
    def _():
        z_starts(0, range(1, nf))
        z_starts(1, range(1, nf))

    y_own_start(0)
    for a in range(2):
        for dx in range(1, chips):
            w_chip(a, dx, k).start()
        w_core(a, 0, k).start()

    copies[1].start()
    copies[2].start()
    for src, dst in arrays:
        for kk in range(nk):
            dst[f, mine(e), cut(kk)] = src[:, strip(kk, f)]

    for n in range(nf - 1):
        z_pass(0, arriving(0, n))
        if n == 0:
            y_own_start(1)

    @pl.when(at_edge)
    def _():
        z_starts(1, range(nf - 1, 1, -1))

    z_pass(1, arriving(1, 0))
    for de in range(ne):
        for d in range(nf):
            if de or d:
                info_copy(de, d).wait_recv()

    def w_pass(a):
        with scope("wait_w"):
            for dx in range(1, chips):
                owner = chip_at(chips - dx, c)
                w_chip(a, dx, owner).wait_recv()
                w_core(a, dx, owner).start()

    def w_done(a):
        with scope("wait_w2"):
            for dx in range(chips):
                w_core(a, dx, chip_at(chips - dx, 1 - c)).wait_recv()

    def codes(g, row):
        return jnp.concatenate([info[g, ee, row : row + 1, :] for ee in range(ne)], axis=1)

    first_slot = (e * slots).astype(f32)

    def choose(g, base, count):
        ids = iota((count, ne * tcount), 0).astype(f32) + base
        return [codes(g, j) - first_slot == ids for j in range(2)]

    def at(l):
        return pl.ds(pl.multiple_of(l * span, span), span)

    def picked(a, dst, g):
        src = arrays[a][1]
        for de in range(1, ne):
            with scope("wait_y"):
                y_whole(a, g, de, e_at(ne - de)).wait_recv()

        def column(kk):
            out = dot(place[g], src[g, :, cut(kk)], ((1,), (0,))).astype(bf)
            for l in range(local):
                dst[l, group(g), cut(kk)] = out[l * span : (l + 1) * span]

        loop(nk, column)

    def partial_sum(a, g):
        with scope("partial"):
            if a == 0:
                zero, one = choose(g, 0.0, slots)
                place[g] = jnp.where(zero, 1.0, 0.0).astype(bf) + jnp.where(one, 1.0, 0.0).astype(bf)
            rows_of, sums = ((inp, pre_s), (ups, prj_s))[a]
            picked(a, rows_of, g)

            def expert(l):
                out = dot(rows_of[l, group(g), :], weights[l, :, wide[a]], ((1,), (0,)))
                sums[g, at(l), :] = out.astype(bf)

                @pl.when(g == f)
                def _():
                    own[at(l), wide[a]] = out

            loop(local, expert)

    first = max(1, local // 2)
    streams = [(pre_s, pre_r, 0, local), (prj_s, prj_r, 0, first)]
    if first < local:
        streams.append((prj_s, prj_r, first, local))

    def rs_copy(a, g, sign):
        sent, got, low, high = streams[a]
        spot = jnp.where((sign < 0) & (g == f - 1), nf, g)
        these = pl.ds(low * span, (high - low) * span)
        return put(sent.at[g, these], got.at[spot, these], sp.at[a, g], rp.at[a, spot], (k, e, f + sign))

    def rs_wait(a, spot):
        _, got, low, high = streams[a]
        these = pl.ds(low * span, (high - low) * span)
        put(got.at[spot, these], got.at[spot, these], sp.at[a, 0], rp.at[a, spot], (k, e, f_at(1))).wait_recv()

    def rs_step(a, g, sign):
        sent, got, low, high = streams[a]
        behind = f - sign

        @pl.when((g - f) * sign > 0)
        def _():
            @pl.when((behind >= 0) & (behind < nf))
            def _():
                with scope("wait_rs"):
                    rs_wait(a, g)

                def add(n):
                    l = n + low
                    sent[g, at(l), :] = (sent[g, at(l), :].astype(f32) + got[g, at(l), :].astype(f32)).astype(bf)

                loop(high - low, add)

            rs_copy(a, g, sign).start()

    def rs_own(a):
        _, got, low, high = streams[a]
        for spot, edge in ((f, 0), (nf, nf - 1)):

            @pl.when(f == edge)
            def _():
                got[spot, low * span : high * span] = jnp.zeros(((high - low) * span, got.shape[2]), bf)

            @pl.when(f != edge)
            def _():
                with scope("wait_own"):
                    rs_wait(a, spot)

    near = jnp.where(f < nf // 2, 1, -1)

    def rs_chain(a, sign, first=0):
        def steps(n):
            t = n + first
            rs_step(a, jnp.where(sign > 0, nf - 1 - t, t), sign)

        loop(nf - 1 - first, steps)

    def both(t, work):
        def side(n):
            g = f + (1 - 2 * n) * t

            @pl.when((g >= 0) & (g < nf))
            def _():
                work(g)

        loop(2, side)

    w_pass(0)
    w_done(0)
    partial_sum(0, f)
    for n in range(nf - 1):
        partial_sum(0, arriving(0, n))

    @pl.when(at_edge)
    def _():
        rs_chain(0, near)

    for n in range(1, nf - 1):
        z_pass(1, arriving(1, n))
        if n == 1:
            w_pass(1)
    w_done(1)

    @pl.when(jnp.logical_not(at_edge))
    def _():
        rs_step(0, jnp.where(near > 0, nf - 1, 0), near)

    partial_sum(1, f)
    for n in range(nf - 1):
        partial_sum(1, arriving(1, n))

    @pl.when(jnp.logical_not(at_edge))
    def _():
        rs_chain(0, near, 1)
        rs_chain(0, -near)

    def middle(l, carry):
        here = at(l)
        gate = own[here, :units] + pre_r[f, here, :units].astype(f32) + pre_r[nf, here, :units].astype(f32)
        up = own[here, units : 2 * units] + pre_r[f, here, units:].astype(f32) + pre_r[nf, here, units:].astype(f32)
        proj = own[here, 2 * units :] + prj_r[f, here, :].astype(f32) + prj_r[nf, here, :].astype(f32)
        zero, one = choose(f, (l * span).astype(f32), span)
        scale = jnp.sum(
            jnp.where(zero, codes(f, 2), 0.0) + jnp.where(one, codes(f, 3), 0.0), axis=1, keepdims=True
        )
        sig = jax.nn.sigmoid(gate)
        act = gate * sig
        hidden = act * up
        slot_gate = jnp.sum(hidden * proj, axis=1, keepdims=True)
        delta = scale * proj
        dl[l, group(f), :units] = (delta * up * sig * (1.0 + gate * (1.0 - sig))).astype(bf)
        dl[l, group(f), units : 2 * units] = (delta * act).astype(bf)
        dl[l, group(f), 2 * units :] = (scale * hidden).astype(bf)
        return (
            carry[0] + jnp.sum(jnp.where(zero, slot_gate, 0.0), axis=0, keepdims=True),
            carry[1] + jnp.sum(jnp.where(one, slot_gate, 0.0), axis=0, keepdims=True),
        )

    def ag_copy(h, g, sign, spot):
        held = dl.at[h, group(g), :]
        return put(held, held, sa.at[h, spot], ra.at[h, g], (k, e, f + sign))

    def has(sign):
        return (f + sign >= 0) & (f + sign < nf)

    def ag_first():
        held = dl.at[0, group(f), :]

        def direct(g):
            put(held, held, sa.at[0, g], ra.at[0, f], (k, e, g)).start()

        @pl.when(at_edge)
        def _():
            for t in range(nf - 1, 0, -1):
                sides(t, direct)

        @pl.when(jnp.logical_not(at_edge))
        def _():
            for t in range(1, nf):
                sides(t, direct)

    def ag_own(h):
        for sign, spot in ((1, f), (-1, nf)):

            @pl.when(has(sign))
            def _():
                ag_copy(h, f, sign, spot).start()

    def ag_step(h, t, sign):
        g = f - sign * t

        @pl.when((g >= 0) & (g < nf))
        def _():
            with scope("wait_ag"):
                ag_copy(h, g, sign, g).wait_recv()

            if h:

                @pl.when(has(sign))
                def _():
                    ag_copy(h, g, sign, g).start()

    nothing = jnp.zeros((1, ne * tcount), f32)
    parts = (nothing, nothing)
    ahead = 2
    for a in range(1, len(streams)):

        @pl.when(at_edge)
        def _():
            rs_chain(a, near)

    for a in range(1, len(streams)):

        @pl.when(jnp.logical_not(at_edge))
        def _():
            rs_chain(a, near)
            rs_chain(a, -near)

        if a == 1:
            rs_own(0)
        rs_own(a)
        for h in range(*streams[a][2:]):
            with scope("middle"):
                parts = middle(jnp.int32(h), parts)
            if h == 0:
                ag_first()
            elif h < ahead:
                ag_own(h)

    for ee in range(ne):
        for j in range(2):
            gg_s[ee, j : j + 1, :] = parts[j][:, ee * tcount : (ee + 1) * tcount]

    def gg_copy(de):
        return put(gg_s.at[e_at(de)], gg_r.at[de], sg_sem.at[de], rg_sem.at[de], (k, e_at(de), f))

    for de in range(1, ne):
        gg_copy(de).start()

    for de in range(1, ne):
        for g in range(nf):
            y_whole(0, g, de, e).wait_send()

    def ret_copy(g, de, kk):
        return put(
            tokb.at[g, mine(e_at(de)), cut(kk)], ret_r.at[g, de - 1, :, cut(kk)], st.at[g, de, kk],
            rt.at[g, de, kk], (k, e_at(de), f),
        )

    def slot_rows(l, g):
        with scope("slot_rows"):
            sg[g, at(l), :] = dot(dl[l, group(g), : 2 * units], weights[l, :, : 2 * units], ((1,), (1,))).astype(bf)

    def returned(g):
        with scope("returned"):

            def column(kk):
                tokb[g, :, cut(kk)] = dot(place[g], sg[g, :, cut(kk)], ((0,), (0,))).astype(bf)
                for de in range(1, ne):
                    ret_copy(g, de, kk).start()

            loop(nk, column)

    def final(g):
        with scope("final"):
            d = lax.rem(g - f + nf, nf)

            def column(kk):
                total = tokb[g, mine(e), cut(kk)].astype(f32)
                for de in range(1, ne):
                    with scope("wait_ret"):
                        ret_copy(g, de, kk).wait_recv()
                    total += ret_r[g, de - 1, :, cut(kk)].astype(f32)
                tg_s[g, :, cut(kk)] = total.astype(bf)
                there = tg_ref.at[:, strip(kk, f)]

                @pl.when(d > 0)
                def _():
                    put(tg_s.at[g, :, cut(kk)], there, so.at[d], ro.at[d], (k, e, g)).start()

                @pl.when(d == 0)
                def _():
                    pltpu.make_async_copy(tg_s.at[g, :, cut(kk)], there, own_sems.at[5]).start()

            loop(nk, column)

    def gradient(kk, l):
        ahead = dot(inp[l, :, cut(kk)], dl[l, :, : 2 * units], ((0,), (0,)))
        down = dot(ups[l, :, cut(kk)], dl[l, :, 2 * units :], ((0,), (0,)))
        return ahead, down

    def g1_copy(dx, l):
        return put(g1_out.at[dx, l], g1_in.at[dx, l], s1.at[dx, l], r1.at[dx, l], (partner, e, f))

    def g2_copy(dx, l):
        return put(g2_out.at[dx - 1, l], g2_in.at[dx - 1, l], s2.at[dx, l], r2.at[dx, l], (chip_at(dx, c), e, f))

    def to_core(l):
        with scope("to_core"):
            for dx in [*range(1, chips), 0]:
                ahead, down = gradient(chip_at(dx, 1 - c), l)
                g1_out[dx, l, :, : 2 * units] = ahead.astype(bf)
                g1_out[dx, l, :, 2 * units :] = down.astype(bf)
                g1_copy(dx, l).start()

    def summed(dx, l):
        ahead, down = gradient(chip_at(dx, c), l)
        with scope("wait_g1"):
            g1_copy(dx, l).wait_recv()
        ahead += g1_in[dx, l, :, : 2 * units].astype(f32)
        down += g1_in[dx, l, :, 2 * units :].astype(f32)
        return ahead, down

    def to_chip(l):
        with scope("to_chip"):
            for dx in range(1, chips):
                ahead, down = summed(dx, l)
                g2_out[dx - 1, l, :, : 2 * units] = ahead.astype(bf)
                g2_out[dx - 1, l, :, 2 * units :] = down.astype(bf)
                g2_copy(dx, l).start()

    def keep(l):
        ahead, down = summed(0, l)
        grad_ref[0, l] = ahead[:, :units]
        grad_ref[1, l] = ahead[:, units:]
        grad_ref[2, l] = down

    def collect(l):
        for dx in range(1, chips):
            with scope("wait_g2"):
                g2_copy(dx, l).wait_recv()
            got = g2_in[dx - 1, l].astype(f32)
            for n in range(3):
                grad_ref[n, l] += got[:, n * units : (n + 1) * units]

    def own_rows(l):
        slot_rows(l, f)

    loop(local, own_rows)
    returned(f)
    tail = min(2, local)
    head = local - tail
    for l in range(head):
        for t in range(1, nf):
            for sign in (1, -1):
                ag_step(l, t, sign)
            if t == 1 and l + ahead < local:
                ag_own(l + ahead)
        to_core(jnp.int32(l))
        for t in range(1, nf):
            both(t, functools.partial(slot_rows, jnp.int32(l)))
        to_chip(jnp.int32(l))
        if l == 0:
            final(f)
        else:
            keep(jnp.int32(l - 1))
    for t in range(1, nf):
        for l in range(head, local):
            for sign in (1, -1):
                ag_step(l, t, sign)
            if t == nf - 1:
                to_core(jnp.int32(l))

        def rows_back(g):
            for l in range(head, local):
                slot_rows(jnp.int32(l), g)
            returned(g)

        both(t, rows_back)
        if t == nf - 1:
            to_chip(jnp.int32(head))
    if not head:
        final(f)
    both(1, final)
    for l in range(head + 1, local):
        to_chip(jnp.int32(l))
    for t in range(2, nf):
        both(t, final)
    with scope("keep"):
        for l in range(max(head - 1, 0), local):
            keep(jnp.int32(l))

    total = [gg_s[e, j : j + 1, :] for j in range(2)]
    for de in range(1, ne):
        gg_copy(de).wait_recv()
        for j in range(2):
            total[j] += gg_r[de, j : j + 1, :]
    for j in range(2):
        gg_ref[j : j + 1, :] = total[j].astype(bf)

    loop(local, collect)

    for d in range(1, nf):
        with scope("wait_tg"):
            put(tg_s.at[0], tg_s.at[0], so.at[d], ro.at[d], (k, e, f_at(d))).wait()
    pltpu.make_async_copy(tg_s.at[0], tg_s.at[0], own_sems.at[5]).wait()
    copies[1].wait()
    copies[2].wait()

    for de in range(ne):
        for d in range(nf):
            if de or d:
                info_copy(de, d).wait_send()
    for g in range(nf):

        @pl.when(f != g)
        def _():
            for a in range(2):
                z_whole(a, g).wait_send()
            for a in range(len(streams)):
                rs_copy(a, g, 1).wait_send()

    for g in range(nf):

        @pl.when(f != g)
        def _():
            put(dl.at[0, group(f), :], dl.at[0, group(f), :], sa.at[0, g], ra.at[0, f], (k, e, g)).wait_send()

    for h in range(1, local):
        for g in range(nf):
            sign = jnp.where(f >= g, 1, -1)

            @pl.when(has(sign))
            def _():
                ag_copy(h, g, sign, g).wait_send()

        @pl.when(f > 0)
        def _():
            ag_copy(h, f, -1, nf).wait_send()

    for de in range(1, ne):
        gg_copy(de).wait_send()
        for g in range(nf):
            y_whole(1, g, de, e).wait_send()
            for kk in range(nk):
                ret_copy(g, de, kk).wait_send()
    for dx in range(chips):
        for a in range(2):
            w_core(a, dx, k).wait_send()
            if dx:
                w_chip(a, dx, k).wait_send()

        def sent(l):
            g1_copy(dx, l).wait_send()
            if dx:
                g2_copy(dx, l).wait_send()

        loop(local, sent)


def per_device(mesh_shape, tokens, out_grad, expert_ids, gate_probs, params, moment_first, moment_second):
    nk, ne, nf = mesh_shape["cuts"], mesh_shape["exp"], mesh_shape["fsdp"]
    token_count, width = tokens.shape
    local, rows, units = params.shape[1:]
    cap = 10 * token_count // 32
    chips = nk // CORES
    span = ne * cap
    slots = local * span
    depth = nk * rows
    bf, f32 = jnp.bfloat16, jnp.float32

    sizes = (nk, ne, nf, local, cap, token_count, rows, units)

    held = []

    def vm(*shape, kind=bf):
        held.append(math.prod(shape) * jnp.dtype(kind).itemsize)
        return pltpu.VMEM(shape, kind)

    def sem(*shape):
        return pltpu.SemaphoreType.DMA(shape)

    scratch = [
        vm(token_count, width),
        vm(token_count, width),
        vm(nf, ne, 8, token_count, kind=f32),
        vm(local, depth, 3 * units),
        vm(nf, ne * token_count, depth),
        vm(nf, ne * token_count, depth),
        vm(nf, slots, ne * token_count),
        vm(local, nf * span, depth),
        vm(local, nf * span, depth),
        vm(nf, slots, 2 * units),
        vm(nf, slots, units),
        vm(nf + 1, slots, 2 * units),
        vm(nf + 1, slots, units),
        vm(slots, 3 * units, kind=f32),
        vm(local, nf * span, 3 * units),
        vm(nf, slots, depth),
        vm(nf, ne - 1, token_count, depth),
        vm(nf, token_count, depth),
        vm(ne, 8, token_count, kind=f32),
        vm(ne, 8, token_count, kind=f32),
        vm(chips, local, rows, 3 * units),
        vm(chips, local, rows, 3 * units),
        vm(chips - 1, local, rows, 3 * units),
        vm(chips - 1, local, rows, 3 * units),
        sem(ne, nf), sem(ne, nf),
        sem(2, nf), sem(2, nf),
        sem(2, nf, ne), sem(2, nf, ne),
        sem(2, chips), sem(2, chips),
        sem(2, chips), sem(2, chips),
        sem(3, nf), sem(3, nf + 1),
        sem(local, nf + 1), sem(local, nf),
        sem(nf, ne, nk), sem(nf, ne, nk),
        sem(nf), sem(nf),
        sem(ne), sem(ne),
        sem(chips, local), sem(chips, local),
        sem(chips, local), sem(chips, local),
        sem(6),
    ]
    grant = sum(held) + MARGIN
    if 3 * grant > 2 * VMEM_ALL:
        grant = VMEM_ALL
    state = jax.ShapeDtypeStruct((3, local, rows, units), f32)
    vmem = pl.BlockSpec(memory_space=pltpu.VMEM)
    hbm = pl.BlockSpec(memory_space=pltpu.HBM)
    anywhere = pl.BlockSpec(memory_space=pl.ANY)
    token_grad, gates, gradient, params, moment_first, moment_second = pl.pallas_call(
        functools.partial(kernel, sizes),
        out_shape=(
            jax.ShapeDtypeStruct((token_count, width), bf),
            jax.ShapeDtypeStruct((2, token_count), bf),
            state, state, state, state,
        ),
        in_specs=[vmem, vmem, hbm, hbm, hbm, hbm, hbm],
        out_specs=(anywhere, vmem, vmem, vmem, vmem, vmem),
        scratch_shapes=scratch,
        compiler_params=pltpu.CompilerParams(
            collective_id=0, has_side_effects=True, vmem_limit_bytes=grant
        ),
    )(
        expert_ids.T,
        gate_probs.T,
        *(pltpu.with_memory_space_constraint(a, pltpu.HBM) for a in (tokens, out_grad, params)),
        *(pltpu.with_memory_space_constraint(a, pltpu.HBM) for a in (moment_first, moment_second)),
    )
    new_params, new_first, new_second = adam_update(params, gradient, moment_first, moment_second)
    return (token_grad, gates.T, new_params, new_first, new_second)


def solution(mesh):
    tokens_spec = P(("cuts", "exp", "fsdp"), None)
    weights_spec = P(None, "exp", ("cuts", "fsdp"), None)
    return jax.shard_map(
        functools.partial(per_device, dict(mesh.shape)),
        mesh=mesh,
        in_specs=(tokens_spec,) * 4 + (weights_spec,) * 3,
        out_specs=(tokens_spec,) * 2 + (weights_spec,) * 3,
        check_vma=False,
    )
```

```python
import functools
import math

import jax
import jax.numpy as jnp
from jax import lax
from jax.experimental import pallas as pl
from jax.experimental.pallas import tpu as pltpu
from jax.sharding import PartitionSpec as P

CORES = 2
VMEM_ALL = 67043328
MARGIN = 2 * 1024 * 1024
MESH = pl.DeviceIdType.MESH

decay_first = 0.9
decay_second = 0.95
correct_first = 1.0 - 0.9**10
correct_second = 1.0 - 0.95**10
epsilon = 1e-08
learn_rate = 0.0003
weight_decay = 0.1


def adam_update(params, gradient, moment_first, moment_second):
    new_first = decay_first * moment_first + (1.0 - decay_first) * gradient
    new_second = decay_second * moment_second + (1.0 - decay_second) * gradient * gradient
    stepped = new_first / correct_first / (jnp.sqrt(new_second / correct_second) + epsilon)
    new_params = params - learn_rate * (stepped + weight_decay * params)
    return (new_params, new_first, new_second)


def loop(count, body):
    def step(i, carry):
        body(i)
        return carry

    lax.fori_loop(0, count, step, 0)


def dot(a, b, dims):
    return lax.dot_general(a, b, (dims, ((), ())), preferred_element_type=jnp.float32)


def kernel(
    sizes,
    ids_ref, gates_ref, tok_hbm, og_hbm, params_hbm, first_hbm, second_hbm,
    tg_ref, gg_ref, grad_ref, par_ref, first_ref, second_ref,
    tok_ref, og_ref, info, weights, tokb, ogb, place, inp, ups, pre_s, prj_s, pre_r, prj_r, own, dl, sg,
    ret_r, tg_s, gg_s, gg_r, g1_out, g1_in, g2_out, g2_in,
    si, ri, sz, rz, sy, ry, sw, rw, sv, rv, sp, rp, sa, ra, st, rt, so, ro, sg_sem, rg_sem, s1, r1, s2, r2,
    own_sems,
):
    nk, ne, nf, local, cap, tcount, rows, units = sizes
    chips = nk // CORES
    span = ne * cap
    slots = local * span
    bf = jnp.bfloat16
    f32 = jnp.float32
    k, e, f = lax.axis_index("cuts"), lax.axis_index("exp"), lax.axis_index("fsdp")
    x, c = k // CORES, lax.rem(k, CORES)
    scope = jax.named_scope

    def f_at(d):
        return lax.rem(f + d, nf)

    def e_at(d):
        return lax.rem(e + d, ne)

    def chip_at(d, core):
        return lax.rem(x + d, chips) * CORES + core

    partner = x * CORES + 1 - c

    def put(src, dst, send, recv, device):
        return pltpu.make_async_remote_copy(
            src_ref=src, dst_ref=dst, send_sem=send, recv_sem=recv, device_id=device, device_id_type=MESH
        )

    def strip(kk, ff):
        return pl.ds(pl.multiple_of((kk * nf + ff) * rows, rows), rows)

    def cut(kk):
        return pl.ds(pl.multiple_of(kk * rows, rows), rows)

    def mine(ee):
        return pl.ds(pl.multiple_of(ee * tcount, tcount), tcount)

    def group(g):
        return pl.ds(pl.multiple_of(g * span, span), span)

    barrier = pltpu.get_barrier_semaphore()
    partners = 0
    for de in range(ne):
        for d in range(nf):
            if de or d:
                pl.semaphore_signal(barrier, inc=1, device_id=(k, e_at(de), f_at(d)), device_id_type=MESH)
                partners += 1
    pl.semaphore_signal(barrier, inc=1, device_id=(partner, e, f), device_id_type=MESH)
    partners += 1
    for dx in range(1, chips):
        pl.semaphore_signal(barrier, inc=1, device_id=(chip_at(dx, c), e, f), device_id_type=MESH)
        partners += 1

    staged = (
        (params_hbm, par_ref), (first_hbm, first_ref), (second_hbm, second_ref), (tok_hbm, tok_ref), (og_hbm, og_ref)
    )
    copies = [pltpu.make_async_copy(src, dst, own_sems.at[n]) for n, (src, dst) in enumerate(staged)]
    for n in (0, 3, 4):
        copies[n].start()

    def iota(shape, dim):
        return lax.broadcasted_iota(jnp.int32, shape, dim)

    experts = iota((local * ne, tcount), 0)
    named = [jnp.where(experts == ids_ref[j : j + 1, :], 1.0, 0.0).astype(f32) for j in range(2)]
    earlier = jnp.where(iota((tcount, tcount), 0) < iota((tcount, tcount), 1), 1.0, 0.0).astype(bf)
    before = dot((named[0] + named[1]).astype(bf), earlier, ((1,), (0,)))
    info[f, e] = jnp.zeros((8, tcount), f32)
    for j in range(2):
        position = jnp.sum(named[j] * before, axis=0, keepdims=True)
        info[f, e, j : j + 1, :] = (ids_ref[j : j + 1, :] * span + e * cap).astype(f32) + position
        info[f, e, j + 2 : j + 3, :] = gates_ref[j : j + 1, :].astype(f32)

    copies[0].wait()
    for l in range(local):
        for n in range(3):
            weights[l, cut(k), n * units : (n + 1) * units] = par_ref[n, l].astype(bf)
    copies[3].wait()
    copies[4].wait()
    with scope("barrier"):
        pl.semaphore_wait(barrier, partners)

    def info_copy(de, d):
        mark = info.at[f, e]
        return put(mark, mark, si.at[de, d], ri.at[de, d], (k, e_at(de), f_at(d)))

    at_edge = (f == 0) | (f == nf - 1)

    def arrivals(a, place):
        if place == 0:
            return [1, *range(nf - 1, 1, -1)]
        ends = [nf - 1, 0] if a == 0 else [0, nf - 1]
        inner = sorted(set(range(1, nf - 1)) - {place}, key=lambda g: abs(g - place))
        return ends + inner

    def arriving(a, n):
        place = jnp.where(f < nf // 2, f, nf - 1 - f)
        g = jnp.int32(arrivals(a, 0)[n])
        for p in range(1, nf // 2):
            g = jnp.where(place == p, arrivals(a, p)[n], g)
        return jnp.where(f < nf // 2, g, nf - 1 - g)

    arrays = ((tok_ref, tokb), (og_ref, ogb))
    wide = (pl.ds(0, 2 * units), pl.ds(2 * units, units))

    def sides(t, work):
        for sign in (1, -1):
            g = f + sign * t

            @pl.when((g >= 0) & (g < nf))
            def _():
                work(g)

    def z_start(a, g):
        src, dst = arrays[a]
        for kk in range(nk):
            put(
                src.at[:, strip(kk, g)], dst.at[f, mine(e), cut(kk)], sz.at[a, g], rz.at[a, f], (k, e, g)
            ).start()

    def y_own_start(a):
        src, dst = arrays[a]
        for de in range(1, ne):
            for kk in range(nk):
                put(
                    src.at[:, strip(kk, f)], dst.at[f, mine(e), cut(kk)], sy.at[a, f, de], ry.at[a, f, de],
                    (k, e_at(de), f),
                ).start()

    def w_chip(a, dx, owner):
        held = weights.at[:, cut(owner), wide[a]]
        return put(held, held, sw.at[a, dx], rw.at[a, dx], (chip_at(dx, c), e, f))

    def w_core(a, dx, owner):
        held = weights.at[:, cut(owner), wide[a]]
        return put(held, held, sv.at[a, dx], rv.at[a, dx], (partner, e, f))

    def whole(dst, g, ee, send, recv, device):
        return put(dst.at[g, mine(ee), :], dst.at[g, mine(ee), :], send, recv, device)

    def z_whole(a, g):
        return whole(arrays[a][1], g, e, sz.at[a, g], rz.at[a, g], (k, e, g))

    def y_whole(a, g, de, ee):
        return whole(arrays[a][1], g, ee, sy.at[a, g, de], ry.at[a, g, de], (k, e_at(de), f))

    def z_pass(a, g):
        with scope("wait_z"):
            z_whole(a, g).wait_recv()
        for de in range(1, ne):
            y_whole(a, g, de, e).start()

    for de in range(ne):
        for d in range(nf):
            if de or d:
                info_copy(de, d).start()
    def z_starts(a, distances):
        for t in distances:
            sides(t, functools.partial(z_start, a))

    @pl.when(at_edge)
    def _():
        z_starts(0, range(nf - 1, 0, -1))
        z_starts(1, [1])

    @pl.when(jnp.logical_not(at_edge))
    def _():
        z_starts(0, range(1, nf))
        z_starts(1, range(1, nf))

    y_own_start(0)
    for a in range(2):
        for dx in range(1, chips):
            w_chip(a, dx, k).start()
        w_core(a, 0, k).start()

    copies[1].start()
    copies[2].start()
    for src, dst in arrays:
        for kk in range(nk):
            dst[f, mine(e), cut(kk)] = src[:, strip(kk, f)]

    for n in range(nf - 1):
        z_pass(0, arriving(0, n))
        if n == 0:
            y_own_start(1)

    @pl.when(at_edge)
    def _():
        z_starts(1, range(nf - 1, 1, -1))

    z_pass(1, arriving(1, 0))
    for de in range(ne):
        for d in range(nf):
            if de or d:
                info_copy(de, d).wait_recv()

    def w_pass(a):
        with scope("wait_w"):
            for dx in range(1, chips):
                owner = chip_at(chips - dx, c)
                w_chip(a, dx, owner).wait_recv()
                w_core(a, dx, owner).start()

    def w_done(a):
        with scope("wait_w2"):
            for dx in range(chips):
                w_core(a, dx, chip_at(chips - dx, 1 - c)).wait_recv()

    def codes(g, row):
        return jnp.concatenate([info[g, ee, row : row + 1, :] for ee in range(ne)], axis=1)

    first_slot = (e * slots).astype(f32)

    def choose(g, base, count):
        ids = iota((count, ne * tcount), 0).astype(f32) + base
        return [codes(g, j) - first_slot == ids for j in range(2)]

    def at(l):
        return pl.ds(pl.multiple_of(l * span, span), span)

    def picked(a, dst, g):
        src = arrays[a][1]
        for de in range(1, ne):
            with scope("wait_y"):
                y_whole(a, g, de, e_at(ne - de)).wait_recv()

        def column(kk):
            out = dot(place[g], src[g, :, cut(kk)], ((1,), (0,))).astype(bf)
            for l in range(local):
                dst[l, group(g), cut(kk)] = out[l * span : (l + 1) * span]

        loop(nk, column)

    def partial_sum(a, g):
        with scope("partial"):
            if a == 0:
                zero, one = choose(g, 0.0, slots)
                place[g] = jnp.where(zero, 1.0, 0.0).astype(bf) + jnp.where(one, 1.0, 0.0).astype(bf)
            rows_of, sums = ((inp, pre_s), (ups, prj_s))[a]
            picked(a, rows_of, g)

            def expert(l):
                out = dot(rows_of[l, group(g), :], weights[l, :, wide[a]], ((1,), (0,)))
                sums[g, at(l), :] = out.astype(bf)

                @pl.when(g == f)
                def _():
                    own[at(l), wide[a]] = out

            loop(local, expert)

    def rs_copy(g, sign):
        spot = jnp.where((sign < 0) & (g == f - 1), nf, g)
        return put(pre_s.at[g], pre_r.at[spot], sp.at[0, g], rp.at[0, spot], (k, e, f + sign))

    def rs_wait(spot):
        put(pre_r.at[spot], pre_r.at[spot], sp.at[0, 0], rp.at[0, spot], (k, e, f_at(1))).wait_recv()

    def rs_step(g, sign):
        behind = f - sign

        @pl.when((g - f) * sign > 0)
        def _():
            @pl.when((behind >= 0) & (behind < nf))
            def _():
                with scope("wait_rs"):
                    rs_wait(g)

                def add(l):
                    pre_s[g, at(l), :] = (pre_s[g, at(l), :].astype(f32) + pre_r[g, at(l), :].astype(f32)).astype(bf)

                loop(local, add)

            rs_copy(g, sign).start()

    def prj_copy(g):
        return put(prj_s.at[g], prj_r.at[f], sp.at[1, g], rp.at[1, f], (k, e, g))

    def prj_wait(g):
        with scope("wait_prj"):
            put(prj_r.at[g], prj_r.at[g], sp.at[1, g], rp.at[1, g], (k, e, g)).wait_recv()

    near = jnp.where(f < nf // 2, 1, -1)

    def rs_chain(sign, first=0):
        def steps(n):
            t = n + first
            rs_step(jnp.where(sign > 0, nf - 1 - t, t), sign)

        loop(nf - 1 - first, steps)

    def both(t, work):
        def side(n):
            g = f + near * (1 - 2 * n) * t

            @pl.when((g >= 0) & (g < nf))
            def _():
                work(g)

        loop(2, side)

    w_pass(0)
    w_done(0)
    partial_sum(0, f)
    for n in range(nf - 1):
        partial_sum(0, arriving(0, n))

    @pl.when(at_edge)
    def _():
        rs_chain(near)

    for n in range(1, nf - 1):
        z_pass(1, arriving(1, n))
        if n == 1:
            w_pass(1)
    w_done(1)

    @pl.when(jnp.logical_not(at_edge))
    def _():
        rs_step(jnp.where(near > 0, nf - 1, 0), near)

    partial_sum(1, f)
    for n in range(nf - 1):
        partial_sum(1, arriving(1, n))

    def prj_start(g):
        prj_copy(g).start()

    @pl.when(at_edge)
    def _():
        for t in range(nf - 1, 0, -1):
            sides(t, prj_start)

    @pl.when(jnp.logical_not(at_edge))
    def _():
        rs_chain(near, 1)
        for t in range(1, nf):
            sides(t, prj_start)
        rs_chain(-near)

    for spot, edge in ((f, 0), (nf, nf - 1)):

        @pl.when(f == edge)
        def _():
            pre_r[spot] = jnp.zeros(pre_r.shape[1:], bf)

        @pl.when(f != edge)
        def _():
            with scope("wait_own"):
                rs_wait(spot)

    for d in range(1, nf):
        prj_wait(f_at(d))

    def middle(l, carry):
        here = at(l)
        gate = own[here, :units] + pre_r[f, here, :units].astype(f32) + pre_r[nf, here, :units].astype(f32)
        up = own[here, units : 2 * units] + pre_r[f, here, units:].astype(f32) + pre_r[nf, here, units:].astype(f32)
        proj = own[here, 2 * units :]
        for d in range(1, nf):
            proj += prj_r[f_at(d), here, :].astype(f32)
        zero, one = choose(f, (l * span).astype(f32), span)
        scale = jnp.sum(
            jnp.where(zero, codes(f, 2), 0.0) + jnp.where(one, codes(f, 3), 0.0), axis=1, keepdims=True
        )
        sig = jax.nn.sigmoid(gate)
        act = gate * sig
        hidden = act * up
        slot_gate = jnp.sum(hidden * proj, axis=1, keepdims=True)
        delta = scale * proj
        dl[l, group(f), :units] = (delta * up * sig * (1.0 + gate * (1.0 - sig))).astype(bf)
        dl[l, group(f), units : 2 * units] = (delta * act).astype(bf)
        dl[l, group(f), 2 * units :] = (scale * hidden).astype(bf)
        return (
            carry[0] + jnp.sum(jnp.where(zero, slot_gate, 0.0), axis=0, keepdims=True),
            carry[1] + jnp.sum(jnp.where(one, slot_gate, 0.0), axis=0, keepdims=True),
        )

    def ag_copy(h, g, sign, spot):
        held = dl.at[h, group(g), :]
        return put(held, held, sa.at[h, spot], ra.at[h, g], (k, e, f + sign))

    def has(sign):
        return (f + sign >= 0) & (f + sign < nf)

    def ag_first():
        held = dl.at[0, group(f), :]

        def direct(g):
            put(held, held, sa.at[0, g], ra.at[0, f], (k, e, g)).start()

        @pl.when(at_edge)
        def _():
            for t in range(nf - 1, 0, -1):
                sides(t, direct)

        @pl.when(jnp.logical_not(at_edge))
        def _():
            for t in range(1, nf):
                sides(t, direct)

    def ag_own(h):
        for sign, spot in ((1, f), (-1, nf)):

            @pl.when(has(sign))
            def _():
                ag_copy(h, f, sign, spot).start()

    def ag_step(h, t, sign):
        g = f - sign * t

        @pl.when((g >= 0) & (g < nf))
        def _():
            with scope("wait_ag"):
                ag_copy(h, g, sign, g).wait_recv()

            if h:

                @pl.when(has(sign))
                def _():
                    ag_copy(h, g, sign, g).start()

    nothing = jnp.zeros((1, ne * tcount), f32)
    parts = (nothing, nothing)
    ahead = 2
    for h in range(local):
        with scope("middle"):
            parts = middle(jnp.int32(h), parts)
        if h == 0:
            ag_first()
        elif h < ahead:
            ag_own(h)

    for ee in range(ne):
        for j in range(2):
            gg_s[ee, j : j + 1, :] = parts[j][:, ee * tcount : (ee + 1) * tcount]

    def gg_copy(de):
        return put(gg_s.at[e_at(de)], gg_r.at[de], sg_sem.at[de], rg_sem.at[de], (k, e_at(de), f))

    for de in range(1, ne):
        gg_copy(de).start()

    for de in range(1, ne):
        for g in range(nf):
            y_whole(0, g, de, e).wait_send()

    def ret_copy(g, de, kk):
        return put(
            tokb.at[g, mine(e_at(de)), cut(kk)], ret_r.at[g, de - 1, :, cut(kk)], st.at[g, de, kk],
            rt.at[g, de, kk], (k, e_at(de), f),
        )

    def slot_rows(l, g):
        with scope("slot_rows"):
            sg[g, at(l), :] = dot(dl[l, group(g), : 2 * units], weights[l, :, : 2 * units], ((1,), (1,))).astype(bf)

    def returned(g):
        with scope("returned"):

            def column(kk):
                tokb[g, :, cut(kk)] = dot(place[g], sg[g, :, cut(kk)], ((0,), (0,))).astype(bf)
                for de in range(1, ne):
                    ret_copy(g, de, kk).start()

            loop(nk, column)

    def final(g):
        with scope("final"):
            d = lax.rem(g - f + nf, nf)

            def column(kk):
                total = tokb[g, mine(e), cut(kk)].astype(f32)
                for de in range(1, ne):
                    with scope("wait_ret"):
                        ret_copy(g, de, kk).wait_recv()
                    total += ret_r[g, de - 1, :, cut(kk)].astype(f32)
                tg_s[g, :, cut(kk)] = total.astype(bf)
                there = tg_ref.at[:, strip(kk, f)]

                @pl.when(d > 0)
                def _():
                    put(tg_s.at[g, :, cut(kk)], there, so.at[d], ro.at[d], (k, e, g)).start()

                @pl.when(d == 0)
                def _():
                    pltpu.make_async_copy(tg_s.at[g, :, cut(kk)], there, own_sems.at[5]).start()

            loop(nk, column)

    def gradient(kk, l):
        ahead = dot(inp[l, :, cut(kk)], dl[l, :, : 2 * units], ((0,), (0,)))
        down = dot(ups[l, :, cut(kk)], dl[l, :, 2 * units :], ((0,), (0,)))
        return ahead, down

    def g1_copy(dx, l):
        return put(g1_out.at[dx, l], g1_in.at[dx, l], s1.at[dx, l], r1.at[dx, l], (partner, e, f))

    def g2_copy(dx, l):
        return put(g2_out.at[dx - 1, l], g2_in.at[dx - 1, l], s2.at[dx, l], r2.at[dx, l], (chip_at(dx, c), e, f))

    def to_core(l):
        with scope("to_core"):
            for dx in [*range(1, chips), 0]:
                ahead, down = gradient(chip_at(dx, 1 - c), l)
                g1_out[dx, l, :, : 2 * units] = ahead.astype(bf)
                g1_out[dx, l, :, 2 * units :] = down.astype(bf)
                g1_copy(dx, l).start()

    def summed(dx, l):
        ahead, down = gradient(chip_at(dx, c), l)
        with scope("wait_g1"):
            g1_copy(dx, l).wait_recv()
        ahead += g1_in[dx, l, :, : 2 * units].astype(f32)
        down += g1_in[dx, l, :, 2 * units :].astype(f32)
        return ahead, down

    def to_chip(l):
        with scope("to_chip"):
            for dx in range(1, chips):
                ahead, down = summed(dx, l)
                g2_out[dx - 1, l, :, : 2 * units] = ahead.astype(bf)
                g2_out[dx - 1, l, :, 2 * units :] = down.astype(bf)
                g2_copy(dx, l).start()

    def keep(l):
        ahead, down = summed(0, l)
        grad_ref[0, l] = ahead[:, :units]
        grad_ref[1, l] = ahead[:, units:]
        grad_ref[2, l] = down

    def collect(l):
        for dx in range(1, chips):
            with scope("wait_g2"):
                g2_copy(dx, l).wait_recv()
            got = g2_in[dx - 1, l].astype(f32)
            for n in range(3):
                grad_ref[n, l] += got[:, n * units : (n + 1) * units]

    def own_rows(l):
        slot_rows(l, f)

    loop(local, own_rows)
    returned(f)
    tail = min(2, local)
    head = local - tail
    for l in range(head):
        for t in range(1, nf):
            for sign in (1, -1):
                ag_step(l, t, sign)
            if t == 1 and l + ahead < local:
                ag_own(l + ahead)
        to_core(jnp.int32(l))
        for t in range(1, nf):
            both(t, functools.partial(slot_rows, jnp.int32(l)))
        to_chip(jnp.int32(l))
        if l == 0:
            final(f)
        else:
            keep(jnp.int32(l - 1))
    for t in range(1, nf):
        for l in range(head, local):
            for sign in (1, -1):
                ag_step(l, t, sign)
            if t == nf - 1:
                to_core(jnp.int32(l))

        def rows_back(g):
            for l in range(head, local):
                slot_rows(jnp.int32(l), g)
            returned(g)

        if t == nf - 1:
            to_chip(jnp.int32(head))
        both(t, rows_back)
    if not head:
        final(f)
    for l in range(head + 1, local):
        to_chip(jnp.int32(l))

    @pl.when(at_edge)
    def _():
        for t in [*range(2, nf - 1), 1, nf - 1]:
            both(t, final)

    @pl.when(jnp.logical_not(at_edge))
    def _():
        for t in range(1, nf):
            both(t, final)

    with scope("keep"):
        for l in range(max(head - 1, 0), local):
            keep(jnp.int32(l))

    total = [gg_s[e, j : j + 1, :] for j in range(2)]
    for de in range(1, ne):
        gg_copy(de).wait_recv()
        for j in range(2):
            total[j] += gg_r[de, j : j + 1, :]
    for j in range(2):
        gg_ref[j : j + 1, :] = total[j].astype(bf)

    loop(local, collect)

    for d in range(1, nf):
        with scope("wait_tg"):
            put(tg_s.at[0], tg_s.at[0], so.at[d], ro.at[d], (k, e, f_at(d))).wait()
    pltpu.make_async_copy(tg_s.at[0], tg_s.at[0], own_sems.at[5]).wait()
    copies[1].wait()
    copies[2].wait()

    for de in range(ne):
        for d in range(nf):
            if de or d:
                info_copy(de, d).wait_send()
    for g in range(nf):

        @pl.when(f != g)
        def _():
            for a in range(2):
                z_whole(a, g).wait_send()
            rs_copy(g, 1).wait_send()
            prj_copy(g).wait_send()

    for g in range(nf):

        @pl.when(f != g)
        def _():
            put(dl.at[0, group(f), :], dl.at[0, group(f), :], sa.at[0, g], ra.at[0, f], (k, e, g)).wait_send()

    for h in range(1, local):
        for g in range(nf):
            sign = jnp.where(f >= g, 1, -1)

            @pl.when(has(sign))
            def _():
                ag_copy(h, g, sign, g).wait_send()

        @pl.when(f > 0)
        def _():
            ag_copy(h, f, -1, nf).wait_send()

    for de in range(1, ne):
        gg_copy(de).wait_send()
        for g in range(nf):
            y_whole(1, g, de, e).wait_send()
            for kk in range(nk):
                ret_copy(g, de, kk).wait_send()
    for dx in range(chips):
        for a in range(2):
            w_core(a, dx, k).wait_send()
            if dx:
                w_chip(a, dx, k).wait_send()

        def sent(l):
            g1_copy(dx, l).wait_send()
            if dx:
                g2_copy(dx, l).wait_send()

        loop(local, sent)


def per_device(mesh_shape, tokens, out_grad, expert_ids, gate_probs, params, moment_first, moment_second):
    nk, ne, nf = mesh_shape["cuts"], mesh_shape["exp"], mesh_shape["fsdp"]
    token_count, width = tokens.shape
    local, rows, units = params.shape[1:]
    cap = 10 * token_count // 32
    chips = nk // CORES
    span = ne * cap
    slots = local * span
    depth = nk * rows
    bf, f32 = jnp.bfloat16, jnp.float32

    sizes = (nk, ne, nf, local, cap, token_count, rows, units)

    held = []

    def vm(*shape, kind=bf):
        held.append(math.prod(shape) * jnp.dtype(kind).itemsize)
        return pltpu.VMEM(shape, kind)

    def sem(*shape):
        return pltpu.SemaphoreType.DMA(shape)

    scratch = [
        vm(token_count, width),
        vm(token_count, width),
        vm(nf, ne, 8, token_count, kind=f32),
        vm(local, depth, 3 * units),
        vm(nf, ne * token_count, depth),
        vm(nf, ne * token_count, depth),
        vm(nf, slots, ne * token_count),
        vm(local, nf * span, depth),
        vm(local, nf * span, depth),
        vm(nf, slots, 2 * units),
        vm(nf, slots, units),
        vm(nf + 1, slots, 2 * units),
        vm(nf, slots, units),
        vm(slots, 3 * units, kind=f32),
        vm(local, nf * span, 3 * units),
        vm(nf, slots, depth),
        vm(nf, ne - 1, token_count, depth),
        vm(nf, token_count, depth),
        vm(ne, 8, token_count, kind=f32),
        vm(ne, 8, token_count, kind=f32),
        vm(chips, local, rows, 3 * units),
        vm(chips, local, rows, 3 * units),
        vm(chips - 1, local, rows, 3 * units),
        vm(chips - 1, local, rows, 3 * units),
        sem(ne, nf), sem(ne, nf),
        sem(2, nf), sem(2, nf),
        sem(2, nf, ne), sem(2, nf, ne),
        sem(2, chips), sem(2, chips),
        sem(2, chips), sem(2, chips),
        sem(2, nf), sem(2, nf + 1),
        sem(local, nf + 1), sem(local, nf),
        sem(nf, ne, nk), sem(nf, ne, nk),
        sem(nf), sem(nf),
        sem(ne), sem(ne),
        sem(chips, local), sem(chips, local),
        sem(chips, local), sem(chips, local),
        sem(6),
    ]
    grant = sum(held) + MARGIN
    if 3 * grant > 2 * VMEM_ALL:
        grant = VMEM_ALL
    state = jax.ShapeDtypeStruct((3, local, rows, units), f32)
    vmem = pl.BlockSpec(memory_space=pltpu.VMEM)
    hbm = pl.BlockSpec(memory_space=pltpu.HBM)
    anywhere = pl.BlockSpec(memory_space=pl.ANY)
    token_grad, gates, gradient, params, moment_first, moment_second = pl.pallas_call(
        functools.partial(kernel, sizes),
        out_shape=(
            jax.ShapeDtypeStruct((token_count, width), bf),
            jax.ShapeDtypeStruct((2, token_count), bf),
            state, state, state, state,
        ),
        in_specs=[vmem, vmem, hbm, hbm, hbm, hbm, hbm],
        out_specs=(anywhere, vmem, vmem, vmem, vmem, vmem),
        scratch_shapes=scratch,
        compiler_params=pltpu.CompilerParams(
            collective_id=0, has_side_effects=True, vmem_limit_bytes=grant
        ),
    )(
        expert_ids.T,
        gate_probs.T,
        *(pltpu.with_memory_space_constraint(a, pltpu.HBM) for a in (tokens, out_grad, params)),
        *(pltpu.with_memory_space_constraint(a, pltpu.HBM) for a in (moment_first, moment_second)),
    )
    new_params, new_first, new_second = adam_update(params, gradient, moment_first, moment_second)
    return (token_grad, gates.T, new_params, new_first, new_second)


def solution(mesh):
    tokens_spec = P(("cuts", "exp", "fsdp"), None)
    weights_spec = P(None, "exp", ("cuts", "fsdp"), None)
    return jax.shard_map(
        functools.partial(per_device, dict(mesh.shape)),
        mesh=mesh,
        in_specs=(tokens_spec,) * 4 + (weights_spec,) * 3,
        out_specs=(tokens_spec,) * 2 + (weights_spec,) * 3,
        check_vma=False,
    )
```

```python
import functools
import math

import jax
import jax.numpy as jnp
from jax import lax
from jax.experimental import pallas as pl
from jax.experimental.pallas import tpu as pltpu
from jax.sharding import PartitionSpec as P

CORES = 2
VMEM_ALL = 67043328
MARGIN = 2 * 1024 * 1024
MESH = pl.DeviceIdType.MESH

decay_first = 0.9
decay_second = 0.95
correct_first = 1.0 - 0.9**10
correct_second = 1.0 - 0.95**10
epsilon = 1e-08
learn_rate = 0.0003
weight_decay = 0.1


def adam_update(params, gradient, moment_first, moment_second):
    new_first = decay_first * moment_first + (1.0 - decay_first) * gradient
    new_second = decay_second * moment_second + (1.0 - decay_second) * gradient * gradient
    stepped = new_first / correct_first / (jnp.sqrt(new_second / correct_second) + epsilon)
    new_params = params - learn_rate * (stepped + weight_decay * params)
    return (new_params, new_first, new_second)


def loop(count, body):
    def step(i, carry):
        body(i)
        return carry

    lax.fori_loop(0, count, step, 0)


def dot(a, b, dims):
    return lax.dot_general(a, b, (dims, ((), ())), preferred_element_type=jnp.float32)


def kernel(
    sizes,
    ids_ref, gates_ref, tok_hbm, og_hbm, params_hbm, first_hbm, second_hbm,
    tg_ref, gg_ref, grad_ref, par_ref, first_ref, second_ref,
    tok_ref, og_ref, info, weights, tokb, ogb, place, inp, ups, pre_s, prj_s, pre_r, prj_r, own, dl, sg,
    ret_r, tg_s, gg_s, gg_r, g1_out, g1_in, g2_out, g2_in,
    si, ri, sz, rz, sy, ry, sw, rw, sv, rv, sp, rp, sa, ra, st, rt, so, ro, sg_sem, rg_sem, s1, r1, s2, r2,
    own_sems,
):
    nk, ne, nf, local, cap, tcount, rows, units = sizes
    chips = nk // CORES
    span = ne * cap
    slots = local * span
    bf = jnp.bfloat16
    f32 = jnp.float32
    k, e, f = lax.axis_index("cuts"), lax.axis_index("exp"), lax.axis_index("fsdp")
    x, c = k // CORES, lax.rem(k, CORES)
    scope = jax.named_scope

    def f_at(d):
        return lax.rem(f + d, nf)

    def e_at(d):
        return lax.rem(e + d, ne)

    def chip_at(d, core):
        return lax.rem(x + d, chips) * CORES + core

    partner = x * CORES + 1 - c

    def put(src, dst, send, recv, device):
        return pltpu.make_async_remote_copy(
            src_ref=src, dst_ref=dst, send_sem=send, recv_sem=recv, device_id=device, device_id_type=MESH
        )

    def strip(kk, ff):
        return pl.ds(pl.multiple_of((kk * nf + ff) * rows, rows), rows)

    def cut(kk):
        return pl.ds(pl.multiple_of(kk * rows, rows), rows)

    def mine(ee):
        return pl.ds(pl.multiple_of(ee * tcount, tcount), tcount)

    def group(g):
        return pl.ds(pl.multiple_of(g * span, span), span)

    barrier = pltpu.get_barrier_semaphore()
    partners = 0
    for de in range(ne):
        for d in range(nf):
            if de or d:
                pl.semaphore_signal(barrier, inc=1, device_id=(k, e_at(de), f_at(d)), device_id_type=MESH)
                partners += 1
    pl.semaphore_signal(barrier, inc=1, device_id=(partner, e, f), device_id_type=MESH)
    partners += 1
    for dx in range(1, chips):
        pl.semaphore_signal(barrier, inc=1, device_id=(chip_at(dx, c), e, f), device_id_type=MESH)
        partners += 1

    staged = (
        (params_hbm, par_ref), (first_hbm, first_ref), (second_hbm, second_ref), (tok_hbm, tok_ref), (og_hbm, og_ref)
    )
    copies = [pltpu.make_async_copy(src, dst, own_sems.at[n]) for n, (src, dst) in enumerate(staged)]
    for n in (0, 3, 4):
        copies[n].start()

    def iota(shape, dim):
        return lax.broadcasted_iota(jnp.int32, shape, dim)

    experts = iota((local * ne, tcount), 0)
    named = [jnp.where(experts == ids_ref[j : j + 1, :], 1.0, 0.0).astype(f32) for j in range(2)]
    earlier = jnp.where(iota((tcount, tcount), 0) < iota((tcount, tcount), 1), 1.0, 0.0).astype(bf)
    before = dot((named[0] + named[1]).astype(bf), earlier, ((1,), (0,)))
    info[f, e] = jnp.zeros((8, tcount), f32)
    for j in range(2):
        position = jnp.sum(named[j] * before, axis=0, keepdims=True)
        info[f, e, j : j + 1, :] = (ids_ref[j : j + 1, :] * span + e * cap).astype(f32) + position
        info[f, e, j + 2 : j + 3, :] = gates_ref[j : j + 1, :].astype(f32)

    copies[0].wait()
    for l in range(local):
        for n in range(3):
            weights[l, cut(k), n * units : (n + 1) * units] = par_ref[n, l].astype(bf)
    copies[3].wait()
    copies[4].wait()
    with scope("barrier"):
        pl.semaphore_wait(barrier, partners)

    def info_copy(de, d):
        mark = info.at[f, e]
        return put(mark, mark, si.at[de, d], ri.at[de, d], (k, e_at(de), f_at(d)))

    at_edge = (f == 0) | (f == nf - 1)

    def arrivals(a, place):
        if place == 0:
            return [nf - 1, 1, *range(nf - 2, 1, -1)] if a == 0 else [1, *range(nf - 1, 1, -1)]
        ends = [nf - 1, 0] if a == 0 else [0, nf - 1]
        inner = sorted(set(range(1, nf - 1)) - {place}, key=lambda g: abs(g - place))
        return ends + inner

    def arriving(a, n):
        place = jnp.where(f < nf // 2, f, nf - 1 - f)
        g = jnp.int32(arrivals(a, 0)[n])
        for p in range(1, nf // 2):
            g = jnp.where(place == p, arrivals(a, p)[n], g)
        return jnp.where(f < nf // 2, g, nf - 1 - g)

    arrays = ((tok_ref, tokb), (og_ref, ogb))
    wide = (pl.ds(0, 2 * units), pl.ds(2 * units, units))

    def sides(t, work):
        for sign in (1, -1):
            g = f + sign * t

            @pl.when((g >= 0) & (g < nf))
            def _():
                work(g)

    def z_start(a, g):
        src, dst = arrays[a]
        for kk in range(nk):
            put(
                src.at[:, strip(kk, g)], dst.at[f, mine(e), cut(kk)], sz.at[a, g], rz.at[a, f], (k, e, g)
            ).start()

    def y_own_start(a):
        src, dst = arrays[a]
        for de in range(1, ne):
            for kk in range(nk):
                put(
                    src.at[:, strip(kk, f)], dst.at[f, mine(e), cut(kk)], sy.at[a, f, de], ry.at[a, f, de],
                    (k, e_at(de), f),
                ).start()

    def w_chip(a, dx, owner):
        held = weights.at[:, cut(owner), wide[a]]
        return put(held, held, sw.at[a, dx], rw.at[a, dx], (chip_at(dx, c), e, f))

    def w_core(a, dx, owner):
        held = weights.at[:, cut(owner), wide[a]]
        return put(held, held, sv.at[a, dx], rv.at[a, dx], (partner, e, f))

    def whole(dst, g, ee, send, recv, device):
        return put(dst.at[g, mine(ee), :], dst.at[g, mine(ee), :], send, recv, device)

    def z_whole(a, g):
        return whole(arrays[a][1], g, e, sz.at[a, g], rz.at[a, g], (k, e, g))

    def y_whole(a, g, de, ee):
        return whole(arrays[a][1], g, ee, sy.at[a, g, de], ry.at[a, g, de], (k, e_at(de), f))

    def z_pass(a, g):
        with scope("wait_z"):
            z_whole(a, g).wait_recv()
        for de in range(1, ne):
            y_whole(a, g, de, e).start()

    for de in range(ne):
        for d in range(nf):
            if de or d:
                info_copy(de, d).start()
    def z_starts(a, distances):
        for t in distances:
            sides(t, functools.partial(z_start, a))

    @pl.when(at_edge)
    def _():
        z_starts(0, range(nf - 1, 0, -1))
        z_starts(1, [1])

    @pl.when(jnp.logical_not(at_edge))
    def _():
        z_starts(0, range(1, nf))
        z_starts(1, range(1, nf))

    y_own_start(0)
    y_own_start(1)
    for a in range(2):
        for dx in range(1, chips):
            w_chip(a, dx, k).start()
        w_core(a, 0, k).start()

    copies[1].start()
    copies[2].start()
    for src, dst in arrays:
        for kk in range(nk):
            dst[f, mine(e), cut(kk)] = src[:, strip(kk, f)]

    for n in range(nf - 1):
        z_pass(0, arriving(0, n))

    @pl.when(at_edge)
    def _():
        z_starts(1, range(nf - 1, 1, -1))

    z_pass(1, arriving(1, 0))
    for de in range(ne):
        for d in range(nf):
            if de or d:
                info_copy(de, d).wait_recv()

    def w_pass(a):
        with scope("wait_w"):
            for dx in range(1, chips):
                owner = chip_at(chips - dx, c)
                w_chip(a, dx, owner).wait_recv()
                w_core(a, dx, owner).start()

    def w_done(a):
        with scope("wait_w2"):
            for dx in range(chips):
                w_core(a, dx, chip_at(chips - dx, 1 - c)).wait_recv()

    def codes(g, row):
        return jnp.concatenate([info[g, ee, row : row + 1, :] for ee in range(ne)], axis=1)

    first_slot = (e * slots).astype(f32)

    def choose(g, base, count):
        ids = iota((count, ne * tcount), 0).astype(f32) + base
        return [codes(g, j) - first_slot == ids for j in range(2)]

    def at(l):
        return pl.ds(pl.multiple_of(l * span, span), span)

    def picked(a, dst, g):
        src = arrays[a][1]
        for de in range(1, ne):
            with scope("wait_y"):
                y_whole(a, g, de, e_at(ne - de)).wait_recv()

        def column(kk):
            out = dot(place[g], src[g, :, cut(kk)], ((1,), (0,))).astype(bf)
            for l in range(local):
                dst[l, group(g), cut(kk)] = out[l * span : (l + 1) * span]

        loop(nk, column)

    def partial_sum(a, g):
        with scope("partial"):
            if a == 0:
                zero, one = choose(g, 0.0, slots)
                place[g] = jnp.where(zero, 1.0, 0.0).astype(bf) + jnp.where(one, 1.0, 0.0).astype(bf)
            rows_of, sums = ((inp, pre_s), (ups, prj_s))[a]
            picked(a, rows_of, g)

            def expert(l):
                out = dot(rows_of[l, group(g), :], weights[l, :, wide[a]], ((1,), (0,)))
                sums[g, at(l), :] = out.astype(bf)

                @pl.when(g == f)
                def _():
                    own[at(l), wide[a]] = out

            loop(local, expert)

    def rs_copy(g, sign):
        spot = jnp.where((sign < 0) & (g == f - 1), nf, g)
        return put(pre_s.at[g], pre_r.at[spot], sp.at[0, g], rp.at[0, spot], (k, e, f + sign))

    def rs_wait(spot):
        put(pre_r.at[spot], pre_r.at[spot], sp.at[0, 0], rp.at[0, spot], (k, e, f_at(1))).wait_recv()

    def rs_step(g, sign):
        behind = f - sign

        @pl.when((g - f) * sign > 0)
        def _():
            @pl.when((behind >= 0) & (behind < nf))
            def _():
                with scope("wait_rs"):
                    rs_wait(g)

                def add(l):
                    pre_s[g, at(l), :] = (pre_s[g, at(l), :].astype(f32) + pre_r[g, at(l), :].astype(f32)).astype(bf)

                loop(local, add)

            rs_copy(g, sign).start()

    def prj_copy(g):
        return put(prj_s.at[g], prj_r.at[f], sp.at[1, g], rp.at[1, f], (k, e, g))

    def prj_wait(g):
        with scope("wait_prj"):
            put(prj_r.at[g], prj_r.at[g], sp.at[1, g], rp.at[1, g], (k, e, g)).wait_recv()

    near = jnp.where(f < nf // 2, 1, -1)

    def rs_chain(sign, first=0):
        def steps(n):
            t = n + first
            rs_step(jnp.where(sign > 0, nf - 1 - t, t), sign)

        loop(nf - 1 - first, steps)

    def both(t, work):
        def side(n):
            g = f + near * (1 - 2 * n) * t

            @pl.when((g >= 0) & (g < nf))
            def _():
                work(g)

        loop(2, side)

    w_pass(0)
    w_done(0)
    partial_sum(0, f)
    for n in range(nf - 1):
        partial_sum(0, arriving(0, n))

    @pl.when(at_edge)
    def _():
        rs_chain(near)

    for n in range(1, nf - 1):
        z_pass(1, arriving(1, n))
        if n == 1:
            w_pass(1)
    w_done(1)

    @pl.when(jnp.logical_not(at_edge))
    def _():
        rs_step(jnp.where(near > 0, nf - 1, 0), near)

    partial_sum(1, f)
    def prj_start(g):
        prj_copy(g).start()

    for n in range(nf - 1):
        partial_sum(1, arriving(1, n))

        @pl.when(jnp.logical_not(at_edge))
        def _():
            prj_start(arriving(1, n))
            if n == 1:
                rs_chain(near, 1)


    @pl.when(at_edge)
    def _():
        for t in range(nf - 1, 0, -1):
            sides(t, prj_start)

    @pl.when(jnp.logical_not(at_edge))
    def _():
        rs_chain(-near)

    for spot, edge in ((f, 0), (nf, nf - 1)):

        @pl.when(f == edge)
        def _():
            pre_r[spot] = jnp.zeros(pre_r.shape[1:], bf)

        @pl.when(f != edge)
        def _():
            with scope("wait_own"):
                rs_wait(spot)

    for d in range(1, nf):
        prj_wait(f_at(d))

    def middle(l, carry):
        here = at(l)
        gate = own[here, :units] + pre_r[f, here, :units].astype(f32) + pre_r[nf, here, :units].astype(f32)
        up = own[here, units : 2 * units] + pre_r[f, here, units:].astype(f32) + pre_r[nf, here, units:].astype(f32)
        proj = own[here, 2 * units :]
        for d in range(1, nf):
            proj += prj_r[f_at(d), here, :].astype(f32)
        zero, one = choose(f, (l * span).astype(f32), span)
        scale = jnp.sum(
            jnp.where(zero, codes(f, 2), 0.0) + jnp.where(one, codes(f, 3), 0.0), axis=1, keepdims=True
        )
        sig = jax.nn.sigmoid(gate)
        act = gate * sig
        hidden = act * up
        slot_gate = jnp.sum(hidden * proj, axis=1, keepdims=True)
        delta = scale * proj
        dl[l, group(f), :units] = (delta * up * sig * (1.0 + gate * (1.0 - sig))).astype(bf)
        dl[l, group(f), units : 2 * units] = (delta * act).astype(bf)
        dl[l, group(f), 2 * units :] = (scale * hidden).astype(bf)
        return (
            carry[0] + jnp.sum(jnp.where(zero, slot_gate, 0.0), axis=0, keepdims=True),
            carry[1] + jnp.sum(jnp.where(one, slot_gate, 0.0), axis=0, keepdims=True),
        )

    def ag_copy(h, g, sign, spot):
        held = dl.at[h, group(g), :]
        return put(held, held, sa.at[h, spot], ra.at[h, g], (k, e, f + sign))

    def has(sign):
        return (f + sign >= 0) & (f + sign < nf)

    def ag_first():
        held = dl.at[0, group(f), :]

        def direct(g):
            put(held, held, sa.at[0, g], ra.at[0, f], (k, e, g)).start()

        @pl.when(at_edge)
        def _():
            for t in range(nf - 1, 0, -1):
                sides(t, direct)

        @pl.when(jnp.logical_not(at_edge))
        def _():
            for t in range(1, nf):
                sides(t, direct)

    def ag_own(h):
        for sign, spot in ((1, f), (-1, nf)):

            @pl.when(has(sign))
            def _():
                ag_copy(h, f, sign, spot).start()

    def ag_step(h, t, sign):
        g = f - sign * t

        @pl.when((g >= 0) & (g < nf))
        def _():
            with scope("wait_ag"):
                ag_copy(h, g, sign, g).wait_recv()

            if h:

                @pl.when(has(sign))
                def _():
                    ag_copy(h, g, sign, g).start()

    nothing = jnp.zeros((1, ne * tcount), f32)
    parts = (nothing, nothing)
    ahead = 2
    for h in range(local):
        with scope("middle"):
            parts = middle(jnp.int32(h), parts)
        if h == 0:
            ag_first()
        elif h < ahead:
            ag_own(h)

    for ee in range(ne):
        for j in range(2):
            gg_s[ee, j : j + 1, :] = parts[j][:, ee * tcount : (ee + 1) * tcount]

    def gg_copy(de):
        return put(gg_s.at[e_at(de)], gg_r.at[de], sg_sem.at[de], rg_sem.at[de], (k, e_at(de), f))

    for de in range(1, ne):
        gg_copy(de).start()

    for de in range(1, ne):
        for g in range(nf):
            y_whole(0, g, de, e).wait_send()

    def ret_copy(g, de, kk):
        return put(
            tokb.at[g, mine(e_at(de)), cut(kk)], ret_r.at[g, de - 1, :, cut(kk)], st.at[g, de, kk],
            rt.at[g, de, kk], (k, e_at(de), f),
        )

    def slot_rows(l, g):
        with scope("slot_rows"):
            sg[g, at(l), :] = dot(dl[l, group(g), : 2 * units], weights[l, :, : 2 * units], ((1,), (1,))).astype(bf)

    def returned(g):
        with scope("returned"):

            def column(kk):
                tokb[g, :, cut(kk)] = dot(place[g], sg[g, :, cut(kk)], ((0,), (0,))).astype(bf)
                for de in range(1, ne):
                    ret_copy(g, de, kk).start()

            loop(nk, column)

    def final(g):
        with scope("final"):
            d = lax.rem(g - f + nf, nf)

            def column(kk):
                total = tokb[g, mine(e), cut(kk)].astype(f32)
                for de in range(1, ne):
                    with scope("wait_ret"):
                        ret_copy(g, de, kk).wait_recv()
                    total += ret_r[g, de - 1, :, cut(kk)].astype(f32)
                tg_s[g, :, cut(kk)] = total.astype(bf)
                there = tg_ref.at[:, strip(kk, f)]

                @pl.when(d > 0)
                def _():
                    put(tg_s.at[g, :, cut(kk)], there, so.at[d], ro.at[d], (k, e, g)).start()

                @pl.when(d == 0)
                def _():
                    pltpu.make_async_copy(tg_s.at[g, :, cut(kk)], there, own_sems.at[5]).start()

            loop(nk, column)

    def gradient(kk, l):
        ahead = dot(inp[l, :, cut(kk)], dl[l, :, : 2 * units], ((0,), (0,)))
        down = dot(ups[l, :, cut(kk)], dl[l, :, 2 * units :], ((0,), (0,)))
        return ahead, down

    def g1_copy(dx, l):
        return put(g1_out.at[dx, l], g1_in.at[dx, l], s1.at[dx, l], r1.at[dx, l], (partner, e, f))

    def g2_copy(dx, l):
        return put(g2_out.at[dx - 1, l], g2_in.at[dx - 1, l], s2.at[dx, l], r2.at[dx, l], (chip_at(dx, c), e, f))

    def to_core(l):
        with scope("to_core"):
            for dx in [*range(1, chips), 0]:
                ahead, down = gradient(chip_at(dx, 1 - c), l)
                g1_out[dx, l, :, : 2 * units] = ahead.astype(bf)
                g1_out[dx, l, :, 2 * units :] = down.astype(bf)
                g1_copy(dx, l).start()

    def summed(dx, l):
        ahead, down = gradient(chip_at(dx, c), l)
        with scope("wait_g1"):
            g1_copy(dx, l).wait_recv()
        ahead += g1_in[dx, l, :, : 2 * units].astype(f32)
        down += g1_in[dx, l, :, 2 * units :].astype(f32)
        return ahead, down

    def to_chip(l):
        with scope("to_chip"):
            for dx in range(1, chips):
                ahead, down = summed(dx, l)
                g2_out[dx - 1, l, :, : 2 * units] = ahead.astype(bf)
                g2_out[dx - 1, l, :, 2 * units :] = down.astype(bf)
                g2_copy(dx, l).start()

    def keep(l):
        ahead, down = summed(0, l)
        grad_ref[0, l] = ahead[:, :units]
        grad_ref[1, l] = ahead[:, units:]
        grad_ref[2, l] = down

    def collect(l):
        for dx in range(1, chips):
            with scope("wait_g2"):
                g2_copy(dx, l).wait_recv()
            got = g2_in[dx - 1, l].astype(f32)
            for n in range(3):
                grad_ref[n, l] += got[:, n * units : (n + 1) * units]

    def own_rows(l):
        slot_rows(l, f)

    loop(local, own_rows)
    returned(f)
    tail = min(2, local)
    head = local - tail
    for l in range(head):
        for t in range(1, nf):
            for sign in (1, -1):
                ag_step(l, t, sign)
            if t == 1 and l + ahead < local:
                ag_own(l + ahead)
        to_core(jnp.int32(l))
        for t in range(1, nf):
            both(t, functools.partial(slot_rows, jnp.int32(l)))
        to_chip(jnp.int32(l))
        if l == 0:
            final(f)
        else:
            keep(jnp.int32(l - 1))
    for t in range(1, nf):
        for l in range(head, local):
            for sign in (1, -1):
                ag_step(l, t, sign)
            if t == nf - 1:
                to_core(jnp.int32(l))

        def rows_back(g):
            for l in range(head, local):
                slot_rows(jnp.int32(l), g)
            returned(g)

        if t == nf - 1:
            to_chip(jnp.int32(head))
        both(t, rows_back)
        if t == 2 and head:

            @pl.when(jnp.logical_not(at_edge))
            def _():
                final(f + near)

    if not head:
        final(f)
    for l in range(head + 1, local):
        to_chip(jnp.int32(l))

    @pl.when(at_edge)
    def _():
        for t in [*range(2, nf - 1), 1, nf - 1]:
            both(t, final)

    @pl.when(jnp.logical_not(at_edge))
    def _():
        if not head:
            final(f + near)
        final(f - near)
        for t in range(2, nf):
            both(t, final)

    with scope("keep"):
        for l in range(max(head - 1, 0), local):
            keep(jnp.int32(l))

    total = [gg_s[e, j : j + 1, :] for j in range(2)]
    for de in range(1, ne):
        gg_copy(de).wait_recv()
        for j in range(2):
            total[j] += gg_r[de, j : j + 1, :]
    for j in range(2):
        gg_ref[j : j + 1, :] = total[j].astype(bf)

    loop(local, collect)

    for d in range(1, nf):
        with scope("wait_tg"):
            put(tg_s.at[0], tg_s.at[0], so.at[d], ro.at[d], (k, e, f_at(d))).wait()
    pltpu.make_async_copy(tg_s.at[0], tg_s.at[0], own_sems.at[5]).wait()
    copies[1].wait()
    copies[2].wait()

    for de in range(ne):
        for d in range(nf):
            if de or d:
                info_copy(de, d).wait_send()
    for g in range(nf):

        @pl.when(f != g)
        def _():
            for a in range(2):
                z_whole(a, g).wait_send()
            rs_copy(g, 1).wait_send()
            prj_copy(g).wait_send()

    for g in range(nf):

        @pl.when(f != g)
        def _():
            put(dl.at[0, group(f), :], dl.at[0, group(f), :], sa.at[0, g], ra.at[0, f], (k, e, g)).wait_send()

    for h in range(1, local):
        for g in range(nf):
            sign = jnp.where(f >= g, 1, -1)

            @pl.when(has(sign))
            def _():
                ag_copy(h, g, sign, g).wait_send()

        @pl.when(f > 0)
        def _():
            ag_copy(h, f, -1, nf).wait_send()

    for de in range(1, ne):
        gg_copy(de).wait_send()
        for g in range(nf):
            y_whole(1, g, de, e).wait_send()
            for kk in range(nk):
                ret_copy(g, de, kk).wait_send()
    for dx in range(chips):
        for a in range(2):
            w_core(a, dx, k).wait_send()
            if dx:
                w_chip(a, dx, k).wait_send()

        def sent(l):
            g1_copy(dx, l).wait_send()
            if dx:
                g2_copy(dx, l).wait_send()

        loop(local, sent)


def per_device(mesh_shape, tokens, out_grad, expert_ids, gate_probs, params, moment_first, moment_second):
    nk, ne, nf = mesh_shape["cuts"], mesh_shape["exp"], mesh_shape["fsdp"]
    token_count, width = tokens.shape
    local, rows, units = params.shape[1:]
    cap = 10 * token_count // 32
    chips = nk // CORES
    span = ne * cap
    slots = local * span
    depth = nk * rows
    bf, f32 = jnp.bfloat16, jnp.float32

    sizes = (nk, ne, nf, local, cap, token_count, rows, units)

    held = []

    def vm(*shape, kind=bf):
        held.append(math.prod(shape) * jnp.dtype(kind).itemsize)
        return pltpu.VMEM(shape, kind)

    def sem(*shape):
        return pltpu.SemaphoreType.DMA(shape)

    scratch = [
        vm(token_count, width),
        vm(token_count, width),
        vm(nf, ne, 8, token_count, kind=f32),
        vm(local, depth, 3 * units),
        vm(nf, ne * token_count, depth),
        vm(nf, ne * token_count, depth),
        vm(nf, slots, ne * token_count),
        vm(local, nf * span, depth),
        vm(local, nf * span, depth),
        vm(nf, slots, 2 * units),
        vm(nf, slots, units),
        vm(nf + 1, slots, 2 * units),
        vm(nf, slots, units),
        vm(slots, 3 * units, kind=f32),
        vm(local, nf * span, 3 * units),
        vm(nf, slots, depth),
        vm(nf, ne - 1, token_count, depth),
        vm(nf, token_count, depth),
        vm(ne, 8, token_count, kind=f32),
        vm(ne, 8, token_count, kind=f32),
        vm(chips, local, rows, 3 * units),
        vm(chips, local, rows, 3 * units),
        vm(chips - 1, local, rows, 3 * units),
        vm(chips - 1, local, rows, 3 * units),
        sem(ne, nf), sem(ne, nf),
        sem(2, nf), sem(2, nf),
        sem(2, nf, ne), sem(2, nf, ne),
        sem(2, chips), sem(2, chips),
        sem(2, chips), sem(2, chips),
        sem(2, nf), sem(2, nf + 1),
        sem(local, nf + 1), sem(local, nf),
        sem(nf, ne, nk), sem(nf, ne, nk),
        sem(nf), sem(nf),
        sem(ne), sem(ne),
        sem(chips, local), sem(chips, local),
        sem(chips, local), sem(chips, local),
        sem(6),
    ]
    grant = sum(held) + MARGIN
    if 3 * grant > 2 * VMEM_ALL:
        grant = VMEM_ALL
    state = jax.ShapeDtypeStruct((3, local, rows, units), f32)
    vmem = pl.BlockSpec(memory_space=pltpu.VMEM)
    hbm = pl.BlockSpec(memory_space=pltpu.HBM)
    anywhere = pl.BlockSpec(memory_space=pl.ANY)
    token_grad, gates, gradient, params, moment_first, moment_second = pl.pallas_call(
        functools.partial(kernel, sizes),
        out_shape=(
            jax.ShapeDtypeStruct((token_count, width), bf),
            jax.ShapeDtypeStruct((2, token_count), bf),
            state, state, state, state,
        ),
        in_specs=[vmem, vmem, hbm, hbm, hbm, hbm, hbm],
        out_specs=(anywhere, vmem, vmem, vmem, vmem, vmem),
        scratch_shapes=scratch,
        compiler_params=pltpu.CompilerParams(
            collective_id=0, has_side_effects=True, vmem_limit_bytes=grant
        ),
    )(
        expert_ids.T,
        gate_probs.T,
        *(pltpu.with_memory_space_constraint(a, pltpu.HBM) for a in (tokens, out_grad, params)),
        *(pltpu.with_memory_space_constraint(a, pltpu.HBM) for a in (moment_first, moment_second)),
    )
    new_params, new_first, new_second = adam_update(params, gradient, moment_first, moment_second)
    return (token_grad, gates.T, new_params, new_first, new_second)


def solution(mesh):
    tokens_spec = P(("cuts", "exp", "fsdp"), None)
    weights_spec = P(None, "exp", ("cuts", "fsdp"), None)
    return jax.shard_map(
        functools.partial(per_device, dict(mesh.shape)),
        mesh=mesh,
        in_specs=(tokens_spec,) * 4 + (weights_spec,) * 3,
        out_specs=(tokens_spec,) * 2 + (weights_spec,) * 3,
        check_vma=False,
    )
```

```python
import functools
import math

import jax
import jax.numpy as jnp
from jax import lax
from jax.experimental import pallas as pl
from jax.experimental.pallas import tpu as pltpu
from jax.sharding import PartitionSpec as P

CORES = 2
VMEM_ALL = 67043328
MARGIN = 2 * 1024 * 1024
MESH = pl.DeviceIdType.MESH

decay_first = 0.9
decay_second = 0.95
correct_first = 1.0 - 0.9**10
correct_second = 1.0 - 0.95**10
epsilon = 1e-08
learn_rate = 0.0003
weight_decay = 0.1


def adam_update(params, gradient, moment_first, moment_second):
    new_first = decay_first * moment_first + (1.0 - decay_first) * gradient
    new_second = decay_second * moment_second + (1.0 - decay_second) * gradient * gradient
    stepped = new_first / correct_first / (jnp.sqrt(new_second / correct_second) + epsilon)
    new_params = params - learn_rate * (stepped + weight_decay * params)
    return (new_params, new_first, new_second)


def loop(count, body):
    def step(i, carry):
        body(i)
        return carry

    lax.fori_loop(0, count, step, 0)


def dot(a, b, dims):
    return lax.dot_general(a, b, (dims, ((), ())), preferred_element_type=jnp.float32)


def kernel(
    sizes,
    ids_ref, gates_ref, tok_hbm, og_hbm, params_hbm, first_hbm, second_hbm,
    tg_ref, gg_ref, grad_ref, par_ref, first_ref, second_ref,
    tok_ref, og_ref, info, weights, tokb, ogb, place, inp, ups, pre_s, prj_s, pre_r, prj_r, own, dl, sg,
    ret_r, tg_s, gg_s, gg_r, g1_out, g1_in, g2_out, g2_in,
    si, ri, sz, rz, sy, ry, sw, rw, sv, rv, sp, rp, sa, ra, st, rt, so, ro, sg_sem, rg_sem, s1, r1, s2, r2,
    own_sems,
):
    nk, ne, nf, local, cap, tcount, rows, units = sizes
    chips = nk // CORES
    span = ne * cap
    slots = local * span
    bf = jnp.bfloat16
    f32 = jnp.float32
    k, e, f = lax.axis_index("cuts"), lax.axis_index("exp"), lax.axis_index("fsdp")
    x, c = k // CORES, lax.rem(k, CORES)
    scope = jax.named_scope

    def f_at(d):
        return lax.rem(f + d, nf)

    def e_at(d):
        return lax.rem(e + d, ne)

    def chip_at(d, core):
        return lax.rem(x + d, chips) * CORES + core

    partner = x * CORES + 1 - c

    def put(src, dst, send, recv, device):
        return pltpu.make_async_remote_copy(
            src_ref=src, dst_ref=dst, send_sem=send, recv_sem=recv, device_id=device, device_id_type=MESH
        )

    def strip(kk, ff):
        return pl.ds(pl.multiple_of((kk * nf + ff) * rows, rows), rows)

    def cut(kk):
        return pl.ds(pl.multiple_of(kk * rows, rows), rows)

    def mine(ee):
        return pl.ds(pl.multiple_of(ee * tcount, tcount), tcount)

    def group(g):
        return pl.ds(pl.multiple_of(g * span, span), span)

    barrier = pltpu.get_barrier_semaphore()
    partners = 0
    for de in range(ne):
        for d in range(nf):
            if de or d:
                pl.semaphore_signal(barrier, inc=1, device_id=(k, e_at(de), f_at(d)), device_id_type=MESH)
                partners += 1
    pl.semaphore_signal(barrier, inc=1, device_id=(partner, e, f), device_id_type=MESH)
    partners += 1
    for dx in range(1, chips):
        pl.semaphore_signal(barrier, inc=1, device_id=(chip_at(dx, c), e, f), device_id_type=MESH)
        partners += 1

    staged = (
        (params_hbm, par_ref), (first_hbm, first_ref), (second_hbm, second_ref), (tok_hbm, tok_ref), (og_hbm, og_ref)
    )
    copies = [pltpu.make_async_copy(src, dst, own_sems.at[n]) for n, (src, dst) in enumerate(staged)]
    for n in (0, 3, 4):
        copies[n].start()

    def iota(shape, dim):
        return lax.broadcasted_iota(jnp.int32, shape, dim)

    experts = iota((local * ne, tcount), 0)
    named = [jnp.where(experts == ids_ref[j : j + 1, :], 1.0, 0.0).astype(f32) for j in range(2)]
    earlier = jnp.where(iota((tcount, tcount), 0) < iota((tcount, tcount), 1), 1.0, 0.0).astype(bf)
    before = dot((named[0] + named[1]).astype(bf), earlier, ((1,), (0,)))
    info[f, e] = jnp.zeros((8, tcount), f32)
    for j in range(2):
        position = jnp.sum(named[j] * before, axis=0, keepdims=True)
        info[f, e, j : j + 1, :] = (ids_ref[j : j + 1, :] * span + e * cap).astype(f32) + position
        info[f, e, j + 2 : j + 3, :] = gates_ref[j : j + 1, :].astype(f32)

    copies[0].wait()
    for l in range(local):
        for n in range(3):
            weights[l, cut(k), n * units : (n + 1) * units] = par_ref[n, l].astype(bf)
    copies[3].wait()
    copies[4].wait()
    with scope("barrier"):
        pl.semaphore_wait(barrier, partners)

    def info_copy(de, d):
        mark = info.at[f, e]
        return put(mark, mark, si.at[de, d], ri.at[de, d], (k, e_at(de), f_at(d)))

    at_edge = (f == 0) | (f == nf - 1)

    def arrivals(a, place):
        if place == 0:
            return [nf - 1, 1, *range(nf - 2, 1, -1)] if a == 0 else [1, *range(nf - 1, 1, -1)]
        ends = [nf - 1, 0] if a == 0 else [0, nf - 1]
        inner = sorted(set(range(1, nf - 1)) - {place}, key=lambda g: abs(g - place))
        return ends + inner

    def arriving(a, n):
        place = jnp.where(f < nf // 2, f, nf - 1 - f)
        g = jnp.int32(arrivals(a, 0)[n])
        for p in range(1, nf // 2):
            g = jnp.where(place == p, arrivals(a, p)[n], g)
        return jnp.where(f < nf // 2, g, nf - 1 - g)

    arrays = ((tok_ref, tokb), (og_ref, ogb))
    wide = (pl.ds(0, 2 * units), pl.ds(2 * units, units))

    def sides(t, work):
        for sign in (1, -1):
            g = f + sign * t

            @pl.when((g >= 0) & (g < nf))
            def _():
                work(g)

    def z_start(a, g):
        src, dst = arrays[a]
        for kk in range(nk):
            put(
                src.at[:, strip(kk, g)], dst.at[f, mine(e), cut(kk)], sz.at[a, g], rz.at[a, f], (k, e, g)
            ).start()

    def y_own_start(a):
        src, dst = arrays[a]
        for de in range(1, ne):
            for kk in range(nk):
                put(
                    src.at[:, strip(kk, f)], dst.at[f, mine(e), cut(kk)], sy.at[a, f, de], ry.at[a, f, de],
                    (k, e_at(de), f),
                ).start()

    def w_chip(a, dx, owner):
        held = weights.at[:, cut(owner), wide[a]]
        return put(held, held, sw.at[a, dx], rw.at[a, dx], (chip_at(dx, c), e, f))

    def w_core(a, dx, owner):
        held = weights.at[:, cut(owner), wide[a]]
        return put(held, held, sv.at[a, dx], rv.at[a, dx], (partner, e, f))

    def whole(dst, g, ee, send, recv, device):
        return put(dst.at[g, mine(ee), :], dst.at[g, mine(ee), :], send, recv, device)

    def z_whole(a, g):
        return whole(arrays[a][1], g, e, sz.at[a, g], rz.at[a, g], (k, e, g))

    def y_whole(a, g, de, ee):
        return whole(arrays[a][1], g, ee, sy.at[a, g, de], ry.at[a, g, de], (k, e_at(de), f))

    def z_pass(a, g):
        with scope("wait_z"):
            z_whole(a, g).wait_recv()
        for de in range(1, ne):
            y_whole(a, g, de, e).start()

    for de in range(ne):
        for d in range(nf):
            if de or d:
                info_copy(de, d).start()
    def z_starts(a, distances):
        for t in distances:
            sides(t, functools.partial(z_start, a))

    @pl.when(at_edge)
    def _():
        z_starts(0, range(nf - 1, 0, -1))
        z_starts(1, [1])

    @pl.when(jnp.logical_not(at_edge))
    def _():
        z_starts(0, range(1, nf))
        z_starts(1, range(1, nf))

    y_own_start(0)
    y_own_start(1)
    for a in range(2):
        for dx in range(1, chips):
            w_chip(a, dx, k).start()
        w_core(a, 0, k).start()

    copies[1].start()
    copies[2].start()
    for src, dst in arrays:
        for kk in range(nk):
            dst[f, mine(e), cut(kk)] = src[:, strip(kk, f)]

    for n in range(nf - 1):
        z_pass(0, arriving(0, n))

    @pl.when(at_edge)
    def _():
        z_starts(1, range(nf - 1, 1, -1))

    z_pass(1, arriving(1, 0))
    for de in range(ne):
        for d in range(nf):
            if de or d:
                info_copy(de, d).wait_recv()

    def w_pass(a):
        with scope("wait_w"):
            for dx in range(1, chips):
                owner = chip_at(chips - dx, c)
                w_chip(a, dx, owner).wait_recv()
                w_core(a, dx, owner).start()

    def w_done(a):
        with scope("wait_w2"):
            for dx in range(chips):
                w_core(a, dx, chip_at(chips - dx, 1 - c)).wait_recv()

    def codes(g, row):
        return jnp.concatenate([info[g, ee, row : row + 1, :] for ee in range(ne)], axis=1)

    first_slot = (e * slots).astype(f32)

    def choose(g, base, count):
        ids = iota((count, ne * tcount), 0).astype(f32) + base
        return [codes(g, j) - first_slot == ids for j in range(2)]

    def at(l):
        return pl.ds(pl.multiple_of(l * span, span), span)

    def picked(a, dst, g):
        src = arrays[a][1]
        for de in range(1, ne):
            with scope("wait_y"):
                y_whole(a, g, de, e_at(ne - de)).wait_recv()

        def column(kk):
            out = dot(place[g], src[g, :, cut(kk)], ((1,), (0,))).astype(bf)
            for l in range(local):
                dst[l, group(g), cut(kk)] = out[l * span : (l + 1) * span]

        loop(nk, column)

    def partial_sum(a, g):
        with scope("partial"):
            if a == 0:
                zero, one = choose(g, 0.0, slots)
                place[g] = jnp.where(zero, 1.0, 0.0).astype(bf) + jnp.where(one, 1.0, 0.0).astype(bf)
            rows_of, sums = ((inp, pre_s), (ups, prj_s))[a]
            picked(a, rows_of, g)

            def expert(l):
                out = dot(rows_of[l, group(g), :], weights[l, :, wide[a]], ((1,), (0,)))
                sums[g, at(l), :] = out.astype(bf)

                @pl.when(g == f)
                def _():
                    own[at(l), wide[a]] = out

            loop(local, expert)

    streams = ((pre_s, pre_r), (prj_s, prj_r))

    def rs_copy(a, g, sign):
        sent, got = streams[a]
        spot = jnp.where((sign < 0) & (g == f - 1), nf, g)
        return put(sent.at[g], got.at[spot], sp.at[a, g], rp.at[a, spot], (k, e, f + sign))

    def rs_wait(a, spot):
        got = streams[a][1]
        put(got.at[spot], got.at[spot], sp.at[a, 0], rp.at[a, spot], (k, e, f_at(1))).wait_recv()

    def rs_step(a, g, sign):
        sent, got = streams[a]
        behind = f - sign

        @pl.when((g - f) * sign > 0)
        def _():
            @pl.when((behind >= 0) & (behind < nf))
            def _():
                with scope("wait_rs"):
                    rs_wait(a, g)

                def add(l):
                    sent[g, at(l), :] = (sent[g, at(l), :].astype(f32) + got[g, at(l), :].astype(f32)).astype(bf)

                loop(local, add)

            rs_copy(a, g, sign).start()

    near = jnp.where(f < nf // 2, 1, -1)

    def rs_chain(a, sign, first=0):
        def steps(n):
            t = n + first
            rs_step(a, jnp.where(sign > 0, nf - 1 - t, t), sign)

        loop(nf - 1 - first, steps)

    def both(t, work):
        def side(n):
            g = f + near * (1 - 2 * n) * t

            @pl.when((g >= 0) & (g < nf))
            def _():
                work(g)

        loop(2, side)

    w_pass(0)
    w_done(0)
    partial_sum(0, f)
    for n in range(nf - 1):
        partial_sum(0, arriving(0, n))

    @pl.when(at_edge)
    def _():
        rs_chain(0, near)

    for n in range(1, nf - 1):
        z_pass(1, arriving(1, n))
        if n == 1:
            w_pass(1)
    w_done(1)

    @pl.when(jnp.logical_not(at_edge))
    def _():
        rs_step(0, jnp.where(near > 0, nf - 1, 0), near)

    partial_sum(1, f)
    for n in range(nf - 1):
        partial_sum(1, arriving(1, n))
        if n == 1:

            @pl.when(jnp.logical_not(at_edge))
            def _():
                rs_chain(0, near, 1)

    @pl.when(jnp.logical_not(at_edge))
    def _():
        rs_chain(0, -near)

    rs_chain(1, near)
    rs_chain(1, -near)

    for a, (_, got) in enumerate(streams):
        for spot, edge in ((f, 0), (nf, nf - 1)):

            @pl.when(f == edge)
            def _():
                got[spot] = jnp.zeros(got.shape[1:], bf)

            @pl.when(f != edge)
            def _():
                with scope("wait_own"):
                    rs_wait(a, spot)

    def middle(l, carry):
        here = at(l)
        gate = own[here, :units] + pre_r[f, here, :units].astype(f32) + pre_r[nf, here, :units].astype(f32)
        up = own[here, units : 2 * units] + pre_r[f, here, units:].astype(f32) + pre_r[nf, here, units:].astype(f32)
        proj = own[here, 2 * units :] + prj_r[f, here, :].astype(f32) + prj_r[nf, here, :].astype(f32)
        zero, one = choose(f, (l * span).astype(f32), span)
        scale = jnp.sum(
            jnp.where(zero, codes(f, 2), 0.0) + jnp.where(one, codes(f, 3), 0.0), axis=1, keepdims=True
        )
        sig = jax.nn.sigmoid(gate)
        act = gate * sig
        hidden = act * up
        slot_gate = jnp.sum(hidden * proj, axis=1, keepdims=True)
        delta = scale * proj
        dl[l, group(f), :units] = (delta * up * sig * (1.0 + gate * (1.0 - sig))).astype(bf)
        dl[l, group(f), units : 2 * units] = (delta * act).astype(bf)
        dl[l, group(f), 2 * units :] = (scale * hidden).astype(bf)
        return (
            carry[0] + jnp.sum(jnp.where(zero, slot_gate, 0.0), axis=0, keepdims=True),
            carry[1] + jnp.sum(jnp.where(one, slot_gate, 0.0), axis=0, keepdims=True),
        )

    def ag_copy(h, g, sign, spot):
        held = dl.at[h, group(g), :]
        return put(held, held, sa.at[h, spot], ra.at[h, g], (k, e, f + sign))

    def has(sign):
        return (f + sign >= 0) & (f + sign < nf)

    def ag_first():
        held = dl.at[0, group(f), :]

        def direct(g):
            put(held, held, sa.at[0, g], ra.at[0, f], (k, e, g)).start()

        @pl.when(at_edge)
        def _():
            for t in range(nf - 1, 0, -1):
                sides(t, direct)

        @pl.when(jnp.logical_not(at_edge))
        def _():
            for t in range(1, nf):
                sides(t, direct)

    def ag_own(h):
        for sign, spot in ((1, f), (-1, nf)):

            @pl.when(has(sign))
            def _():
                ag_copy(h, f, sign, spot).start()

    def ag_step(h, t, sign):
        g = f - sign * t

        @pl.when((g >= 0) & (g < nf))
        def _():
            with scope("wait_ag"):
                ag_copy(h, g, sign, g).wait_recv()

            if h:

                @pl.when(has(sign))
                def _():
                    ag_copy(h, g, sign, g).start()

    nothing = jnp.zeros((1, ne * tcount), f32)
    parts = (nothing, nothing)
    ahead = 2
    for h in range(local):
        with scope("middle"):
            parts = middle(jnp.int32(h), parts)
        if h == 0:
            ag_first()
        elif h < ahead:
            ag_own(h)

    for ee in range(ne):
        for j in range(2):
            gg_s[ee, j : j + 1, :] = parts[j][:, ee * tcount : (ee + 1) * tcount]

    def gg_copy(de):
        return put(gg_s.at[e_at(de)], gg_r.at[de], sg_sem.at[de], rg_sem.at[de], (k, e_at(de), f))

    for de in range(1, ne):
        gg_copy(de).start()

    for de in range(1, ne):
        for g in range(nf):
            y_whole(0, g, de, e).wait_send()

    def ret_copy(g, de, kk):
        return put(
            tokb.at[g, mine(e_at(de)), cut(kk)], ret_r.at[g, de - 1, :, cut(kk)], st.at[g, de, kk],
            rt.at[g, de, kk], (k, e_at(de), f),
        )

    def slot_rows(l, g):
        with scope("slot_rows"):
            sg[g, at(l), :] = dot(dl[l, group(g), : 2 * units], weights[l, :, : 2 * units], ((1,), (1,))).astype(bf)

    def returned(g):
        with scope("returned"):

            def column(kk):
                tokb[g, :, cut(kk)] = dot(place[g], sg[g, :, cut(kk)], ((0,), (0,))).astype(bf)
                for de in range(1, ne):
                    ret_copy(g, de, kk).start()

            loop(nk, column)

    def final(g):
        with scope("final"):
            d = lax.rem(g - f + nf, nf)

            def column(kk):
                total = tokb[g, mine(e), cut(kk)].astype(f32)
                for de in range(1, ne):
                    with scope("wait_ret"):
                        ret_copy(g, de, kk).wait_recv()
                    total += ret_r[g, de - 1, :, cut(kk)].astype(f32)
                tg_s[g, :, cut(kk)] = total.astype(bf)
                there = tg_ref.at[:, strip(kk, f)]

                @pl.when(d > 0)
                def _():
                    put(tg_s.at[g, :, cut(kk)], there, so.at[d], ro.at[d], (k, e, g)).start()

                @pl.when(d == 0)
                def _():
                    pltpu.make_async_copy(tg_s.at[g, :, cut(kk)], there, own_sems.at[5]).start()

            loop(nk, column)

    def gradient(kk, l):
        ahead = dot(inp[l, :, cut(kk)], dl[l, :, : 2 * units], ((0,), (0,)))
        down = dot(ups[l, :, cut(kk)], dl[l, :, 2 * units :], ((0,), (0,)))
        return ahead, down

    def g1_copy(dx, l):
        return put(g1_out.at[dx, l], g1_in.at[dx, l], s1.at[dx, l], r1.at[dx, l], (partner, e, f))

    def g2_copy(dx, l):
        return put(g2_out.at[dx - 1, l], g2_in.at[dx - 1, l], s2.at[dx, l], r2.at[dx, l], (chip_at(dx, c), e, f))

    def to_core(l):
        with scope("to_core"):
            for dx in [*range(1, chips), 0]:
                ahead, down = gradient(chip_at(dx, 1 - c), l)
                g1_out[dx, l, :, : 2 * units] = ahead.astype(bf)
                g1_out[dx, l, :, 2 * units :] = down.astype(bf)
                g1_copy(dx, l).start()

    def summed(dx, l):
        ahead, down = gradient(chip_at(dx, c), l)
        with scope("wait_g1"):
            g1_copy(dx, l).wait_recv()
        ahead += g1_in[dx, l, :, : 2 * units].astype(f32)
        down += g1_in[dx, l, :, 2 * units :].astype(f32)
        return ahead, down

    def to_chip(l):
        with scope("to_chip"):
            for dx in range(1, chips):
                ahead, down = summed(dx, l)
                g2_out[dx - 1, l, :, : 2 * units] = ahead.astype(bf)
                g2_out[dx - 1, l, :, 2 * units :] = down.astype(bf)
                g2_copy(dx, l).start()

    def keep(l):
        ahead, down = summed(0, l)
        grad_ref[0, l] = ahead[:, :units]
        grad_ref[1, l] = ahead[:, units:]
        grad_ref[2, l] = down

    def collect(l):
        for dx in range(1, chips):
            with scope("wait_g2"):
                g2_copy(dx, l).wait_recv()
            got = g2_in[dx - 1, l].astype(f32)
            for n in range(3):
                grad_ref[n, l] += got[:, n * units : (n + 1) * units]

    def own_rows(l):
        slot_rows(l, f)

    loop(local, own_rows)
    returned(f)
    tail = min(2, local)
    head = local - tail
    for l in range(head):
        for t in range(1, nf):
            for sign in (1, -1):
                ag_step(l, t, sign)
            if t == 1 and l + ahead < local:
                ag_own(l + ahead)
        to_core(jnp.int32(l))
        for t in range(1, nf):
            both(t, functools.partial(slot_rows, jnp.int32(l)))
        to_chip(jnp.int32(l))
        if l == 0:
            final(f)
        else:
            keep(jnp.int32(l - 1))
    for t in range(1, nf):
        for l in range(head, local):
            for sign in (1, -1):
                ag_step(l, t, sign)
            if t == nf - 1:
                to_core(jnp.int32(l))

        def rows_back(g):
            for l in range(head, local):
                slot_rows(jnp.int32(l), g)
            returned(g)

        if t == nf - 1:
            to_chip(jnp.int32(head))
        both(t, rows_back)
        if t == 2 and head:

            @pl.when(jnp.logical_not(at_edge))
            def _():
                final(f + near)

    if not head:
        final(f)
    for l in range(head + 1, local):
        to_chip(jnp.int32(l))

    @pl.when(at_edge)
    def _():
        for t in [*range(2, nf - 1), 1, nf - 1]:
            both(t, final)

    @pl.when(jnp.logical_not(at_edge))
    def _():
        if not head:
            final(f + near)
        final(f - near)
        for t in range(2, nf):
            both(t, final)

    with scope("keep"):
        for l in range(max(head - 1, 0), local):
            keep(jnp.int32(l))

    total = [gg_s[e, j : j + 1, :] for j in range(2)]
    for de in range(1, ne):
        gg_copy(de).wait_recv()
        for j in range(2):
            total[j] += gg_r[de, j : j + 1, :]
    for j in range(2):
        gg_ref[j : j + 1, :] = total[j].astype(bf)

    loop(local, collect)

    for d in range(1, nf):
        with scope("wait_tg"):
            put(tg_s.at[0], tg_s.at[0], so.at[d], ro.at[d], (k, e, f_at(d))).wait()
    pltpu.make_async_copy(tg_s.at[0], tg_s.at[0], own_sems.at[5]).wait()
    copies[1].wait()
    copies[2].wait()

    for de in range(ne):
        for d in range(nf):
            if de or d:
                info_copy(de, d).wait_send()
    for g in range(nf):

        @pl.when(f != g)
        def _():
            for a in range(2):
                z_whole(a, g).wait_send()
            for a in range(2):
                rs_copy(a, g, 1).wait_send()

    for g in range(nf):

        @pl.when(f != g)
        def _():
            put(dl.at[0, group(f), :], dl.at[0, group(f), :], sa.at[0, g], ra.at[0, f], (k, e, g)).wait_send()

    for h in range(1, local):
        for g in range(nf):
            sign = jnp.where(f >= g, 1, -1)

            @pl.when(has(sign))
            def _():
                ag_copy(h, g, sign, g).wait_send()

        @pl.when(f > 0)
        def _():
            ag_copy(h, f, -1, nf).wait_send()

    for de in range(1, ne):
        gg_copy(de).wait_send()
        for g in range(nf):
            y_whole(1, g, de, e).wait_send()
            for kk in range(nk):
                ret_copy(g, de, kk).wait_send()
    for dx in range(chips):
        for a in range(2):
            w_core(a, dx, k).wait_send()
            if dx:
                w_chip(a, dx, k).wait_send()

        def sent(l):
            g1_copy(dx, l).wait_send()
            if dx:
                g2_copy(dx, l).wait_send()

        loop(local, sent)


def per_device(mesh_shape, tokens, out_grad, expert_ids, gate_probs, params, moment_first, moment_second):
    nk, ne, nf = mesh_shape["cuts"], mesh_shape["exp"], mesh_shape["fsdp"]
    token_count, width = tokens.shape
    local, rows, units = params.shape[1:]
    cap = 10 * token_count // 32
    chips = nk // CORES
    span = ne * cap
    slots = local * span
    depth = nk * rows
    bf, f32 = jnp.bfloat16, jnp.float32

    sizes = (nk, ne, nf, local, cap, token_count, rows, units)

    held = []

    def vm(*shape, kind=bf):
        held.append(math.prod(shape) * jnp.dtype(kind).itemsize)
        return pltpu.VMEM(shape, kind)

    def sem(*shape):
        return pltpu.SemaphoreType.DMA(shape)

    scratch = [
        vm(token_count, width),
        vm(token_count, width),
        vm(nf, ne, 8, token_count, kind=f32),
        vm(local, depth, 3 * units),
        vm(nf, ne * token_count, depth),
        vm(nf, ne * token_count, depth),
        vm(nf, slots, ne * token_count),
        vm(local, nf * span, depth),
        vm(local, nf * span, depth),
        vm(nf, slots, 2 * units),
        vm(nf, slots, units),
        vm(nf + 1, slots, 2 * units),
        vm(nf + 1, slots, units),
        vm(slots, 3 * units, kind=f32),
        vm(local, nf * span, 3 * units),
        vm(nf, slots, depth),
        vm(nf, ne - 1, token_count, depth),
        vm(nf, token_count, depth),
        vm(ne, 8, token_count, kind=f32),
        vm(ne, 8, token_count, kind=f32),
        vm(chips, local, rows, 3 * units),
        vm(chips, local, rows, 3 * units),
        vm(chips - 1, local, rows, 3 * units),
        vm(chips - 1, local, rows, 3 * units),
        sem(ne, nf), sem(ne, nf),
        sem(2, nf), sem(2, nf),
        sem(2, nf, ne), sem(2, nf, ne),
        sem(2, chips), sem(2, chips),
        sem(2, chips), sem(2, chips),
        sem(2, nf), sem(2, nf + 1),
        sem(local, nf + 1), sem(local, nf),
        sem(nf, ne, nk), sem(nf, ne, nk),
        sem(nf), sem(nf),
        sem(ne), sem(ne),
        sem(chips, local), sem(chips, local),
        sem(chips, local), sem(chips, local),
        sem(6),
    ]
    grant = sum(held) + MARGIN
    if 3 * grant > 2 * VMEM_ALL:
        grant = VMEM_ALL
    state = jax.ShapeDtypeStruct((3, local, rows, units), f32)
    vmem = pl.BlockSpec(memory_space=pltpu.VMEM)
    hbm = pl.BlockSpec(memory_space=pltpu.HBM)
    anywhere = pl.BlockSpec(memory_space=pl.ANY)
    token_grad, gates, gradient, params, moment_first, moment_second = pl.pallas_call(
        functools.partial(kernel, sizes),
        out_shape=(
            jax.ShapeDtypeStruct((token_count, width), bf),
            jax.ShapeDtypeStruct((2, token_count), bf),
            state, state, state, state,
        ),
        in_specs=[vmem, vmem, hbm, hbm, hbm, hbm, hbm],
        out_specs=(anywhere, vmem, vmem, vmem, vmem, vmem),
        scratch_shapes=scratch,
        compiler_params=pltpu.CompilerParams(
            collective_id=0, has_side_effects=True, vmem_limit_bytes=grant
        ),
    )(
        expert_ids.T,
        gate_probs.T,
        *(pltpu.with_memory_space_constraint(a, pltpu.HBM) for a in (tokens, out_grad, params)),
        *(pltpu.with_memory_space_constraint(a, pltpu.HBM) for a in (moment_first, moment_second)),
    )
    new_params, new_first, new_second = adam_update(params, gradient, moment_first, moment_second)
    return (token_grad, gates.T, new_params, new_first, new_second)


def solution(mesh):
    tokens_spec = P(("cuts", "exp", "fsdp"), None)
    weights_spec = P(None, "exp", ("cuts", "fsdp"), None)
    return jax.shard_map(
        functools.partial(per_device, dict(mesh.shape)),
        mesh=mesh,
        in_specs=(tokens_spec,) * 4 + (weights_spec,) * 3,
        out_specs=(tokens_spec,) * 2 + (weights_spec,) * 3,
        check_vma=False,
    )
```
